128 devices in a mesh: model: 16 (over z, y), data: 8 (over x, core).
Axes of the slice: x: 4, y: 4, z: 4, core: 2. Of those that a mesh axis runs over, the one named last changes fastest.
Arguments:
- h_a: bfloat16 [16384, 2048], P('data')
- h_b: bfloat16 [16384, 2048], P('data')
- w_one: bfloat16 [2048, 2048], P(None, 'model')
- w_two: bfloat16 [2048, 2048], P('model')
- w_three: bfloat16 [2048, 2048], P(None, 'model')
- g_one: float32 [2048], P('model')
- b_one: float32 [2048], P('model')
- g_two: float32 [2048], replicated
- b_two: float32 [2048], replicated
- lam_off: float32 [1], replicated
Outputs:
- output 1: float32 [1], replicated
- output 2: float32 [2048, 2048], P(None, 'model')
- output 3: float32 [2048, 2048], P('model')
- output 4: float32 [2048, 2048], P(None, 'model')
- output 5: float32 [2048], P('model')
- output 6: float32 [2048], P('model')
- output 7: float32 [2048], replicated
- output 8: float32 [2048], replicated
All inputs are finite; a program needn't handle non-finite values.
Results may differ from the reference program's by a relative error of at most 0.001.
Values are sent between devices in bfloat16 or wider.
A program may use at most 1 GiB of HBM per device.

```python
import jax
import jax.numpy as jnp
from jax import lax
import math

N = 16384
F = 2048
D = 2048
SHARDS = 8
BN_EPS = 1e-5


def setup_inputs(seed: int = 0) -> dict:
    root_key = jax.random.key(seed)
    key_list = jax.random.split(root_key, 13)
    shard_rows = N // SHARDS
    shared_img = jax.random.normal(key_list[0], (N, F), jnp.float32)
    shard_shift = 0.5 * jax.random.normal(key_list[1], (SHARDS, 1, F), jnp.float32)
    shard_scale = jnp.exp(0.3 * jax.random.normal(key_list[2], (SHARDS, 1, F), jnp.float32))

    def make_view(view_key):
        noisy_img = shared_img + 0.6 * jax.random.normal(view_key, (N, F), jnp.float32)
        shaped = noisy_img.reshape(SHARDS, shard_rows, F) * shard_scale + shard_shift
        return shaped.reshape(N, F).astype(jnp.bfloat16)

    def make_weight(w_key, fan_in, fan_out):
        return (jax.random.normal(w_key, (fan_in, fan_out), jnp.float32) / math.sqrt(fan_in)).astype(jnp.bfloat16)

    lam_scale = 0.5 * F * N / (D * (N + 2.0 * F))
    return {
        'h_a': make_view(key_list[3]),
        'h_b': make_view(key_list[4]),
        'w_one': make_weight(key_list[5], F, D),
        'w_two': make_weight(key_list[6], D, D),
        'w_three': make_weight(key_list[7], D, D),
        'g_one': 1.0 + 0.25 * jax.random.normal(key_list[8], (D,), jnp.float32),
        'b_one': 0.4 * jax.random.normal(key_list[9], (D,), jnp.float32),
        'g_two': 1.0 + 0.25 * jax.random.normal(key_list[10], (D,), jnp.float32),
        'b_two': 0.4 * jax.random.normal(key_list[11], (D,), jnp.float32),
        'lam_off': lam_scale * (0.5 + jax.random.uniform(key_list[12], (1,), jnp.float32)),
    }


def matmul(left, right):
    return jnp.dot(left, right, preferred_element_type=jnp.float32)


def batch_norm(pre_act):
    mean_val = jnp.sum(pre_act, axis=1, keepdims=True) / N
    mean_sq = jnp.sum(pre_act * pre_act, axis=1, keepdims=True) / N
    inv_std = lax.rsqrt(mean_sq - mean_val * mean_val + BN_EPS)
    return (pre_act - mean_val) * inv_std, inv_std


def bn_backward(d_act, lin_val, norm_val, inv_std, gamma_vec):
    d_lin = jnp.where(lin_val > 0, d_act, 0.0)
    sum_lin = jnp.sum(d_lin, axis=1, keepdims=True)
    sum_norm = jnp.sum(d_lin * norm_val, axis=1, keepdims=True)
    d_pre = gamma_vec * inv_std * (d_lin - (sum_lin + norm_val * sum_norm) / N)
    return d_pre.astype(jnp.bfloat16), jnp.sum(sum_norm, axis=(0, 1)), jnp.sum(sum_lin, axis=(0, 1))


def reference(h_a, h_b, w_one, w_two, w_three, g_one, b_one, g_two, b_two, lam_off):
    view_feats = jnp.concatenate([h_a, h_b], axis=0)
    pre_one = matmul(view_feats, w_one).reshape(2, N, D)
    norm_one, inv_one = batch_norm(pre_one)
    lin_one = g_one * norm_one + b_one
    act_one = jnp.maximum(lin_one, 0.0).astype(jnp.bfloat16)
    pre_two = matmul(act_one.reshape(2 * N, D), w_two).reshape(2, N, D)
    norm_two, inv_two = batch_norm(pre_two)
    lin_two = g_two * norm_two + b_two
    act_two = jnp.maximum(lin_two, 0.0).astype(jnp.bfloat16)
    pre_out = matmul(act_two.reshape(2 * N, D), w_three).reshape(2, N, D)
    norm_out, inv_out = batch_norm(pre_out)
    embed_bf = norm_out.astype(jnp.bfloat16)
    corr_mat = matmul(embed_bf[0].T, embed_bf[1]) / N
    is_diag = jnp.arange(D)[:, None] == jnp.arange(D)[None, :]
    lam_val = lam_off[0]
    loss_val = jnp.sum(jnp.where(is_diag, (1.0 - corr_mat) * (1.0 - corr_mat), lam_val * corr_mat * corr_mat))
    grad_c = jnp.where(is_diag, -2.0 * (1.0 - corr_mat), 2.0 * lam_val * corr_mat).astype(jnp.bfloat16)
    d_emb = jnp.stack([matmul(embed_bf[1], grad_c.T), matmul(embed_bf[0], grad_c)]) / N
    embed_f = embed_bf.astype(jnp.float32)
    sum_g = jnp.sum(d_emb, axis=1, keepdims=True)
    sum_gz = jnp.sum(d_emb * embed_f, axis=1, keepdims=True)
    d_out = (inv_out * (d_emb - (sum_g + embed_f * sum_gz) / N)).astype(jnp.bfloat16)
    dw_three = matmul(act_two.reshape(2 * N, D).T, d_out.reshape(2 * N, D))
    d_act_two = matmul(d_out.reshape(2 * N, D), w_three.T).reshape(2, N, D)
    d_pre_two, dg_two, db_two = bn_backward(d_act_two, lin_two, norm_two, inv_two, g_two)
    dw_two = matmul(act_one.reshape(2 * N, D).T, d_pre_two.reshape(2 * N, D))
    d_act_one = matmul(d_pre_two.reshape(2 * N, D), w_two.T).reshape(2, N, D)
    d_pre_one, dg_one, db_one = bn_backward(d_act_one, lin_one, norm_one, inv_one, g_one)
    dw_one = matmul(view_feats.T, d_pre_one.reshape(2 * N, D))
    return loss_val.reshape(1), dw_one, dw_two, dw_three, dg_one, db_one, dg_two, db_two
```

```python
import jax
import jax.numpy as jnp
from jax import lax
from jax.sharding import PartitionSpec as P

BN_EPS = 1e-5
ALL = ('model', 'data')


def batch_norm(pre_act, total_rows):
    local_sums = jnp.stack([jnp.sum(pre_act, axis=1, keepdims=True), jnp.sum(pre_act * pre_act, axis=1, keepdims=True)])
    moments = lax.psum(local_sums, ALL) / total_rows
    inv_std = lax.rsqrt(moments[1] - moments[0] * moments[0] + BN_EPS)
    return (pre_act - moments[0]) * inv_std, inv_std


def bn_backward(d_act, lin_val, norm_val, inv_std, gamma_vec, total_rows):
    d_lin = jnp.where(lin_val > 0, d_act, 0.0)
    local_sums = jnp.stack([jnp.sum(d_lin, axis=1, keepdims=True), jnp.sum(d_lin * norm_val, axis=1, keepdims=True)])
    global_sums = lax.psum(local_sums, ALL)
    d_pre = gamma_vec * inv_std * (d_lin - (global_sums[0] + norm_val * global_sums[1]) / total_rows)
    return d_pre.astype(jnp.bfloat16), jnp.sum(global_sums[1], axis=(0, 1)), jnp.sum(global_sums[0], axis=(0, 1))


def solution(mesh):
    data_size = mesh.shape['data']
    model_size = mesh.shape['model']

    def shard_body(h_a, h_b, w_one, w_two, w_three, g_one, b_one, g_two, b_two, lam_off):
        group_rows = h_a.shape[0]
        total_rows = group_rows * data_size
        rows = group_rows // model_size
        full_dim, feat_dev = w_three.shape
        mid = lax.axis_index('model')
        h_all = jnp.stack([h_a, h_b])
        h_loc = lax.dynamic_slice_in_dim(h_all, mid * rows, rows, axis=1)
        w1 = lax.all_gather(w_one, 'model', axis=1, tiled=True)
        w2 = lax.all_gather(w_two, 'model', axis=0, tiled=True)
        w3 = lax.all_gather(w_three, 'model', axis=1, tiled=True)
        gb = lax.all_gather(jnp.stack([g_one, b_one]), 'model', axis=1, tiled=True)
        g1, b1 = gb[0], gb[1]

        def mm(spec, a, b):
            return jnp.einsum(spec, a, b, preferred_element_type=jnp.float32)

        pre_one = mm('vnf,fd->vnd', h_loc, w1)
        norm_one, inv_one = batch_norm(pre_one, total_rows)
        lin_one = g1 * norm_one + b1
        act_one = jnp.maximum(lin_one, 0.0).astype(jnp.bfloat16)
        pre_two = mm('woe,ef->wof', act_one, w2)
        norm_two, inv_two = batch_norm(pre_two, total_rows)
        lin_two = g_two * norm_two + b_two
        act_two = jnp.maximum(lin_two, 0.0).astype(jnp.bfloat16)
        pre_out = mm('woe,ef->wof', act_two, w3)
        norm_out, inv_out = batch_norm(pre_out, total_rows)
        emb = norm_out.astype(jnp.bfloat16)
        corr = lax.psum_scatter(mm('ni,nj->ij', emb[0], emb[1]), ALL, scatter_dimension=0, tiled=True) / total_rows
        piece = corr.shape[0]
        did = mid * data_size + lax.axis_index('data')
        row_ids = did * piece + lax.broadcasted_iota(jnp.int32, (piece, 1), 0)
        is_diag = row_ids == lax.broadcasted_iota(jnp.int32, (1, full_dim), 1)
        lam = lam_off[0]
        loss = lax.psum(jnp.sum(jnp.where(is_diag, (1.0 - corr) * (1.0 - corr), lam * corr * corr)), ALL)
        grad_piece = jnp.where(is_diag, -2.0 * (1.0 - corr), 2.0 * lam * corr).astype(jnp.bfloat16)
        grad_c = lax.all_gather(grad_piece, ALL, axis=0, tiled=True)
        d_emb = jnp.stack([mm('nj,ij->ni', emb[1], grad_c), mm('ni,ij->nj', emb[0], grad_c)]) / total_rows
        emb_f = emb.astype(jnp.float32)
        sums = jnp.stack([jnp.sum(d_emb, axis=1, keepdims=True), jnp.sum(d_emb * emb_f, axis=1, keepdims=True)])
        gm = lax.psum(sums, ALL) / total_rows
        d_out = (inv_out * (d_emb - gm[0] - emb_f * gm[1])).astype(jnp.bfloat16)
        dw3 = lax.psum_scatter(mm('woe,wof->ef', act_two, d_out), 'model', scatter_dimension=1, tiled=True)
        d_act_two = mm('wof,ef->woe', d_out, w3)
        d_pre_two, dg_two, db_two = bn_backward(d_act_two, lin_two, norm_two, inv_two, g_two, total_rows)
        dw2 = lax.psum_scatter(mm('woe,wof->ef', act_one, d_pre_two), 'model', scatter_dimension=0, tiled=True)
        d_act_one = mm('wof,ef->woe', d_pre_two, w2)
        d_pre_one, dg_one, db_one = bn_backward(d_act_one, lin_one, norm_one, inv_one, g1, total_rows)
        d_cols = lax.all_to_all(d_pre_one, 'model', split_axis=2, concat_axis=1, tiled=True)
        dw1 = mm('vnf,vnd->fd', h_all, d_cols)
        dw1, dw2, dw3 = lax.psum((dw1, dw2, dw3), 'data')
        dgb = lax.dynamic_slice_in_dim(jnp.stack([dg_one, db_one]), mid * feat_dev, feat_dev, axis=1)
        return loss.reshape(1), dw1, dw2, dw3, dgb[0], dgb[1], dg_two, db_two

    in_specs = (P('data', None), P('data', None), P(None, 'model'), P('model', None), P(None, 'model'),
                P('model'), P('model'), P(), P(), P())
    out_specs = (P(), P(None, 'model'), P('model', None), P(None, 'model'), P('model'), P('model'), P(), P())
    return jax.shard_map(shard_body, mesh=mesh, in_specs=in_specs, out_specs=out_specs, check_vma=False)
```

```python
import functools

import jax
import jax.numpy as jnp
from jax import lax
from jax.experimental import pallas as pl
from jax.experimental.pallas import tpu as pltpu
from jax.sharding import PartitionSpec as P

BN_EPS = 1e-5
MESH_ID = pl.DeviceIdType.MESH
RING = 4
PAIR = 2
AXES = ('z', 'y', 'x')
ORDERS = (('x', 'y', 'z'), ('y', 'z', 'x'), ('z', 'x', 'y'))
LANES = tuple((sub, colour) for sub in range(PAIR) for colour in range(3))
OTHERS = (1, 2, 3)
N_SEND = 250
N_RECV = 480
F32 = jnp.float32
BF16 = jnp.bfloat16
WHOLE = slice(None)


def dot_nn(a, b):
    return lax.dot_general(a, b, (((1,), (0,)), ((), ())), preferred_element_type=F32)


def dot_nt(a, b):
    return lax.dot_general(a, b, (((1,), (1,)), ((), ())), preferred_element_type=F32)


def dot_tn(a, b):
    return lax.dot_general(a, b, (((0,), (0,)), ((), ())), preferred_element_type=F32)


def col_sum(value):
    return jnp.sum(value, axis=0, keepdims=True)


def lanes_of(values):
    return jnp.concatenate(list(values), axis=1)


def wrap(value):
    return lax.rem(value, RING)


def step(*gens):
    for gen in gens:
        next(gen, None)


def finish(gens):
    live = list(gens)
    while live:
        live = [gen for gen in live if next(gen, WHOLE) is not WHOLE]


def mega_kernel(cfg, h_a, h_b, w_one, w_two, w_three, g_one, b_one, g_two, b_two, lam_ref,
                dw_out, small_out,
                hx, u1, u2, u3, xf1, xf2, zf, wg1, wq1, wg2, wq2, wg3, part, part2, rv1, rv2, rv3,
                gbuf, stat, sres, dgb, du1, a2a, out_w, ssem, rsem, lsem, hsem, credit):
    blk, rows, total_rows, splits = cfg
    half = 8 * blk
    quad = PAIR * blk
    vrows = PAIR * rows
    inv_n = 1.0 / total_rows

    mid = lax.axis_index('model')
    did = lax.axis_index('data')
    core = lax.rem(did, PAIR)
    other = 1 - core
    coord = {'z': lax.div(mid, RING), 'y': wrap(mid), 'x': lax.div(did, PAIR)}
    zc, yc, xc = coord['z'], coord['y'], coord['x']
    near = {axis: [coord[axis]] + [wrap(coord[axis] + off) for off in OTHERS] for axis in AXES}
    z_base, x_base = zc * RING, xc * PAIR
    targets_of = {'z': [(q * RING + yc, did) for q in near['z']], 'y': [(z_base + q, did) for q in near['y']],
                  'x': [(mid, q * PAIR + core) for q in near['x']]}
    peer = (mid, x_base + other)

    def device(axis, off):
        return targets_of[axis][off]

    z_own, z_other = PAIR * core, PAIR * other
    counters = {'s': 0, 'r': 0, 'l': 0}

    def new_ids(kind, count):
        first = counters[kind]
        counters[kind] = first + count
        assert counters[kind] <= {'s': N_SEND, 'r': N_RECV, 'l': 16}[kind]
        return list(range(first, first + count))

    def rcopy(src, dst, send_id, recv_id, target):
        return pltpu.make_async_remote_copy(src_ref=src, dst_ref=dst, send_sem=ssem.at[send_id],
                                            recv_sem=rsem.at[recv_id], device_id=target, device_id_type=MESH_ID)

    def band(sub, colour):
        begin = 0
        for size in splits[sub][:colour]:
            begin += size
        return pl.ds(begin, splits[sub][colour])

    def gather_lane(buf, sub, colour, sid, rid):
        order = ORDERS[colour]
        rsl = band(sub, colour)

        def region(axis, have, q, part_id=None):
            idx = dict(coord)
            idx[axis] = q
            for name in have:
                idx[name] = pl.ds(0, RING)
            if part_id is not None:
                idx[have[-1]] = pl.ds(PAIR * part_id, PAIR)
            return buf.at[idx['z'], idx['y'], idx['x'], sub, rsl, :]

        axis = order[0]
        own = region(axis, (), coord[axis])
        pending = [rcopy(own, own, sid[off - 1], rid[off - 1], device(axis, off)) for off in OTHERS]
        for copy in pending:
            copy.start()
        yield
        for copy in pending:
            copy.wait_recv()
        for phase in (1, 2):
            axis, have = order[phase], order[:phase]
            base = phase * RING - 1
            p = coord[axis]
            up, down = device(axis, 1), device(axis, 3)
            own = region(axis, have, p)
            to_up = rcopy(own, own, sid[base], rid[base], up)
            to_down = rcopy(own, own, sid[base + 1], rid[base + 1], down)
            to_up.start()
            to_down.start()
            yield
            to_up.wait_recv()
            src = region(axis, have, near[axis][3], 0)
            relay_up = rcopy(src, src, sid[base + 2], rid[base + 2], up)
            relay_up.start()
            to_down.wait_recv()
            src = region(axis, have, near[axis][1], 1)
            relay_down = rcopy(src, src, sid[base + 3], rid[base + 3], down)
            relay_down.start()
            yield
            relay_up.wait_recv()
            relay_down.wait_recv()
            pending.extend((to_up, to_down, relay_up, relay_down))
        for copy in pending:
            copy.wait_send()

    def gather_lanes(buf, send_ids, recv_ids):
        width = 11
        return [gather_lane(buf, sub, colour, send_ids[k * width:(k + 1) * width], recv_ids[k * width:(k + 1) * width])
                for k, (sub, colour) in enumerate(LANES)]

    def scatter_lane(buf, bank, sub, colour, sid, rid, give, take):
        order = ORDERS[colour]
        rsl = band(sub, colour)
        pending = []
        for phase in (0, 1):
            axis = order[phase]
            left = tuple(name for name in AXES if name in order[phase + 1:])
            p = coord[axis]
            base = phase * 6

            def region(q, part_id, axis=axis, left=left):
                idx = dict(coord)
                idx[axis] = q
                for name in left[:-1]:
                    idx[name] = pl.ds(0, RING)
                idx[left[-1]] = pl.ds(PAIR * part_id, PAIR)
                return buf.at[idx['z'], idx['y'], idx['x'], sub, rsl, :]

            def landing(slot, phase=phase):
                if phase:
                    return rv2.at[bank, sub, slot, :, rsl, :]
                return rv1.at[sub, slot, :, :, rsl, :]

            def add(q, part_id, slots, axis=axis, left=left, phase=phase):
                def one(i, j):
                    idx = dict(coord)
                    idx[axis] = q
                    idx[left[-1]] = PAIR * part_id + j
                    if not phase:
                        idx[left[0]] = i
                    total = buf[idx['z'], idx['y'], idx['x'], sub, rsl, :]
                    for slot in slots:
                        total = total + (rv2[bank, sub, slot, j, rsl, :] if phase else rv1[sub, slot, i, j, rsl, :])
                    buf[idx['z'], idx['y'], idx['x'], sub, rsl, :] = total

                if phase:
                    for j in range(PAIR):
                        one(0, j)
                else:
                    @pl.loop(0, RING)
                    def _(i):
                        for j in range(PAIR):
                            one(i, j)

            up, down = device(axis, 1), device(axis, 3)
            p1, p2, p3 = near[axis][1:]
            if take is not None and not phase:
                pl.semaphore_wait(credit.at[take], PAIR)
            relay_up = rcopy(region(p2, 1), landing(0), sid[base], rid[base], up)
            relay_down = rcopy(region(p2, 0), landing(1), sid[base + 1], rid[base + 1], down)
            own_up = rcopy(region(p1, 0), landing(2), sid[base + 2], rid[base + 2], up)
            own_down = rcopy(region(p3, 1), landing(3), sid[base + 3], rid[base + 3], down)
            relay_up.start()
            relay_down.start()
            if not phase:
                yield
            own_up.start()
            own_down.start()
            yield
            relay_up.wait_recv()
            add(p1, 1, (0,))
            sum_up = rcopy(region(p1, 1), landing(4), sid[base + 4], rid[base + 4], up)
            sum_up.start()
            relay_down.wait_recv()
            add(p3, 0, (1,))
            sum_down = rcopy(region(p3, 0), landing(5), sid[base + 5], rid[base + 5], down)
            sum_down.start()
            yield
            own_up.wait_recv()
            sum_down.wait_recv()
            add(p, 0, (2, 5))
            own_down.wait_recv()
            sum_up.wait_recv()
            add(p, 1, (3, 4))
            if give is not None and not phase:
                for target in (up, down):
                    pl.semaphore_signal(credit.at[give], inc=1, device_id=target, device_id_type=MESH_ID)
            pending.extend((relay_up, relay_down, own_up, own_down, sum_up, sum_down))
        axis = order[2]
        p = coord[axis]
        base = 12
        last = []
        for k, off in enumerate(OTHERS):
            idx = dict(coord)
            idx[axis] = near[axis][off]
            last.append(rcopy(buf.at[idx['z'], idx['y'], idx['x'], sub, rsl, :], rv3.at[bank, sub, k, rsl, :],
                              sid[base + k], rid[base + k], device(axis, off)))
        for copy in last:
            copy.start()
        yield
        for copy in last:
            copy.wait_recv()
        got = [rv3[bank, sub, k, rsl, :] for k in range(3)]
        buf[zc, yc, xc, sub, rsl, :] = (buf[zc, yc, xc, sub, rsl, :] + got[0]) + (got[1] + got[2])
        for copy in pending + last:
            copy.wait_send()

    def scatter_lanes(buf, bank, send_ids, recv_ids, give=None, take=None):
        width = 15
        return [scatter_lane(buf, bank, sub, colour, send_ids[k * width:(k + 1) * width],
                             recv_ids[k * width:(k + 1) * width], k if give else None, k if take else None)
                for k, (sub, colour) in enumerate(LANES)]

    def quarter(src, dst, sub, send_id, recv_id):
        copy = rcopy(src.at[pl.ds(z_other, PAIR), :, :, sub], dst.at[:, :, :, sub], send_id, recv_id, peer)
        copy.start()
        return copy

    stat_recv = [new_ids('r', 9) for _ in range(PAIR)]
    stat_send = new_ids('s', 9)

    def stat_sum(parity, width, fill=None):
        pending = []
        for d, axis in enumerate(AXES):
            own = stat.at[parity, d, coord[axis], :, pl.ds(0, width)]
            copies = [rcopy(own, own, stat_send[d * 3 + off - 1], stat_recv[parity][d * 3 + off - 1], device(axis, off))
                      for off in OTHERS]
            for copy in copies:
                copy.start()
            if fill is not None:
                step(*fill[d])
            for copy in copies:
                copy.wait_recv()
            got = [stat[parity, d, q, :, 0:width] for q in range(RING)]
            total = (got[0] + got[1]) + (got[2] + got[3])
            if axis != 'x':
                stat[parity, d + 1, coord[AXES[d + 1]], :, 0:width] = total
            pending.extend(copies)
        for copy in pending:
            copy.wait_send()
        return total

    def row(k):
        return slice(k, k + 1)

    def first_row(v):
        return row(PAIR * v)

    def second_row(v):
        return row(PAIR * v + 1)

    def put_stat(parity, v, cols, first, second):
        stat[parity, 0, zc, first_row(v), cols] = first
        stat[parity, 0, zc, second_row(v), cols] = second

    def local(src, dst):
        copy = pltpu.make_async_copy(src, dst, lsem.at[new_ids('l', 1)[0]])
        copy.start()
        return copy

    row0 = pl.multiple_of(core * half + xc * quad, quad)
    subs = range(PAIR)
    w1_loads = [local(w_one.at[pl.ds(row0 + s * blk, blk), :], wg1.at[zc, yc, xc, s]) for s in subs]
    hrow = pl.multiple_of(mid * rows, rows)
    h_ids = [new_ids('s', RING), new_ids('r', RING)]
    h_pairs = []
    for v, h_ref in enumerate((h_a, h_b)):
        for kh in subs:
            h_pairs.append((h_ref.at[pl.ds(hrow, rows), pl.ds(kh * half, half)],
                            hx.at[kh, pl.ds(pl.multiple_of(v * vrows + core * rows, rows), rows), :]))
    more_loads = [local(src, dst) for src, dst in h_pairs]
    more_loads.append(local(g_one, gbuf.at[zc, yc, row(0), :]))
    more_loads.append(local(b_one, gbuf.at[zc, yc, row(1), :]))
    for s in subs:
        more_loads.append(local(w_two.at[:, pl.ds(row0 + s * blk, blk)], wg2.at[zc, yc, xc, s]))
        more_loads.append(local(w_three.at[pl.ds(row0 + s * blk, blk), :], wg3.at[zc, yc, xc, s]))

    barrier = pltpu.get_barrier_semaphore()
    greeted = [device(axis, off) for axis in AXES for off in OTHERS] + [peer]
    for target in greeted:
        pl.semaphore_signal(barrier, inc=1, device_id=target, device_id_type=MESH_ID)
    pl.semaphore_wait(barrier, len(greeted))

    gather_width = 66
    send_a, send_b = new_ids('s', 90), new_ids('s', 90)
    gather_recv = [new_ids('r', gather_width) for _ in range(3)]
    scatter_recv = [new_ids('r', 90), gather_recv[1] + gather_recv[2][:24]]
    q_send, q_recv = new_ids('s', 8), new_ids('r', 8)

    for copy in w1_loads:
        copy.wait()
    lanes1 = gather_lanes(wg1, send_a, gather_recv[0])
    step(*lanes1)
    h_copies = [rcopy(src, dst, h_ids[0][k], h_ids[1][k], peer) for k, (src, dst) in enumerate(h_pairs)]
    for copy in h_copies:
        copy.start()
    for copy in more_loads:
        copy.wait()

    gb_recv = new_ids('r', 6)

    def gain_copies(k, axis, own):
        made = [rcopy(own, own, stat_send[k + off - 1], gb_recv[k + off - 1], device(axis, off)) for off in OTHERS]
        for copy in made:
            copy.start()
        return made

    gb_y = gain_copies(0, 'y', gbuf.at[zc, yc])
    lanes2 = gather_lanes(wg2, send_b, gather_recv[1])
    lanes3 = gather_lanes(wg3, send_a, gather_recv[2])
    step(*lanes1)
    for copy in gb_y:
        copy.wait_recv()
    gb_z = gain_copies(3, 'z', gbuf.at[zc])
    step(*lanes2)
    step(*lanes1)
    step(*lanes1)
    step(*lanes2)
    step(*lanes1)
    step(*lanes2)
    q1 = []
    for s in subs:
        finish(lanes1[s * 3:s * 3 + 3])
        q1.append(quarter(wg1, wq1, s, q_send[s], q_recv[s]))
    for copy in gb_z:
        copy.wait_recv()
    for copy in gb_y + gb_z:
        copy.wait_send()
    for copy in h_copies:
        copy.wait_recv()
    step(*lanes2[:3])
    for copy in q1:
        copy.wait_recv()

    def gathered(k):
        return lanes_of(gbuf[z, i, row(k), :] for z in (z_own, z_own + 1) for i in range(RING))

    gain1, shift1 = gathered(0), gathered(1)
    my_cols = pl.ds(pl.multiple_of(core * half, half), half)
    gain2, shift2 = g_two[:, my_cols], b_two[:, my_cols]
    for k, value in enumerate((gain1, shift1, gain2, shift2)):
        sres[3, row(k), :] = value

    def view_rows(v):
        return pl.ds(v * vrows, vrows)

    def chunk_cols(j):
        return pl.ds(pl.multiple_of(j * quad, quad), quad)

    def over_chunks(fn):
        pl.loop(0, RING)(fn)

    def forward_rowsplit(act, own, got, views, emit, ready):
        for v, src_v in views:
            ready[v]()

            def body(j):
                zz, y0 = lax.div(j, PAIR), lax.rem(j, PAIR) * PAIR
                sides = [lanes_of(ref[z, yy].reshape(half, blk) for yy in (y0, y0 + 1))
                         for ref, z in ((own, z_own + zz), (got, zz))]
                emit(j, v, dot_nn(act[core, view_rows(src_v), :], sides[0])
                     + dot_nn(act[other, view_rows(src_v), :], sides[1]))
            over_chunks(body)

    def forward_colsplit(act, own, emit, ready):
        for v in subs:
            ready[v]()

            def body(j):
                sides = [lanes_of(own[PAIR * hh:PAIR * hh + PAIR, :, j, s].reshape(half, blk) for s in subs)
                         for hh in subs]
                emit(j, v, dot_nn(act[0, view_rows(v), :], sides[0]) + dot_nn(act[1, view_rows(v), :], sides[1]))
            over_chunks(body)

    def backward_rowsplit(act, own, views, emit, ready):
        for v, src_v in views:
            ready[v]()

            def body(j):
                sides = [lanes_of(own[PAIR * hh + i // RING, i % RING, j].reshape(quad, blk) for i in range(8))
                         for hh in subs]
                emit(j, v, dot_nt(act[0, view_rows(src_v), :], sides[0])
                     + dot_nt(act[1, view_rows(src_v), :], sides[1]))
            over_chunks(body)

    def backward_colsplit(act, own, got, emit, ready):
        for v in subs:
            ready[v]()

            def body(j):
                sides = []
                zz, y0 = lax.div(j, PAIR), lax.rem(j, PAIR) * PAIR
                for ref, z in ((own, z_own + zz), (got, zz)):
                    bands = [lanes_of(ref[z, yy, t // PAIR, t % PAIR] for t in range(8)) for yy in (y0, y0 + 1)]
                    sides.append(jnp.concatenate(bands, axis=0))
                emit(j, v, dot_nt(act[core, view_rows(v), :], sides[0]) + dot_nt(act[other, view_rows(v), :], sides[1]))
            over_chunks(body)

    def partial_rowsplit(dst, lhs, lhs_rows, rhs, rhs_rows):
        def body(j):
            left = lhs[core, lhs_rows, chunk_cols(j)]
            for hh in subs:
                for t in range(RING):
                    res = dot_tn(left, rhs[hh, rhs_rows, t * quad:(t + 1) * quad])
                    for i in subs:
                        for s in subs:
                            dst[PAIR * hh + t // PAIR, (t % PAIR) * PAIR + i, j, s] = res[s * blk:(s + 1) * blk,
                                                                                         i * blk:(i + 1) * blk]
        over_chunks(body)

    def partial_colsplit(dst, lhs, rhs, hh):
        def body(t):
            left = lhs[hh, :, chunk_cols(t)]
            zz, y0 = PAIR * hh + lax.div(t, PAIR), lax.rem(t, PAIR) * PAIR
            for q in range(RING):
                res = dot_tn(left, rhs[core, :, q * quad:(q + 1) * quad])
                for i, yy in enumerate((y0, y0 + 1)):
                    for s in subs:
                        dst[zz, yy, q, s] = res[i * blk:(i + 1) * blk, s * blk:(s + 1) * blk]
        over_chunks(body)

    def forward_emit(dst, parity):
        def emit(j, v, acc):
            cols = chunk_cols(j)
            dst[view_rows(v), cols] = acc
            put_stat(parity, v, cols, col_sum(acc), col_sum(acc * acc))
        return emit

    def moments(total, slot):
        for v in subs:
            mean = total[first_row(v), 0:half] * inv_n
            inv = lax.rsqrt(total[second_row(v), 0:half] * inv_n - mean * mean + BN_EPS)
            sres[slot, first_row(v), :] = mean
            sres[slot, second_row(v), :] = inv

    act_send, act_recv = new_ids('s', PAIR), new_ids('r', 10)

    def share(dst, v):
        region = dst.at[core, view_rows(v), :]
        copy = rcopy(region, region, act_send[v], act_recv.pop(), peer)
        copy.start()
        return copy

    rstep = min(32, vrows)

    def apply_rows(v, fn):
        @pl.loop(0, vrows // rstep)
        def _(i):
            fn(pl.ds(pl.multiple_of(v * vrows + i * rstep, rstep), rstep))

    def activate(src, slot, gain, shift, dst):
        copies = []
        for v in subs:
            mean = sres[slot, first_row(v), :]
            inv = sres[slot, second_row(v), :]

            def fn(rsl, mean=mean, inv=inv):
                norm = (src[rsl, :] - mean) * inv
                if gain is not None:
                    norm = jnp.maximum(gain * norm + shift, 0.0)
                dst[core, rsl, :] = norm.astype(BF16)
            apply_rows(v, fn)
            copies.append(share(dst, v))
        return copies

    def received(copies):
        return [copy.wait_recv for copy in copies]

    def sent(copies):
        for copy in copies:
            copy.wait_send()

    def nothing():
        pass

    both = ((0, 0), (1, 1))
    at_once = (nothing, nothing)
    all_rows = pl.ds(0, PAIR * vrows)

    forward_rowsplit(hx, wg1, wq1, both, forward_emit(u1, 0), at_once)
    sub0, sub1 = lanes2[:3], lanes2[3:]
    moments(stat_sum(0, half, (sub0, (sub1[0], sub1[1]), (sub1[2],))), 0)
    copies = activate(u1, 0, gain1, shift1, xf1)
    sent(q1 + h_copies)
    finish(lanes2)
    q2 = [quarter(wg2, wq2, s, q_send[PAIR + s], q_recv[PAIR + s]) for s in subs]
    step(*lanes3)
    forward_colsplit(xf1, wg2, forward_emit(u2, 1), received(copies))
    sent(copies)
    step(*lanes3)
    sub0, sub1 = lanes3[:3], lanes3[3:]
    moments(stat_sum(1, half, (lanes3, sub0, (sub1[0], sub1[1]))), 1)
    copies = activate(u2, 1, gain2, shift2, xf2)
    step(sub1[2])
    q3 = []
    for s, group in enumerate((sub0, sub1)):
        finish(group)
        q3.append(quarter(wg3, wq1, s, q_send[RING + s], q_recv[RING + s]))
    for copy in q3:
        copy.wait_recv()
    forward_rowsplit(xf2, wg3, wq1, both, forward_emit(u3, 0), received(copies))
    sent(copies)
    moments(stat_sum(0, half), PAIR)
    copies = activate(u3, PAIR, None, None, zf)
    for copy in copies:
        copy.wait_recv()
    sent(copies)

    partial_rowsplit(part, zf, view_rows(0), zf, view_rows(1))
    lanes_c = scatter_lanes(part, 0, send_a, scatter_recv[0])
    lanes_g = gather_lanes(wg1, send_b, gather_recv[0])
    lam = lam_ref[0]
    col_ids = mid * blk + lax.broadcasted_iota(jnp.int32, (blk, blk), 1)

    def gradient_piece(s):
        corr = part[zc, yc, xc, s] * inv_n
        row_ids = core * half + xc * quad + s * blk + lax.broadcasted_iota(jnp.int32, (blk, blk), 0)
        diag = row_ids == col_ids
        terms = jnp.where(diag, (1.0 - corr) * (1.0 - corr), lam * corr * corr)
        wg1[zc, yc, xc, s] = jnp.where(diag, -2.0 * (1.0 - corr), 2.0 * lam * corr).astype(BF16)
        return jnp.sum(jnp.sum(terms, axis=0, keepdims=True), axis=1, keepdims=True)

    ca, cb = lanes_c[:3], lanes_c[3:]
    for group in (ca, ca, cb, ca, cb, cb, ca, ca, cb, ca, cb):
        step(*group)
    finish(ca)
    loss_part = gradient_piece(0)
    ga, gb = lanes_g[:3], lanes_g[3:]
    step(*ga)
    step(*cb)
    finish(cb)
    loss_part = loss_part + gradient_piece(1)
    for group in (gb, ga, ga, gb, ga, gb, ga, gb):
        step(*group)
    finish(ga)
    qg = [quarter(wg1, wq1, 0, q_send[6], q_recv[6])]
    finish(gb)
    qg.append(quarter(wg1, wq1, 1, q_send[7], q_recv[7]))

    def embed_emit(j, v, acc):
        cols = chunk_cols(j)
        grad = acc * inv_n
        u3[view_rows(v), cols] = grad
        put_stat(1, v, cols, col_sum(grad), col_sum(grad * zf[core, view_rows(v), cols].astype(F32)))

    backward_rowsplit(zf, wg1, ((0, 1),), embed_emit, at_once)
    for copy in qg:
        copy.wait_recv()
    forward_rowsplit(zf, wg1, wq1, ((1, 0),), embed_emit, at_once)
    dzf, duf = hx, zf
    stat[1, 0, zc, :, half:half + blk] = jnp.broadcast_to(loss_part, (RING, blk))
    total = stat_sum(1, half + blk)
    dgb[core, :, half:half + blk] = total[:, half:half + blk]
    copies = []
    for v in subs:
        def embed_rows(rsl, mean_g=total[first_row(v), 0:half], mean_gz=total[second_row(v), 0:half],
                       inv=sres[PAIR, second_row(v), :]):
            emb = zf[core, rsl, :].astype(F32)
            dzf[core, rsl, :] = (inv * (u3[rsl, :] - (mean_g + emb * mean_gz) * inv_n)).astype(BF16)
        apply_rows(v, embed_rows)
        copies.append(share(dzf, v))
    for copy in copies:
        copy.wait_recv()
    sent(copies + q2 + q3 + qg)

    out_recv = new_ids('r', 15)
    out_send = new_ids('s', 15)

    def publish(slot):
        up, down = device('x', 1), device('x', 3)
        sid, rid = out_send[slot * 5:slot * 5 + 5], out_recv[slot * 5:slot * 5 + 5]
        own = out_w.at[slot, core, xc]
        made = [rcopy(own, own, sid[0], rid[0], up), rcopy(own, own, sid[1], rid[1], down)]
        for copy in made:
            copy.start()
        yield
        for k, (off, target) in enumerate(((3, up), (1, down))):
            made[k].wait_recv()
            src = out_w.at[slot, core, near['x'][off], k]
            made.append(rcopy(src, src, sid[PAIR + k], rid[PAIR + k], target))
            made[-1].start()
        yield
        made[2].wait_recv()
        made[3].wait_recv()
        own = out_w.at[slot, core]
        made.append(rcopy(own, own, sid[RING], rid[RING], peer))
        made[-1].start()
        yield
        made[-1].wait_recv()
        sent(made)

    def result(slot, buf, group):
        finish(group)
        out_w[slot, core, xc] = buf[zc, yc, xc]
        yield
        yield from publish(slot)

    def layer_emit(src, slot, parity, k):
        def emit(j, v, acc):
            cols = chunk_cols(j)
            norm = (src[view_rows(v), cols] - sres[slot, first_row(v), cols]) * sres[slot, second_row(v), cols]
            lin = sres[3, row(k), cols] * norm + sres[3, row(k + 1), cols]
            grad = jnp.where(lin > 0, acc, 0.0)
            u3[view_rows(v), cols] = grad
            put_stat(parity, v, cols, col_sum(grad), col_sum(grad * norm))
        return emit

    def layer_rows(src, slot, k, total, v, store):
        sum_lin, sum_norm = total[first_row(v), 0:half], total[second_row(v), 0:half]
        mean, inv = sres[slot, first_row(v), :], sres[slot, second_row(v), :]
        scale = sres[3, row(k), :] * inv

        def fn(rsl):
            norm = (src[rsl, :] - mean) * inv
            store(rsl, (scale * (u3[rsl, :] - (sum_lin + norm * sum_norm) * inv_n)).astype(BF16))
        apply_rows(v, fn)

    def affine_grads(total, k):
        dgb[core, row(k), 0:half] = total[second_row(0), 0:half] + total[second_row(1), 0:half]
        dgb[core, row(k + 1), 0:half] = total[first_row(0), 0:half] + total[first_row(1), 0:half]

    lanes_3 = scatter_lanes(part, 0, send_a, scatter_recv[0], give=True)
    lanes_2 = scatter_lanes(part2, 1, send_b, scatter_recv[1], take=True)
    a3, b3 = lanes_3[:3], lanes_3[3:]
    a2, b2 = lanes_2[:3], lanes_2[3:]

    partial_rowsplit(part, xf2, all_rows, dzf, all_rows)
    step(*a3)
    step(*a3)
    backward_rowsplit(dzf, wg3, both, layer_emit(u2, 1, 0, PAIR), at_once)
    total = stat_sum(0, half, (a3, b3, b3))
    affine_grads(total, 0)
    copies = []
    for v in subs:
        def put_du2(rsl, value):
            duf[core, rsl, :] = value
        layer_rows(u2, 1, PAIR, total, v, put_du2)
        copies.append(share(duf, v))
    step(*b3)
    step(*a3)
    for copy in q2:
        copy.wait_recv()
    backward_colsplit(duf, wg2, wq2, layer_emit(u1, 0, 1, 0), received(copies))
    sent(copies)
    step(*a3)

    def later(fn, *args):
        fn(*args)
        yield

    total = stat_sum(1, half, ((*b3, later(partial_colsplit, part2, xf1, duf, 0)),
                               (*a3, *b3, later(partial_colsplit, part2, xf1, duf, 1)),
                               (*a2,)))
    affine_grads(total, PAIR)
    dg_send, dg_recv = new_ids('s', 1)[0], new_ids('r', 1)[0]
    dg_copy = rcopy(dgb.at[core], dgb.at[core], dg_send, dg_recv, peer)
    dg_copy.start()

    for v in subs:
        def put_du1(rsl, value, v=v):
            start = rsl.start - v * vrows
            r = pl.multiple_of(lax.rem(start, rows), min(rstep, rows))
            c = lax.div(start, rows)
            for i in range(8):
                du1[i // RING, i % RING, c, v, pl.ds(r, rstep), :] = value[:, i * blk:(i + 1) * blk]
        layer_rows(u1, 0, 0, total, v, put_du1)

    a2a_recv, a2a_send = new_ids('r', 16), new_ids('s', 16)
    targets = [(i // RING, i % RING, c) for i in range(8) for c in subs]

    own_half = lax.div(mid, 8)
    self_out = jnp.where(own_half == core, PAIR * (mid - 8 * core) + core, -1)
    self_in = jnp.where(own_half == core, mid, -1)
    a2a_home, a2a_sem = a2a.at[zc, yc], rsem.at[a2a_recv[0] + mid]

    for k, (zi, yy, c) in enumerate(targets):
        src = du1.at[zi, yy, c]

        @pl.when(self_out == k)
        def _():
            a2a_home[...] = src[...]

        @pl.when(self_out != k)
        def _():
            pltpu.make_async_remote_copy(
                src_ref=src, dst_ref=a2a_home, send_sem=ssem.at[a2a_send[k]], recv_sem=a2a_sem,
                device_id=(8 * core + zi * RING + yy, x_base + c), device_id_type=MESH_ID).start()

    slots = (hx, zf, xf1, xf2)
    per = RING * rows

    def h_fetch(chunk):
        at = chunk % RING
        made = [pltpu.make_async_copy((h_a, h_b)[chunk // RING].at[pl.ds(at * per, per), pl.ds(kh * half, half)],
                                      slots[at].at[kh], hsem.at[at * PAIR + kh]) for kh in subs]
        for copy in made:
            copy.start()
        return made

    fetches = [h_fetch(chunk) for chunk in range(RING)]
    step(*a2)
    step(*b2)
    for i in range(16):
        @pl.when(self_in != i)
        def _():
            pltpu.make_async_copy(a2a.at[i // RING, i % RING], a2a.at[i // RING, i % RING],
                                  rsem.at[a2a_recv[i]]).wait()
    step(*a2)
    step(*b2)
    for chunk in range(8):
        v, at = chunk // RING, chunk % RING
        for copy in fetches[chunk]:
            copy.wait()
        grad = jnp.concatenate([a2a[at, i, v] for i in range(RING)], axis=0)
        for kh in subs:
            for q in range(RING):
                res = dot_tn(grad, slots[at][kh, :, q * quad:(q + 1) * quad])
                spot = (slice(kh * blk, (kh + 1) * blk), slice(q * quad, (q + 1) * quad))
                u2[spot] = res + u2[spot] if chunk else res
        if chunk < RING:
            fetches.append(h_fetch(chunk + RING))
    for k, (zi, yy, c) in enumerate(targets):
        @pl.when(self_out != k)
        def _():
            pltpu.make_async_copy(du1.at[zi, yy, c], du1.at[zi, yy, c], ssem.at[a2a_send[k]]).wait()

    x_recv, x_send = new_ids('r', RING), new_ids('s', RING)
    def strip(k, cols=pl.ds(0, half)):
        return u2.at[pl.ds(pl.multiple_of(k * blk, blk), blk), cols]

    swap = rcopy(strip(other), strip(PAIR), x_send[0], x_recv[0], peer)
    swap.start()
    step(*b2)
    step(*a2)
    pub3 = result(2, part, a3 + b3)
    step(pub3)
    swap.wait_recv()
    swap.wait_send()
    strip(core)[...] = strip(core)[...] + strip(PAIR)[...]
    shifts = [rcopy(strip(core, chunk_cols(near['x'][off])), strip(3, chunk_cols(off)), x_send[off], x_recv[off],
                    device('x', off)) for off in OTHERS]
    for copy in shifts:
        copy.start()
    step(pub3)
    step(*b2)
    step(*a2)
    for copy in shifts:
        copy.wait_recv()
    got = [strip(3, chunk_cols(off))[...] for off in OTHERS]
    piece_sum = (strip(core, chunk_cols(xc))[...] + got[0]) + (got[1] + got[2])
    for s in subs:
        out_w[0, core, xc, s] = piece_sum[:, s * blk:(s + 1) * blk].T
    sent(shifts)
    pub1 = publish(0)
    step(pub1)
    step(pub3)
    step(*b2)
    step(*a2)
    step(pub1)
    step(*b2)
    step(pub1)
    pub2 = result(1, part2, a2 + b2)
    finish([pub3, pub1, pub2])
    dg_copy.wait_recv()
    dg_copy.wait_send()
    w_copy = pltpu.make_async_copy(out_w, dw_out, lsem.at[0])
    w_copy.start()
    small_out[...] = dgb[...]
    w_copy.wait()


def split_kernel(blk, dw_ref, small_ref, loss_out, dw1_out, dw2_out, dw3_out, dg1_out, db1_out, dg2_out, db2_out,
                 stage, sem_in, sem_out):
    half = 8 * blk
    mid = lax.axis_index('model')
    loads = []
    for slot in range(3):
        loads.append(pltpu.make_async_copy(dw_ref.at[slot], stage.at[slot], sem_in.at[slot]))
        loads[-1].start()
    loss_out[...] = small_ref[0, 0:1, half:half + 1] + small_ref[1, 0:1, half:half + 1]
    for hh in range(PAIR):
        dg2_out[:, hh * half:(hh + 1) * half] = small_ref[hh, 0:1, 0:half]
        db2_out[:, hh * half:(hh + 1) * half] = small_ref[hh, 1:2, 0:half]
    mcols = pl.ds(pl.multiple_of(lax.rem(mid, 8) * blk, blk), blk)
    dg1_out[...] = small_ref[lax.div(mid, 8), 2:3, mcols]
    db1_out[...] = small_ref[lax.div(mid, 8), 3:4, mcols]
    stores = []
    for slot in range(3):
        loads[slot].wait()
        for t in range(16):
            begin = pl.ds(t * blk, blk)
            dst = (dw1_out.at[begin, :], dw2_out.at[:, begin], dw3_out.at[begin, :])[slot]
            stores.append(pltpu.make_async_copy(stage.at[slot, t // 8, (t // PAIR) % RING, t % PAIR], dst,
                                                sem_out.at[len(stores)]))
            stores[-1].start()
    for copy in stores:
        copy.wait()


def build_call(blk, rows, total_rows, splits, vmem_limit):
    dim, half = 16 * blk, 8 * blk
    trows = RING * rows
    pieces = (RING, RING, RING, PAIR, blk, blk)
    got = (PAIR, RING, RING, PAIR, blk, blk)
    act = pltpu.VMEM((PAIR, trows, half), BF16)
    pre = pltpu.VMEM((trows, half), F32)
    bank = (PAIR, RING, PAIR, blk, blk)
    dma = pltpu.SemaphoreType.DMA
    scratch = [
        act, pre, pre, pre, act, act, act,
        pltpu.VMEM(pieces, BF16), pltpu.VMEM(got, BF16), pltpu.VMEM(pieces, BF16), pltpu.VMEM(got, BF16),
        pltpu.VMEM(pieces, BF16),
        pltpu.VMEM(pieces, F32), pltpu.VMEM(pieces, F32),
        pltpu.VMEM((PAIR, 6, RING, PAIR, blk, blk), F32), pltpu.VMEM((PAIR, PAIR, 6, PAIR, blk, blk), F32),
        pltpu.VMEM((PAIR, PAIR, 3, blk, blk), F32),
        pltpu.VMEM((RING, RING, 8, blk), F32),
        pltpu.VMEM((PAIR, 3, RING, RING, half + blk), F32), pltpu.VMEM((RING, RING, half), F32),
        pltpu.VMEM((PAIR, RING, half + blk), F32),
        pltpu.VMEM((PAIR, RING, PAIR, PAIR, rows, blk), BF16), pltpu.VMEM((RING, RING, PAIR, rows, blk), BF16),
        pltpu.VMEM((3,) + bank, F32),
        dma((N_SEND,)), dma((N_RECV,)), dma((16,)), dma((8,)), pltpu.SemaphoreType.REGULAR((8,)),
    ]
    anyspec = pl.BlockSpec(memory_space=pl.ANY)
    vmem = pl.BlockSpec(memory_space=pltpu.VMEM)
    smem = pl.BlockSpec(memory_space=pltpu.SMEM)
    packed = jax.ShapeDtypeStruct((3,) + bank, F32)
    step_call = pl.pallas_call(
        functools.partial(mega_kernel, (blk, rows, total_rows, splits)),
        out_shape=[packed, jax.ShapeDtypeStruct((PAIR, RING, half + blk), F32)],
        in_specs=[anyspec] * 7 + [vmem, vmem, smem],
        out_specs=[anyspec, vmem],
        scratch_shapes=scratch,
        compiler_params=pltpu.CompilerParams(collective_id=0, has_side_effects=True, vmem_limit_bytes=vmem_limit),
        name='barlow_step',
    )

    def line(n):
        return jax.ShapeDtypeStruct((1, n), F32)

    tall, wide = jax.ShapeDtypeStruct((dim, blk), F32), jax.ShapeDtypeStruct((blk, dim), F32)
    split_call = pl.pallas_call(
        functools.partial(split_kernel, blk),
        out_shape=[line(1), tall, wide, tall, line(blk), line(blk), line(dim), line(dim)],
        in_specs=[anyspec, vmem],
        out_specs=[vmem, anyspec, anyspec, anyspec, vmem, vmem, vmem, vmem],
        scratch_shapes=[pltpu.VMEM((3,) + bank, F32), dma((3,)), dma((48,))],
        name='split_results',
    )

    def call(*args):
        return split_call(*step_call(*args))

    return call


def solution(mesh):
    data_size = mesh.shape['data']

    def shard_body(h_a, h_b, w_one, w_two, w_three, g_one, b_one, g_two, b_two, lam_off):
        group_rows = h_a.shape[0]
        blk = w_three.shape[1]
        rows = group_rows // 16
        splits = ((40, 48, 40), (48, 40, 40))
        call = build_call(blk, rows, group_rows * data_size, splits, 67_000_000)
        outs = call(h_a, h_b, w_one, w_two, w_three, g_one.reshape(1, -1), b_one.reshape(1, -1),
                    g_two.reshape(1, -1), b_two.reshape(1, -1), lam_off)
        loss, dw1, dw2, dw3, dg1, db1, dg2, db2 = outs
        return (loss.reshape(1), dw1, dw2, dw3, dg1.reshape(-1), db1.reshape(-1), dg2.reshape(-1), db2.reshape(-1))

    in_specs = (P('data', None), P('data', None), P(None, 'model'), P('model', None), P(None, 'model'),
                P('model'), P('model'), P(), P(), P())
    out_specs = (P(), P(None, 'model'), P('model', None), P(None, 'model'), P('model'), P('model'), P(), P())
    return jax.shard_map(shard_body, mesh=mesh, in_specs=in_specs, out_specs=out_specs, check_vma=False)
```

```python
import functools

import jax
import jax.numpy as jnp
from jax import lax
from jax.experimental import pallas as pl
from jax.experimental.pallas import tpu as pltpu
from jax.sharding import PartitionSpec as P

BN_EPS = 1e-5
MESH_ID = pl.DeviceIdType.MESH
RING = 4
PAIR = 2
AXES = ('z', 'y', 'x')
ORDERS = (('x', 'y', 'z'), ('y', 'z', 'x'), ('z', 'x', 'y'))
COARSE = ((0, 0, (40, 48, 40)), (1, 0, (48, 40, 40)))
FINE = COARSE
MERGED = ((slice(PAIR), 0, (40, 48, 40)),)
BACK = COARSE
OTHERS = (1, 2, 3)
N_SEND = 520
N_RECV = 520
BYTES_PER_US = 46600.0
HOP = 1.9
TWO_HOPS = 2.7
BACKLOG = 5.0
SMALL = 60000
FAR = 1e9
F32 = jnp.float32
BF16 = jnp.bfloat16
WHOLE = slice(None)
FIRST, SECOND = 0, 1
BLOCKS, HALF_BLOCKS = 16, 8
NOW = 0.0
STEP = 0.2
STAT_SIZE = 32768


def dot_nn(a, b):
    return lax.dot_general(a, b, (((1,), (0,)), ((), ())), preferred_element_type=F32)


def dot_nt(a, b):
    return lax.dot_general(a, b, (((1,), (1,)), ((), ())), preferred_element_type=F32)


def dot_tn(a, b):
    return lax.dot_general(a, b, (((0,), (0,)), ((), ())), preferred_element_type=F32)


def col_sum(value):
    return jnp.sum(value, axis=0, keepdims=True)


def lanes_of(values):
    return jnp.concatenate(list(values), axis=1)


def wrap(value):
    return lax.rem(value, RING)


class Plan:
    def __init__(self):
        self.now = 0.0
        self.free = dict.fromkeys(AXES, 0.0)
        self.need = dict.fromkeys(AXES, FAR)
        self.lanes = []
        self.first = None

    def work(self, us):
        self.now += us

    def until(self, when):
        self.now = max(self.now, when)

    def send(self, axis, size, flight=HOP):
        self.free[axis] = max(self.free[axis], self.now) + size / BYTES_PER_US
        return self.free[axis] + flight

    def add(self, gens, then=None, first=False):
        group = {'left': 0, 'then': then}
        made = []
        for gen in gens:
            group['left'] += 1
            made.append([gen, next(gen), group])
        self.lanes = made + self.lanes if first else self.lanes + made
        return group

    def start_of(self, lane):
        ready, loads, _ = lane[1]
        start = max(self.now, ready() if callable(ready) else ready)
        if self.first is not None and lane[2] not in self.first and max(loads.values(), default=0) > SMALL:
            return FAR
        for axis, size in loads.items():
            start = max(start, self.free[axis] - BACKLOG)
        for axis, size in loads.items():
            if max(self.free[axis], start) + size / BYTES_PER_US > self.need[axis] + 1.0:
                return FAR
        return start

    def advance(self, limit):
        best, begin = None, limit
        for lane in self.lanes:
            start = self.start_of(lane)
            if start < begin and start + lane[1][2] < limit + 1.0:
                best, begin = lane, start
        if best is None:
            return False
        self.until(begin)
        info = next(best[0], None)
        if info is not None:
            best[1] = info
            return True
        self.lanes = [lane for lane in self.lanes if lane is not best]
        group = best[2]
        group['left'] -= 1
        if not group['left'] and group['then'] is not None:
            group['then']()
        return True

    def pump(self, limit):
        while self.advance(limit):
            pass

    def finish(self, *groups, alone=False):
        self.first = groups if alone else None
        while any(group['left'] for group in groups):
            if not self.advance(FAR):
                self.need = dict.fromkeys(AXES, FAR)
        self.first = None

    def expect(self, when):
        for axis in AXES:
            self.need[axis] = when
            when += 3.6


def mega_kernel(cfg, h_a, h_b, w_one, w_two, w_three, g_one, b_one, g_two, b_two, lam_ref,
                dw_out, small_out,
                hx, u1, u2, u3, xf1, xf2, zf, wg1, wq1, wg2, wq2, wg3, part, part2, rv1, rv2, rv3,
                gbuf, stat, sres, dgb, zsum, vec, vecx, vecp, du1, a2a, out_w, ssem, rsem, lsem, hsem, credit):
    blk, rows, total_rows = cfg
    plan = Plan()
    half = HALF_BLOCKS * blk
    quad = PAIR * blk
    vrows = PAIR * rows
    inv_n = 1.0 / total_rows

    mid = lax.axis_index('model')
    did = lax.axis_index('data')
    core = lax.rem(did, PAIR)
    other = 1 - core
    coord = {'z': lax.div(mid, RING), 'y': wrap(mid), 'x': lax.div(did, PAIR)}
    zc, yc, xc = coord['z'], coord['y'], coord['x']
    near = {axis: [coord[axis]] + [wrap(coord[axis] + off) for off in OTHERS] for axis in AXES}
    z_base, x_base = zc * RING, xc * PAIR
    targets_of = {'z': [(q * RING + yc, did) for q in near['z']], 'y': [(z_base + q, did) for q in near['y']],
                  'x': [(mid, q * PAIR + core) for q in near['x']]}
    peer = (mid, x_base + other)

    def device(axis, off):
        return targets_of[axis][off]

    z_own, z_other = PAIR * core, PAIR * other
    counters = {'s': 0, 'r': 0, 'l': 0}

    def new_ids(kind, count):
        first = counters[kind]
        counters[kind] = first + count
        assert counters[kind] <= {'s': N_SEND, 'r': N_RECV, 'l': BLOCKS}[kind]
        return list(range(first, first + count))

    def rcopy(src, dst, send_id, recv_id, target):
        return pltpu.make_async_remote_copy(src_ref=src, dst_ref=dst, send_sem=ssem.at[send_id],
                                            recv_sem=rsem.at[recv_id], device_id=target, device_id_type=MESH_ID)

    def bands(batches):
        for sub, begin, sizes in batches:
            for colour, size in enumerate(sizes):
                yield sub, colour, pl.ds(begin, size), size * blk * (PAIR if isinstance(sub, slice) else 1)
                begin += size

    def gather_lane(buf, sub, colour, rsl, cells, sid, rid):
        order = ORDERS[colour]
        size = PAIR * cells

        def region(axis, have, q, part_id=None):
            idx = dict(coord)
            idx[axis] = q
            for name in have:
                idx[name] = WHOLE
            if part_id is not None:
                idx[have[-1]] = pl.ds(PAIR * part_id, PAIR)
            return buf.at[idx['z'], idx['y'], idx['x'], sub, rsl, :]

        axis = order[0]
        yield NOW, {axis: PAIR * size}, NOW
        own = region(axis, (), coord[axis])
        pending = [rcopy(own, own, sid[off - 1], rid[off - 1], device(axis, off)) for off in OTHERS]
        for copy in pending:
            copy.start()
        ready = plan.send(axis, PAIR * size, TWO_HOPS)
        for phase in (1, 2):
            size *= RING
            axis, have = order[phase], order[:phase]
            yield ready, {axis: size}, STEP
            for copy in pending[-3:] if phase == 1 else pending[-2:]:
                copy.wait_recv()
            base = phase * RING - 1
            up, down = device(axis, 1), device(axis, 3)
            own = region(axis, have, coord[axis])
            to_up = rcopy(own, own, sid[base], rid[base], up)
            to_down = rcopy(own, own, sid[base + 1], rid[base + 1], down)
            to_up.start()
            to_down.start()
            yield plan.send(axis, size), {axis: size / PAIR}, STEP
            to_up.wait_recv()
            src = region(axis, have, near[axis][3], 0)
            relay_up = rcopy(src, src, sid[base + 2], rid[base + 2], up)
            relay_up.start()
            to_down.wait_recv()
            src = region(axis, have, near[axis][1], 1)
            relay_down = rcopy(src, src, sid[base + 3], rid[base + 3], down)
            relay_down.start()
            ready = plan.send(axis, size / PAIR)
            pending.extend((to_up, to_down, relay_up, relay_down))
        yield ready, {}, STEP
        for copy in pending[-2:]:
            copy.wait_recv()
        for copy in pending:
            copy.wait_send()

    def lanes_by_batch(make, batches, send_ids, recv_ids, width):
        lanes = []
        for k, found in enumerate(bands(batches)):
            ids = slice(k * width, (k + 1) * width)
            lanes.append(make(k, *found, send_ids[ids], recv_ids[ids]))
        return [lanes[k:k + 3] for k in range(0, len(lanes), 3)]

    def gather_lanes(buf, batches, send_ids, recv_ids):
        return lanes_by_batch(lambda k, *args: gather_lane(buf, *args), batches, send_ids, recv_ids, 11)

    given = {}

    def scatter_lane(buf, bank, give, take, sub, colour, rsl, cells, sid, rid):
        order = ORDERS[colour]
        pending = []
        ready = NOW
        size = cells * 32
        for phase in (0, 1):
            axis = order[phase]
            left = tuple(name for name in AXES if name in order[phase + 1:])
            p = coord[axis]
            base = phase * 6

            def region(q, part_id, axis=axis, left=left):
                idx = dict(coord)
                idx[axis] = q
                for name in left[:-1]:
                    idx[name] = WHOLE
                idx[left[-1]] = pl.ds(PAIR * part_id, PAIR)
                return buf.at[idx['z'], idx['y'], idx['x'], sub, rsl, :]

            def landing(slot, phase=phase):
                if phase:
                    return rv2.at[bank, sub, slot, :, rsl, :]
                return rv1.at[sub, slot, :, :, rsl, :]

            def add(q, part_id, slots, axis=axis, left=left, phase=phase):
                def one(i, j):
                    idx = dict(coord)
                    idx[axis] = q
                    idx[left[-1]] = PAIR * part_id + j
                    if not phase:
                        idx[left[0]] = i
                    total = buf[idx['z'], idx['y'], idx['x'], sub, rsl, :]
                    for slot in slots:
                        total = total + (rv2[bank, sub, slot, j, rsl, :] if phase else rv1[sub, slot, i, j, rsl, :])
                    buf[idx['z'], idx['y'], idx['x'], sub, rsl, :] = total

                if phase:
                    for j in range(PAIR):
                        one(0, j)
                else:
                    @pl.loop(0, RING)
                    def _(i):
                        for j in range(PAIR):
                            one(i, j)

            up, down = device(axis, 1), device(axis, 3)
            p1, p2, p3 = near[axis][1:]
            if phase:
                yield ready, {axis: PAIR * size}, STEP
                finals()
            else:
                yield (ready if take is None else lambda: given.get(take, FAR)), {axis: size}, NOW
                if take is not None:
                    pl.semaphore_wait(credit.at[take], PAIR)
            relay_up = rcopy(region(p2, 1), landing(0), sid[base], rid[base], up)
            relay_down = rcopy(region(p2, 0), landing(1), sid[base + 1], rid[base + 1], down)
            own_up = rcopy(region(p1, 0), landing(2), sid[base + 2], rid[base + 2], up)
            own_down = rcopy(region(p3, 1), landing(3), sid[base + 3], rid[base + 3], down)
            relay_up.start()
            relay_down.start()
            relayed = plan.send(axis, size)
            if not phase:
                yield NOW, {axis: size}, NOW
            own_up.start()
            own_down.start()
            plan.send(axis, size)
            yield relayed, {axis: size}, STEP
            relay_up.wait_recv()
            add(p1, 1, (0,))
            sum_up = rcopy(region(p1, 1), landing(4), sid[base + 4], rid[base + 4], up)
            sum_up.start()
            relay_down.wait_recv()
            add(p3, 0, (1,))
            sum_down = rcopy(region(p3, 0), landing(5), sid[base + 5], rid[base + 5], down)
            sum_down.start()
            ready = plan.send(axis, size)
            size /= RING

            def finals(phase=phase, p=p, add=add, own_up=own_up, own_down=own_down, sum_up=sum_up, sum_down=sum_down,
                       up=up, down=down):
                own_up.wait_recv()
                sum_down.wait_recv()
                add(p, 0, (2, 5))
                own_down.wait_recv()
                sum_up.wait_recv()
                add(p, 1, (3, 4))
                if give is not None and not phase:
                    given[give] = plan.now + 1.0
                    for target in (up, down):
                        pl.semaphore_signal(credit.at[give], device_id=target, device_id_type=MESH_ID)

            pending.extend((relay_up, relay_down, own_up, own_down, sum_up, sum_down))
        axis = order[2]
        size *= RING
        yield ready, {axis: size}, STEP
        finals()
        base = 12
        last = []
        for k, off in enumerate(OTHERS):
            idx = dict(coord)
            idx[axis] = near[axis][off]
            last.append(rcopy(buf.at[idx['z'], idx['y'], idx['x'], sub, rsl, :], rv3.at[bank, sub, k, rsl, :],
                              sid[base + k], rid[base + k], device(axis, off)))
        for copy in last:
            copy.start()
        yield plan.send(axis, size, TWO_HOPS), {}, STEP
        for copy in last:
            copy.wait_recv()
        got = [rv3[bank, sub, k, rsl, :] for k in range(3)]
        buf[zc, yc, xc, sub, rsl, :] = (buf[zc, yc, xc, sub, rsl, :] + got[0]) + (got[1] + got[2])
        for copy in pending + last:
            copy.wait_send()

    def scatter_lanes(buf, bank, batches, send_ids, recv_ids, give=False, take=False):
        return lanes_by_batch(lambda k, *args: scatter_lane(buf, bank, k if give else None, k if take else None, *args),
                              batches, send_ids, recv_ids, 15)

    released = []

    def quarter(src, dst, batch, send_id, recv_id, made, held=None):
        sub, begin, sizes = batch
        rsl = pl.ds(begin, sum(sizes))

        def send():
            if held is not None and not released:
                held.append(send)
                return
            copy = rcopy(src.at[pl.ds(z_other, PAIR), :, :, sub, rsl, :], dst.at[:, :, :, sub, rsl, :], send_id, recv_id,
                         peer)
            copy.start()
            made.append(copy)
        return send

    stat_recv = [new_ids('r', 9) for _ in range(PAIR)]
    stat_send = new_ids('s', 9)

    def stat_steps(parity, out):
        pending, ready, width = [], NOW, slice(half)
        for d, axis in enumerate(AXES):
            yield ready, {axis: STAT_SIZE}, STEP
            if d:
                stat[parity, d, coord[axis], :, width] = gathered_stat(parity, d - 1, pending)
            own = stat.at[parity, d, coord[axis], :, width]
            copies = [rcopy(own, own, stat_send[d * 3 + off - 1], stat_recv[parity][d * 3 + off - 1], device(axis, off))
                      for off in OTHERS]
            for copy in copies:
                copy.start()
            pending.extend(copies)
            ready = plan.send(axis, STAT_SIZE, TWO_HOPS)
        yield ready, {}, STEP
        out.append(gathered_stat(parity, d, pending))
        for copy in pending:
            copy.wait_send()

    def gathered_stat(parity, d, pending):
        for copy in pending[-3:]:
            copy.wait_recv()
        got = [stat[parity, d, q, :, :half] for q in range(RING)]
        return (got[0] + got[1]) + (got[PAIR] + got[3])

    def stat_sum(parity):
        out = []
        steps = stat_steps(parity, out)
        next(steps)
        plan.expect(plan.now)
        for axis in AXES:
            ready = next(steps)[0]
            plan.need[axis] = FAR
            plan.pump(ready)
            plan.until(ready)
            plan.work(STEP)
        next(steps, None)
        return out[0]

    def row(k):
        return slice(k, k + 1)

    def first_row(v):
        return row(PAIR * v)

    def second_row(v):
        return row(PAIR * v + 1)

    def put_stat(parity, v, cols, first, second):
        stat[parity, 0, zc, first_row(v), cols] = first
        stat[parity, 0, zc, second_row(v), cols] = second

    def local(src, dst):
        copy = pltpu.make_async_copy(src, dst, lsem.at[new_ids('l', 1)[0]])
        copy.start()
        return copy

    row0 = pl.multiple_of(core * half + xc * quad, quad)
    subs = range(PAIR)
    w1_loads = [local(w_one.at[pl.ds(row0 + s * blk, blk), :], wg1.at[zc, yc, xc, s]) for s in subs]
    hrow = pl.multiple_of(mid * rows, rows)
    h_ids = [new_ids('s', RING), new_ids('r', RING)]
    h_pairs = []
    for v, h_ref in enumerate((h_a, h_b)):
        for kh in subs:
            h_pairs.append((h_ref.at[pl.ds(hrow, rows), pl.ds(kh * half, half)],
                            hx.at[kh, pl.ds(pl.multiple_of(v * vrows + core * rows, rows), rows), :]))
    more_loads = [local(src, dst) for src, dst in h_pairs]
    more_loads.append(local(g_one, gbuf.at[zc, yc, row(FIRST), :]))
    more_loads.append(local(b_one, gbuf.at[zc, yc, row(SECOND), :]))
    for s in subs:
        more_loads.append(local(w_two.at[:, pl.ds(row0 + s * blk, blk)], wg2.at[zc, yc, xc, s]))
        more_loads.append(local(w_three.at[pl.ds(row0 + s * blk, blk), :], wg3.at[zc, yc, xc, s]))

    barrier = pltpu.get_barrier_semaphore()
    greeted = [device(axis, off) for axis in AXES for off in OTHERS] + [peer]
    for target in greeted:
        pl.semaphore_signal(barrier, device_id=target, device_id_type=MESH_ID)
    pl.semaphore_wait(barrier, len(greeted))

    width = 66
    send_w = [new_ids('s', width) for _ in range(3)]
    recv_w = [new_ids('r', width) for _ in range(3)]
    send_w_all, recv_w_all = sum(send_w, []), sum(recv_w, [])
    send_g, recv_c = new_ids('s', 180), new_ids('r', 180)
    q_send, q_recv = new_ids('s', 10), new_ids('r', 10)
    q1, q2, q3, qg, held3 = [], [], [], [], []

    def add_gather(buf, dst, batches, send_ids, recv_ids, quarter_at, made, held=None):
        return [plan.add(lanes, quarter(buf, dst, batch, q_send[quarter_at + k], q_recv[quarter_at + k], made, held))
                for k, (batch, lanes) in enumerate(zip(batches, gather_lanes(buf, batches, send_ids, recv_ids)))]

    gb_recv = new_ids('r', 6)

    def gain_lane():
        ready, sent_copies = NOW, []
        for k, axis, own in ((0, 'y', gbuf.at[zc, yc]), (3, 'z', gbuf.at[zc])):
            yield ready, {axis: STAT_SIZE}, NOW
            for copy in sent_copies:
                copy.wait_recv()
            made = [rcopy(own, own, stat_send[k + off - 1], gb_recv[k + off - 1], device(axis, off)) for off in OTHERS]
            for copy in made:
                copy.start()
            ready = plan.send(axis, STAT_SIZE, TWO_HOPS)
            sent_copies.extend(made)
        yield ready, {}, NOW
        for copy in made:
            copy.wait_recv()
        for copy in sent_copies:
            copy.wait_send()

    for copy in w1_loads:
        copy.wait()
    gather1 = add_gather(wg1, wq1, COARSE, send_w[0], recv_w[0], 0, q1)
    plan.pump(0.1)
    h_copies = [rcopy(src, dst, h_ids[0][k], h_ids[1][k], peer) for k, (src, dst) in enumerate(h_pairs)]
    for copy in h_copies:
        copy.start()
    for copy in more_loads:
        copy.wait()
    gather1.append(plan.add([gain_lane()], first=True))
    gather2 = add_gather(wg2, wq2, MERGED, send_w[1], recv_w[1], PAIR, q2)
    plan.finish(*gather1, alone=True)
    gather3 = add_gather(wg3, wq1, MERGED, send_w[PAIR], recv_w[PAIR], RING, q3, held3)
    for copy in h_copies:
        copy.wait_recv()
    plan.pump(plan.now + STEP)
    for copy in q1:
        copy.wait_recv()
    plan.work(PAIR)

    def gathered(k):
        return lanes_of(gbuf[z, i, row(k), :] for z in (z_own, z_own + 1) for i in range(RING))

    gain1, shift1 = gathered(0), gathered(1)
    my_cols = pl.ds(pl.multiple_of(core * half, half), half)
    gain2, shift2 = g_two[:, my_cols], b_two[:, my_cols]
    for k, value in enumerate((gain1, shift1, gain2, shift2)):
        sres[3, row(k), :] = value

    def view_rows(v):
        return pl.ds(v * vrows, vrows)

    def chunk_cols(j):
        return pl.ds(pl.multiple_of(j * quad, quad), quad)

    def over_chunks(fn):
        pl.loop(0, RING)(fn)

    def forward_rowsplit(act, own, got, views, emit, ready):
        for v, src_v in views:
            ready[v]()

            def body(j):
                zz, y0 = lax.div(j, PAIR), lax.rem(j, PAIR) * PAIR
                sides = [lanes_of(ref[z, yy].reshape(half, blk) for yy in (y0, y0 + 1))
                         for ref, z in ((own, z_own + zz), (got, zz))]
                emit(j, v, dot_nn(act[core, view_rows(src_v), :], sides[0])
                     + dot_nn(act[other, view_rows(src_v), :], sides[1]))
            over_chunks(body)

    def forward_colsplit(act, own, emit, ready):
        for v in subs:
            ready[v]()

            def body(j):
                sides = [lanes_of(own[PAIR * hh:PAIR * hh + PAIR, :, j, s].reshape(half, blk) for s in subs)
                         for hh in subs]
                emit(j, v, dot_nn(act[0, view_rows(v), :], sides[0]) + dot_nn(act[1, view_rows(v), :], sides[1]))
            over_chunks(body)

    def backward_rowsplit(act, own, views, emit, ready):
        for v, src_v in views:
            ready[v]()

            def body(j):
                sides = [lanes_of(own[PAIR * hh + i // RING, i % RING, j].reshape(quad, blk) for i in range(HALF_BLOCKS))
                         for hh in subs]
                emit(j, v, dot_nt(act[0, view_rows(src_v), :], sides[0])
                     + dot_nt(act[1, view_rows(src_v), :], sides[1]))
            over_chunks(body)

    def backward_colsplit(act, own, got, emit, ready):
        for v in subs:
            ready[v]()

            def body(j):
                sides = []
                zz, y0 = lax.div(j, PAIR), lax.rem(j, PAIR) * PAIR
                for ref, z in ((own, z_own + zz), (got, zz)):
                    bands = [lanes_of(ref[z, yy, t // PAIR, t % PAIR] for t in range(HALF_BLOCKS)) for yy in (y0, y0 + 1)]
                    sides.append(jnp.concatenate(bands, axis=0))
                emit(j, v, dot_nt(act[core, view_rows(v), :], sides[0]) + dot_nt(act[other, view_rows(v), :], sides[1]))
            over_chunks(body)

    def partial_rowsplit(dst, lhs, lhs_rows, rhs, rhs_rows):
        def body(j):
            left = lhs[core, lhs_rows, chunk_cols(j)]
            for hh in subs:
                for t in range(RING):
                    res = dot_tn(left, rhs[hh, rhs_rows, t * quad:(t + 1) * quad])
                    for i in subs:
                        for s in subs:
                            dst[PAIR * hh + t // PAIR, (t % PAIR) * PAIR + i, j, s] = res[s * blk:(s + 1) * blk,
                                                                                         i * blk:(i + 1) * blk]
        over_chunks(body)

    def partial_colsplit(dst, lhs, rhs, hh):
        def body(t):
            left = lhs[hh, :, chunk_cols(t)]
            zz, y0 = PAIR * hh + lax.div(t, PAIR), lax.rem(t, PAIR) * PAIR
            for q in range(RING):
                res = dot_tn(left, rhs[core, :, q * quad:(q + 1) * quad])
                for i, yy in enumerate((y0, y0 + 1)):
                    for s in subs:
                        dst[zz, yy, q, s] = res[i * blk:(i + 1) * blk, s * blk:(s + 1) * blk]
        over_chunks(body)

    def forward_emit(dst, parity):
        def emit(j, v, acc):
            cols = chunk_cols(j)
            dst[view_rows(v), cols] = acc
            put_stat(parity, v, cols, col_sum(acc), col_sum(acc * acc))
        return emit

    def moments(total, slot):
        for v in subs:
            mean = total[first_row(v), :half] * inv_n
            inv = lax.rsqrt(total[second_row(v), :half] * inv_n - mean * mean + BN_EPS)
            sres[slot, first_row(v), :] = mean
            sres[slot, second_row(v), :] = inv

    act_send, act_recv = new_ids('s', PAIR), new_ids('r', 10)

    def share(dst, v):
        region = dst.at[core, view_rows(v), :]
        copy = rcopy(region, region, act_send[v], act_recv.pop(), peer)
        copy.start()
        return copy

    rstep = min(32, vrows)

    def apply_rows(v, fn):
        @pl.loop(0, vrows // rstep)
        def _(i):
            fn(pl.ds(pl.multiple_of(v * vrows + i * rstep, rstep), rstep))

    def activate(src, slot, gain, shift, dst):
        copies = []
        for v in subs:
            mean = sres[slot, first_row(v), :]
            inv = sres[slot, second_row(v), :]

            def fn(rsl, mean=mean, inv=inv):
                norm = (src[rsl, :] - mean) * inv
                if gain is not None:
                    norm = jnp.maximum(gain * norm + shift, NOW)
                dst[core, rsl, :] = norm.astype(BF16)
            apply_rows(v, fn)
            copies.append(share(dst, v))
        plan.work(1)
        plan.pump(plan.now + PAIR)
        return copies

    def received(copies):
        return [copy.wait_recv for copy in copies]

    def sent(copies):
        for copy in copies:
            copy.wait_send()

    def nothing():
        pass

    both = ((0, 0), (1, 1))
    at_once = (nothing, nothing)
    all_rows = pl.ds(0, PAIR * vrows)

    MM = 3.7

    def product(fn, *args):
        plan.expect(plan.now + MM)
        plan.pump(plan.now + STEP)
        fn(*args)
        plan.work(MM)

    product(forward_rowsplit, hx, wg1, wq1, both, forward_emit(u1, 0), at_once)
    moments(stat_sum(0), 0)
    copies = activate(u1, 0, gain1, shift1, xf1)
    sent(q1 + h_copies)
    plan.finish(*gather2)
    product(forward_colsplit, xf1, wg2, forward_emit(u2, 1), received(copies))
    released.append(True)
    for send in held3:
        send()
    sent(copies)
    moments(stat_sum(1), 1)
    copies = activate(u2, 1, gain2, shift2, xf2)
    plan.finish(*gather3)
    for copy in q3:
        copy.wait_recv()
    product(forward_rowsplit, xf2, wg3, wq1, both, forward_emit(u3, 0), received(copies))
    sent(copies)
    moments(stat_sum(0), PAIR)
    copies = activate(u3, PAIR, None, None, zf)
    for copy in copies:
        copy.wait_recv()
    sent(copies)

    for v in subs:
        stat[1, 0, zc, row(v), :half] = col_sum(zf[core, view_rows(v), :].astype(F32))
    zsum_ids = new_ids('s', 1) + new_ids('r', 1)

    def zsum_lane():
        out = []
        yield from stat_steps(1, out)
        zsum[core] = out[0]
        copy = rcopy(zsum.at[core], zsum.at[core], *zsum_ids, peer)
        copy.start()
        yield plan.now + PAIR, {}, NOW
        copy.wait_recv()
        copy.wait_send()

    zsum_group = plan.add([zsum_lane()], first=True)

    partial_rowsplit(part, zf, view_rows(0), zf, view_rows(1))
    lam = lam_ref[0]
    losses = []

    def gradient_of(k, batch):
        def go():
            sub, begin, sizes = batch
            count = sum(sizes)
            rsl = pl.ds(begin, count)
            corr = part[zc, yc, xc, sub, rsl, :] * inv_n
            row_ids = (core * half + xc * quad + (sub * blk + begin)) + lax.broadcasted_iota(jnp.int32, (count, blk), 0)
            diag = row_ids == mid * blk + lax.broadcasted_iota(jnp.int32, (count, blk), 1)
            terms = jnp.where(diag, (1.0 - corr) * (1.0 - corr), lam * corr * corr)
            losses.append(jnp.sum(col_sum(terms), axis=1, keepdims=True))
            wg1[zc, yc, xc, sub, rsl, :] = jnp.where(diag, -2.0 * (1.0 - corr), 2.0 * lam * corr).astype(BF16)
            gather_g.append(plan.add(lanes_g[k], quarter(wg1, wq1, batch, q_send[6 + k], q_recv[6 + k], qg)))
        return go

    gather_g = []
    lanes_g = gather_lanes(wg1, FINE, send_g, recv_w_all)
    scatter_c = [plan.add(lanes, gradient_of(k, FINE[k]))
                 for k, lanes in enumerate(scatter_lanes(part, 0, FINE, send_w_all, recv_c))]
    plan.finish(zsum_group, *scatter_c)

    share_of = []
    sum_b = zsum[lax.div(mid, HALF_BLOCKS), row(SECOND), pl.ds(pl.multiple_of(lax.rem(mid, HALF_BLOCKS) * blk, blk), blk)]
    for s in subs:
        grad = wg1[zc, yc, xc, s].astype(F32)
        both_terms = grad * (part[zc, yc, xc, s] * inv_n)
        sum_a = zsum[core, row(FIRST), pl.ds(pl.multiple_of(xc * quad + s * blk, blk), blk)]
        share_of.append((col_sum((grad.T * sum_a).T) * inv_n, col_sum(both_terms), col_sum((grad * sum_b).T) * inv_n,
                         col_sum(both_terms.T)))
    (c0, c1, r00, r10), (d0, d1, r01, r11) = share_of
    loss_row = jnp.broadcast_to(sum(losses[1:], losses[0]), (1, blk))
    vec[zc, yc] = jnp.concatenate([c0 + d0, c1 + d1, r00, r01, r10, r11, loss_row, loss_row], axis=0)
    vec_send, vec_recv = new_ids('s', 10), new_ids('r', 10)

    def vec_lane():
        ready, pending = NOW, []
        for k, axis in enumerate(AXES[::-1][1:] + AXES[PAIR:]):
            yield ready, {axis: STAT_SIZE}, STEP
            for copy in pending[-3:]:
                copy.wait_recv()
            if axis == 'x':
                plane = [vec[t // RING, t % RING] for t in range(BLOCKS)]
                rest_rows = sum(plane[1:], plane[0])
                vecx[xc] = jnp.concatenate([item[:PAIR] for item in plane] + [rest_rows], axis=0)
            own = {'y': vec.at[zc, yc], 'z': vec.at[zc], 'x': vecx.at[xc]}[axis]
            made = [rcopy(own, own, vec_send[k * 3 + off - 1], vec_recv[k * 3 + off - 1], device(axis, off))
                    for off in OTHERS]
            for copy in made:
                copy.start()
            ready = plan.send(axis, STAT_SIZE, TWO_HOPS)
            pending.extend(made)
        yield ready, {}, STEP
        for copy in made:
            copy.wait_recv()
        got = [vecx[q] for q in range(RING)]
        vecp[core] = (got[0] + got[1]) + (got[PAIR] + got[3])
        copy = rcopy(vecp.at[core], vecp.at[core], vec_send[9], vec_recv[9], peer)
        copy.start()
        yield plan.now + PAIR, {}, NOW
        copy.wait_recv()
        sent(pending + [copy])

    vec_group = plan.add([vec_lane()], first=True)
    plan.finish(*gather_g)

    def embed_emit(j, v, acc):
        u3[view_rows(v), chunk_cols(j)] = acc * inv_n

    backward_rowsplit(zf, wg1, ((0, 1),), embed_emit, at_once)
    for copy in qg:
        copy.wait_recv()
    forward_rowsplit(zf, wg1, wq1, ((1, 0),), embed_emit, at_once)
    dzf, duf = hx, zf
    plan.work(MM)
    plan.finish(vec_group)
    first_r = PAIR * BLOCKS + PAIR
    dgb[core, :, half:half + blk] = jnp.broadcast_to(vecp[core, row(first_r + RING), :], (RING, blk))
    mine = pl.ds(pl.multiple_of(BLOCKS * core, BLOCKS), BLOCKS)
    both_cores = vecp[0, mine, :] + vecp[1, mine, :]
    sums = [[lanes_of(vecx[q, row(first_r + PAIR * t + s), :] for q in range(RING) for s in subs) for t in subs],
            [lanes_of(both_cores[row(PAIR * i + t)] for i in range(HALF_BLOCKS)) for t in subs]]
    copies = []
    for v in subs:
        def embed_rows(rsl, mean_g=sums[v][0], mean_gz=sums[v][1], inv=sres[PAIR, second_row(v), :]):
            emb = zf[core, rsl, :].astype(F32)
            dzf[core, rsl, :] = (inv * (u3[rsl, :] - (mean_g + emb * mean_gz) * inv_n)).astype(BF16)
        apply_rows(v, embed_rows)
        copies.append(share(dzf, v))
    for copy in copies:
        copy.wait_recv()
    sent(copies + q2 + q3 + qg)

    out_ids = {(slot, s): (new_ids('s', 5), new_ids('r', 5)) for slot in range(3) for s in subs}

    def publish(slot, s):
        size = PAIR * blk * blk * PAIR
        up, down = device('x', 1), device('x', 3)
        sid, rid = out_ids[slot, s]
        own = out_w.at[slot, core, xc, s]
        made = [rcopy(own, own, sid[FIRST], rid[FIRST], up), rcopy(own, own, sid[SECOND], rid[SECOND], down)]
        yield NOW, {'x': size}, NOW
        for copy in made:
            copy.start()
        yield plan.send('x', size), {'x': size / PAIR}, NOW
        for k, (off, target) in enumerate(((3, up), (1, down))):
            made[k].wait_recv()
            src = out_w.at[slot, core, near['x'][off], s, pl.ds(k * blk // PAIR, blk // PAIR), :]
            made.append(rcopy(src, src, sid[PAIR + k], rid[PAIR + k], target))
            made[-1].start()
        yield plan.send('x', size / PAIR), {}, NOW
        made[PAIR].wait_recv()
        made[3].wait_recv()
        own = out_w.at[slot, core, :, s]
        made.append(rcopy(own, own, sid[RING], rid[RING], peer))
        made[-1].start()
        yield plan.now + PAIR, {}, NOW
        made[-1].wait_recv()
        sent(made)

    published = []

    def result(slot, buf, s, groups):
        def go():
            if not any(group['left'] for group in groups):
                out_w[slot, core, xc, s] = buf[zc, yc, xc, s]
                published.append(plan.add([publish(slot, s)], first=True))
        return go

    def layer_emit(src, slot, parity, k):
        def emit(j, v, acc):
            cols = chunk_cols(j)
            norm = (src[view_rows(v), cols] - sres[slot, first_row(v), cols]) * sres[slot, second_row(v), cols]
            lin = sres[3, row(k), cols] * norm + sres[3, row(k + 1), cols]
            grad = jnp.where(lin > 0, acc, NOW)
            u3[view_rows(v), cols] = grad
            put_stat(parity, v, cols, col_sum(grad), col_sum(grad * norm))
        return emit

    def layer_rows(src, slot, k, total, v, store):
        sum_lin, sum_norm = total[first_row(v), :half], total[second_row(v), :half]
        mean, inv = sres[slot, first_row(v), :], sres[slot, second_row(v), :]
        scale = sres[3, row(k), :] * inv

        def fn(rsl):
            norm = (src[rsl, :] - mean) * inv
            store(rsl, (scale * (u3[rsl, :] - (sum_lin + norm * sum_norm) * inv_n)).astype(BF16))
        apply_rows(v, fn)

    def affine_grads(total, k):
        dgb[core, row(k), :half] = total[second_row(FIRST), :half] + total[second_row(SECOND), :half]
        dgb[core, row(k + 1), :half] = total[first_row(FIRST), :half] + total[first_row(SECOND), :half]

    def add_scatter(slot, buf, batches, lanes):
        groups = {s: [] for s in subs}
        for batch, batch_lanes in zip(batches, lanes):
            s = batch[0]
            groups[s].append(plan.add(batch_lanes, result(slot, buf, s, groups[s])))
        return groups[0] + groups[1]

    partial_rowsplit(part, xf2, all_rows, dzf, all_rows)
    plan.work(3)
    scatter_3 = add_scatter(PAIR, part, BACK, scatter_lanes(part, 0, BACK, send_w_all, recv_c, give=True))
    product(backward_rowsplit, dzf, wg3, both, layer_emit(u2, 1, 0, PAIR), at_once)
    total = stat_sum(0)
    affine_grads(total, 0)
    copies = []
    for v in subs:
        def put_du2(rsl, value):
            duf[core, rsl, :] = value
        layer_rows(u2, 1, PAIR, total, v, put_du2)
        copies.append(share(duf, v))
    plan.work(1)
    plan.pump(plan.now + PAIR)
    for copy in q2:
        copy.wait_recv()
    product(backward_colsplit, duf, wg2, wq2, layer_emit(u1, 0, 1, 0), received(copies))
    sent(copies)
    scatter_2 = []

    def part2_lane(hh):
        yield NOW, {}, 1.9
        partial_colsplit(part2, xf1, duf, hh)
        plan.work(1.9)

    def start_2():
        scatter_2.extend(add_scatter(1, part2, BACK, scatter_lanes(part2, 1, BACK, send_g, recv_w_all, take=True)))

    part2_group = plan.add([part2_lane(hh) for hh in subs], start_2, first=True)
    total = stat_sum(1)
    plan.finish(part2_group)
    affine_grads(total, PAIR)
    dg_send, dg_recv = new_ids('s', 1)[0], new_ids('r', 1)[0]
    dg_copy = rcopy(dgb.at[core], dgb.at[core], dg_send, dg_recv, peer)
    dg_copy.start()

    for v in subs:
        def put_du1(rsl, value, v=v):
            start = rsl.start - v * vrows
            r = pl.multiple_of(lax.rem(start, rows), min(rstep, rows))
            c = lax.div(start, rows)
            for i in range(HALF_BLOCKS):
                du1[i // RING, i % RING, c, v, pl.ds(r, rstep), :] = value[:, i * blk:(i + 1) * blk]
        layer_rows(u1, 0, 0, total, v, put_du1)

    a2a_recv, a2a_send = new_ids('r', BLOCKS), new_ids('s', BLOCKS)
    targets = [(i // RING, i % RING, c) for i in range(HALF_BLOCKS) for c in subs]

    slots = (hx, zf, xf1, xf2)
    per = RING * rows

    turn = (0, 1, 3, PAIR)

    def h_fetch(chunk):
        at = chunk % RING
        begin = pl.multiple_of(near['z'][turn[chunk // PAIR]] * per, per)
        made = [pltpu.make_async_copy((h_a, h_b)[chunk % PAIR].at[pl.ds(begin, per), pl.ds(kh * half, half)],
                                      slots[at].at[kh], hsem.at[at * PAIR + kh]) for kh in subs]
        for copy in made:
            copy.start()
        return made

    fetches = [h_fetch(chunk) for chunk in range(RING)]
    own_half = lax.div(mid, HALF_BLOCKS)
    self_out = jnp.where(own_half == core, PAIR * (mid - HALF_BLOCKS * core) + core, -1)
    self_in = jnp.where(own_half == core, mid, -1)
    a2a_home, a2a_sem = a2a.at[zc, yc], rsem.at[a2a_recv[0] + mid]

    for k, (zi, yy, c) in enumerate(targets):
        src = du1.at[zi, yy, c]

        @pl.when(self_out == k)
        def _():
            a2a_home[...] = src[...]

        @pl.when(self_out != k)
        def _():
            pltpu.make_async_remote_copy(
                src_ref=src, dst_ref=a2a_home, send_sem=ssem.at[a2a_send[k]], recv_sem=a2a_sem,
                device_id=(HALF_BLOCKS * core + zi * RING + yy, x_base + c), device_id_type=MESH_ID).start()

    plan.work(1)
    arrived = max([plan.send(axis, 32 * rows * blk, TWO_HOPS) for axis in 'zy'])
    arrivals = [arrived - off for off in (4, PAIR, 1, 0)]
    for k in range(RING):
        plan.pump(arrivals[k])
        plan.until(arrivals[k])
        zz = near['z'][turn[k]]
        for i in range(RING):
            @pl.when(self_in != zz * RING + i)
            def _():
                pltpu.make_async_copy(a2a.at[zz, i], a2a.at[zz, i], rsem.at[a2a_recv[0] + zz * RING + i]).wait()
        for v in subs:
            chunk = PAIR * k + v
            at = chunk % RING
            for copy in fetches[chunk]:
                copy.wait()
            grad = jnp.concatenate([a2a[zz, i, v] for i in range(RING)], axis=0)
            for kh in subs:
                for q in range(RING):
                    res = dot_tn(grad, slots[at][kh, :, q * quad:(q + 1) * quad])
                    spot = (slice(kh * blk, (kh + 1) * blk), slice(q * quad, (q + 1) * quad))
                    u2[spot] = res + u2[spot] if chunk else res
            if chunk < RING:
                fetches.append(h_fetch(chunk + RING))
        plan.work(1)
    for k, (zi, yy, c) in enumerate(targets):
        @pl.when(self_out != k)
        def _():
            pltpu.make_async_copy(du1.at[zi, yy, c], du1.at[zi, yy, c], ssem.at[a2a_send[k]]).wait()

    x_recv, x_send = new_ids('r', RING), new_ids('s', RING)

    def strip(k, cols=pl.ds(0, half)):
        return u2.at[pl.ds(pl.multiple_of(k * blk, blk), blk), cols]

    swap = rcopy(strip(other), strip(PAIR), x_send[0], x_recv[0], peer)
    swap.start()
    plan.need['x'] = plan.now + 3.0
    plan.pump(plan.now + PAIR)
    swap.wait_recv()
    swap.wait_send()
    strip(core)[...] = strip(core)[...] + strip(PAIR)[...]
    shifts = [rcopy(strip(core, chunk_cols(near['x'][off])), strip(3, chunk_cols(off)), x_send[off], x_recv[off],
                    device('x', off)) for off in OTHERS]
    for copy in shifts:
        copy.start()
    arrived = plan.send('x', PAIR * quad * blk * RING, TWO_HOPS)
    plan.pump(arrived)
    for copy in shifts:
        copy.wait_recv()
    got = [strip(3, chunk_cols(off))[...] for off in OTHERS]
    piece_sum = (strip(core, chunk_cols(xc))[...] + got[0]) + (got[1] + got[2])
    for s in subs:
        out_w[0, core, xc, s] = piece_sum[:, s * blk:(s + 1) * blk].T
    sent(shifts)
    plan.need['x'] = FAR
    published.append(plan.add([publish(0, s) for s in subs], first=True))
    plan.finish(*scatter_3, *scatter_2)
    plan.finish(*published)
    dg_copy.wait_recv()
    dg_copy.wait_send()
    w_copy = pltpu.make_async_copy(out_w, dw_out, lsem.at[0])
    w_copy.start()
    small_out[...] = dgb[...]
    w_copy.wait()


def split_kernel(blk, dw_ref, small_ref, loss_out, dw1_out, dw2_out, dw3_out, dg1_out, db1_out, dg2_out, db2_out,
                 stage, sem_in, sem_out):
    half = HALF_BLOCKS * blk
    mid = lax.axis_index('model')
    loads = []
    for slot in range(3):
        loads.append(pltpu.make_async_copy(dw_ref.at[slot], stage.at[slot], sem_in.at[slot]))
        loads[-1].start()
    loss_out[...] = small_ref[0, FIRST:SECOND, half:half + 1] + small_ref[1, FIRST:SECOND, half:half + 1]
    for hh in range(PAIR):
        dg2_out[:, hh * half:(hh + 1) * half] = small_ref[hh, FIRST:SECOND, :half]
        db2_out[:, hh * half:(hh + 1) * half] = small_ref[hh, SECOND:PAIR, :half]
    mcols = pl.ds(pl.multiple_of(lax.rem(mid, HALF_BLOCKS) * blk, blk), blk)
    dg1_out[...] = small_ref[lax.div(mid, HALF_BLOCKS), 2:3, mcols]
    db1_out[...] = small_ref[lax.div(mid, HALF_BLOCKS), 3:4, mcols]
    stores = []
    for slot in range(3):
        loads[slot].wait()
        for t in range(BLOCKS):
            begin = pl.ds(t * blk, blk)
            dst = (dw1_out.at[begin, :], dw2_out.at[:, begin], dw3_out.at[begin, :])[slot]
            stores.append(pltpu.make_async_copy(stage.at[slot, t // HALF_BLOCKS, (t // PAIR) % RING, t % PAIR], dst,
                                                sem_out.at[len(stores)]))
            stores[-1].start()
    for copy in stores:
        copy.wait()


def build_call(blk, rows, total_rows, vmem_limit):
    dim, half = BLOCKS * blk, HALF_BLOCKS * blk
    trows = RING * rows
    pieces = (RING, RING, RING, PAIR, blk, blk)
    got = (PAIR, RING, RING, PAIR, blk, blk)
    act = pltpu.VMEM((PAIR, trows, half), BF16)
    pre = pltpu.VMEM((trows, half), F32)
    bank = (PAIR, RING, PAIR, blk, blk)
    dma = pltpu.SemaphoreType.DMA
    scratch = [
        act, pre, pre, pre, act, act, act,
        pltpu.VMEM(pieces, BF16), pltpu.VMEM(got, BF16), pltpu.VMEM(pieces, BF16), pltpu.VMEM(got, BF16),
        pltpu.VMEM(pieces, BF16),
        pltpu.VMEM(pieces, F32), pltpu.VMEM(pieces, F32),
        pltpu.VMEM((PAIR, 6, RING, PAIR, blk, blk), F32), pltpu.VMEM((PAIR, PAIR, 6, PAIR, blk, blk), F32),
        pltpu.VMEM((PAIR, PAIR, 3, blk, blk), F32),
        pltpu.VMEM((RING, RING, HALF_BLOCKS, blk), F32),
        pltpu.VMEM((PAIR, 3, RING, RING, half), F32), pltpu.VMEM((RING, RING, half), F32),
        pltpu.VMEM((PAIR, RING, half + blk), F32),
        pltpu.VMEM((PAIR, RING, half), F32), pltpu.VMEM((RING, RING, HALF_BLOCKS, blk), F32),
        pltpu.VMEM((RING, 40, blk), F32), pltpu.VMEM((PAIR, 40, blk), F32),
        pltpu.VMEM((PAIR, RING, PAIR, PAIR, rows, blk), BF16), pltpu.VMEM((RING, RING, PAIR, rows, blk), BF16),
        pltpu.VMEM((3,) + bank, F32),
        dma((N_SEND,)), dma((N_RECV,)), dma((BLOCKS,)), dma((HALF_BLOCKS,)), pltpu.SemaphoreType.REGULAR((12,)),
    ]
    anyspec = pl.BlockSpec(memory_space=pl.ANY)
    vmem = pl.BlockSpec(memory_space=pltpu.VMEM)
    smem = pl.BlockSpec(memory_space=pltpu.SMEM)
    packed = jax.ShapeDtypeStruct((3,) + bank, F32)
    step_call = pl.pallas_call(
        functools.partial(mega_kernel, (blk, rows, total_rows)),
        out_shape=[packed, jax.ShapeDtypeStruct((PAIR, RING, half + blk), F32)],
        in_specs=[anyspec] * 7 + [vmem, vmem, smem],
        out_specs=[anyspec, vmem],
        scratch_shapes=scratch,
        compiler_params=pltpu.CompilerParams(collective_id=0, has_side_effects=True, vmem_limit_bytes=vmem_limit),
        name='barlow_step',
    )

    def line(n):
        return jax.ShapeDtypeStruct((1, n), F32)

    tall, wide = jax.ShapeDtypeStruct((dim, blk), F32), jax.ShapeDtypeStruct((blk, dim), F32)
    split_call = pl.pallas_call(
        functools.partial(split_kernel, blk),
        out_shape=[line(1), tall, wide, tall, line(blk), line(blk), line(dim), line(dim)],
        in_specs=[anyspec, vmem],
        out_specs=[vmem, anyspec, anyspec, anyspec, vmem, vmem, vmem, vmem],
        scratch_shapes=[pltpu.VMEM((3,) + bank, F32), dma((3,)), dma((48,))],
        name='split_results',
    )

    def call(*args):
        return split_call(*step_call(*args))

    return call


def solution(mesh):
    data_size = mesh.shape['data']

    def shard_body(h_a, h_b, w_one, w_two, w_three, g_one, b_one, g_two, b_two, lam_off):
        group_rows = h_a.shape[0]
        blk = w_three.shape[1]
        rows = group_rows // BLOCKS
        call = build_call(blk, rows, group_rows * data_size, 67_000_000)
        outs = call(h_a, h_b, w_one, w_two, w_three, g_one.reshape(1, -1), b_one.reshape(1, -1),
                    g_two.reshape(1, -1), b_two.reshape(1, -1), lam_off)
        loss, dw1, dw2, dw3, dg1, db1, dg2, db2 = outs
        return (loss.reshape(1), dw1, dw2, dw3, dg1.reshape(-1), db1.reshape(-1), dg2.reshape(-1), db2.reshape(-1))

    in_specs = (P('data', None), P('data', None), P(None, 'model'), P('model', None), P(None, 'model'),
                P('model'), P('model'), P(), P(), P())
    out_specs = (P(), P(None, 'model'), P('model', None), P(None, 'model'), P('model'), P('model'), P(), P())
    return jax.shard_map(shard_body, mesh=mesh, in_specs=in_specs, out_specs=out_specs, check_vma=False)
```

```python
import functools

import jax
import jax.numpy as jnp
from jax import lax
from jax.experimental import pallas as pl
from jax.experimental.pallas import tpu as pltpu
from jax.sharding import PartitionSpec as P

BN_EPS = 1e-5
MESH_ID = pl.DeviceIdType.MESH
RING = 4
PAIR = 2
AXES = ('z', 'y', 'x')
ORDERS = (('x', 'y', 'z'), ('y', 'z', 'x'), ('z', 'x', 'y'))
COARSE = ((0, 0, (40, 48, 40)), (1, 0, (48, 40, 40)))
FINE = COARSE
BACK = COARSE
OTHERS = (1, 2, 3)
N_SEND = 520
N_RECV = 520
BYTES_PER_US = 46600.0
HOP = 1.9
TWO_HOPS = 2.7
BACKLOG = 5.0
SMALL = 60000
FAR = 1e9
F32 = jnp.float32
BF16 = jnp.bfloat16
WHOLE = slice(None)
FIRST, SECOND = 0, 1
BLOCKS, HALF_BLOCKS = 16, 8
NOW = 0.0
STEP = 0.2
STAT_SIZE = 32768


def dot_nn(a, b):
    return lax.dot_general(a, b, (((1,), (0,)), ((), ())), preferred_element_type=F32)


def dot_nt(a, b):
    return lax.dot_general(a, b, (((1,), (1,)), ((), ())), preferred_element_type=F32)


def dot_tn(a, b):
    return lax.dot_general(a, b, (((0,), (0,)), ((), ())), preferred_element_type=F32)


def col_sum(value):
    return jnp.sum(value, axis=0, keepdims=True)


def lanes_of(values):
    return jnp.concatenate(list(values), axis=1)


def wrap(value):
    return lax.rem(value, RING)


class Plan:
    def __init__(self):
        self.now = 0.0
        self.free = dict.fromkeys(AXES, 0.0)
        self.need = dict.fromkeys(AXES, FAR)
        self.lanes = []
        self.first = None

    def work(self, us):
        self.now += us

    def until(self, when):
        self.now = max(self.now, when)

    def send(self, axis, size, flight=HOP):
        self.free[axis] = max(self.free[axis], self.now) + size / BYTES_PER_US
        return self.free[axis] + flight

    def add(self, gens, then=None, first=False):
        group = {'left': 0, 'then': then}
        made = []
        for gen in gens:
            group['left'] += 1
            made.append([gen, next(gen), group])
        self.lanes = made + self.lanes if first else self.lanes + made
        return group

    def start_of(self, lane):
        ready, loads, _ = lane[1]
        start = max(self.now, ready() if callable(ready) else ready)
        if self.first is not None and lane[2] not in self.first and max(loads.values(), default=0) > SMALL:
            return FAR
        for axis, size in loads.items():
            start = max(start, self.free[axis] - BACKLOG)
        for axis, size in loads.items():
            if max(self.free[axis], start) + size / BYTES_PER_US > self.need[axis] + 1.0:
                return FAR
        return start

    def advance(self, limit):
        best, begin = None, limit
        for lane in self.lanes:
            start = self.start_of(lane)
            if start < begin and start + lane[1][2] < limit + 1.0:
                best, begin = lane, start
        if best is None:
            return False
        self.until(begin)
        info = next(best[0], None)
        if info is not None:
            best[1] = info
            return True
        self.lanes = [lane for lane in self.lanes if lane is not best]
        group = best[2]
        group['left'] -= 1
        if not group['left'] and group['then'] is not None:
            group['then']()
        return True

    def pump(self, limit):
        while self.advance(limit):
            pass

    def finish(self, *groups, alone=False):
        self.first = groups if alone else None
        while any(group['left'] for group in groups):
            if not self.advance(FAR):
                self.need = dict.fromkeys(AXES, FAR)
        self.first = None

    def expect(self, when):
        for axis in AXES:
            self.need[axis] = when
            when += 3.6


def mega_kernel(cfg, h_a, h_b, w_one, w_two, w_three, g_one, b_one, g_two, b_two, lam_ref,
                dw_out, small_out,
                hx, u1, u2, u3, xf1, xf2, zf, wg1, wq1, wg2, wq2, wg3, part, part2, rv1, rv2, rv3,
                gbuf, stat, sres, dgb, zsum, vec, vecx, vecp, du1, a2a, out_w, ssem, rsem, lsem, hsem, credit):
    blk, rows, total_rows = cfg
    plan = Plan()
    half = HALF_BLOCKS * blk
    quad = PAIR * blk
    vrows = PAIR * rows
    inv_n = 1.0 / total_rows

    mid = lax.axis_index('model')
    did = lax.axis_index('data')
    core = lax.rem(did, PAIR)
    other = 1 - core
    coord = {'z': lax.div(mid, RING), 'y': wrap(mid), 'x': lax.div(did, PAIR)}
    zc, yc, xc = coord['z'], coord['y'], coord['x']
    near = {axis: [coord[axis]] + [wrap(coord[axis] + off) for off in OTHERS] for axis in AXES}
    z_base, x_base = zc * RING, xc * PAIR
    targets_of = {'z': [(q * RING + yc, did) for q in near['z']], 'y': [(z_base + q, did) for q in near['y']],
                  'x': [(mid, q * PAIR + core) for q in near['x']]}
    peer = (mid, x_base + other)

    def device(axis, off):
        if isinstance(off, int):
            return targets_of[axis][off]
        q = wrap(coord[axis] + off)
        return {'z': (q * RING + yc, did), 'y': (z_base + q, did), 'x': (mid, q * PAIR + core)}[axis]

    class Fan:
        def __init__(self, axis, place, sid, rid):
            def make(off):
                src, dst = place(off)
                return rcopy(src, dst, sid[0] + off - 1, rid[0] + off - 1, device(axis, off))
            self.make = make

        def each(self, action):
            @pl.loop(1, RING)
            def _(off):
                getattr(self.make(off), action)()

        def start(self):
            self.each('start')

        def wait_recv(self):
            self.each('wait_recv')

        def wait_send(self):
            self.each('wait_send')

    z_own, z_other = PAIR * core, PAIR * other
    counters = {'s': 0, 'r': 0, 'l': 0}

    def new_ids(kind, count):
        first = counters[kind]
        counters[kind] = first + count
        assert counters[kind] <= {'s': N_SEND, 'r': N_RECV, 'l': BLOCKS}[kind]
        return list(range(first, first + count))

    def rcopy(src, dst, send_id, recv_id, target):
        return pltpu.make_async_remote_copy(src_ref=src, dst_ref=dst, send_sem=ssem.at[send_id],
                                            recv_sem=rsem.at[recv_id], device_id=target, device_id_type=MESH_ID)

    def bands(batches):
        for sub, begin, sizes in batches:
            for colour, size in enumerate(sizes):
                yield sub, colour, pl.ds(begin, size), size * blk
                begin += size

    def gather_lane(buf, sub, colour, rsl, cells, sid, rid):
        order = ORDERS[colour]
        size = PAIR * cells

        def region(axis, have, q, part_id=None):
            idx = dict(coord)
            idx[axis] = q
            for name in have:
                idx[name] = WHOLE
            if part_id is not None:
                idx[have[-1]] = pl.ds(PAIR * part_id, PAIR)
            return buf.at[idx['z'], idx['y'], idx['x'], sub, rsl, :]

        axis = order[0]
        yield NOW, {axis: PAIR * size}, NOW
        own = region(axis, (), coord[axis])
        pending = [Fan(axis, lambda off, own=own: (own, own), sid, rid)]
        pending[0].start()
        ready = plan.send(axis, PAIR * size, TWO_HOPS)
        for phase in (1, 2):
            size *= RING
            axis, have = order[phase], order[:phase]
            yield ready, {axis: size}, STEP
            for copy in pending[-PAIR:]:
                copy.wait_recv()
            base = phase * RING - 1
            up, down = device(axis, 1), device(axis, 3)
            own = region(axis, have, coord[axis])
            to_up = rcopy(own, own, sid[base], rid[base], up)
            to_down = rcopy(own, own, sid[base + 1], rid[base + 1], down)
            to_up.start()
            to_down.start()
            yield plan.send(axis, size), {axis: size / PAIR}, STEP
            to_up.wait_recv()
            src = region(axis, have, near[axis][3], 0)
            relay_up = rcopy(src, src, sid[base + 2], rid[base + 2], up)
            relay_up.start()
            to_down.wait_recv()
            src = region(axis, have, near[axis][1], 1)
            relay_down = rcopy(src, src, sid[base + 3], rid[base + 3], down)
            relay_down.start()
            ready = plan.send(axis, size / PAIR)
            pending.extend((to_up, to_down, relay_up, relay_down))
        yield ready, {}, STEP
        for copy in pending[-2:]:
            copy.wait_recv()
        for copy in pending:
            copy.wait_send()

    def lanes_by_batch(make, batches, send_ids, recv_ids, width):
        lanes = []
        for k, found in enumerate(bands(batches)):
            ids = slice(k * width, (k + 1) * width)
            lanes.append(make(k, *found, send_ids[ids], recv_ids[ids]))
        return [lanes[k:k + 3] for k in range(0, len(lanes), 3)]

    def gather_lanes(buf, batches, send_ids, recv_ids):
        return lanes_by_batch(lambda k, *args: gather_lane(buf, *args), batches, send_ids, recv_ids, 11)

    given = {}

    def scatter_lane(buf, bank, give, take, sub, colour, rsl, cells, sid, rid):
        order = ORDERS[colour]
        pending = []
        ready = NOW
        size = cells * 32
        for phase in (0, 1):
            axis = order[phase]
            left = tuple(name for name in AXES if name in order[phase + 1:])
            p = coord[axis]
            base = phase * 6

            def region(q, part_id, axis=axis, left=left):
                idx = dict(coord)
                idx[axis] = q
                for name in left[:-1]:
                    idx[name] = WHOLE
                idx[left[-1]] = pl.ds(PAIR * part_id, PAIR)
                return buf.at[idx['z'], idx['y'], idx['x'], sub, rsl, :]

            def landing(slot, phase=phase):
                if phase:
                    return rv2.at[bank, sub, slot, :, rsl, :]
                return rv1.at[sub, slot, :, :, rsl, :]

            def add(q, part_id, slots, axis=axis, left=left, phase=phase):
                def one(i, j):
                    idx = dict(coord)
                    idx[axis] = q
                    idx[left[-1]] = PAIR * part_id + j
                    if not phase:
                        idx[left[0]] = i
                    total = buf[idx['z'], idx['y'], idx['x'], sub, rsl, :]
                    for slot in slots:
                        total = total + (rv2[bank, sub, slot, j, rsl, :] if phase else rv1[sub, slot, i, j, rsl, :])
                    buf[idx['z'], idx['y'], idx['x'], sub, rsl, :] = total

                if phase:
                    for j in range(PAIR):
                        one(0, j)
                else:
                    @pl.loop(0, RING)
                    def _(i):
                        for j in range(PAIR):
                            one(i, j)

            up, down = device(axis, 1), device(axis, 3)
            p1, p2, p3 = near[axis][1:]
            if phase:
                yield ready, {axis: PAIR * size}, STEP
                finals()
            else:
                yield (ready if take is None else lambda: given.get(take, FAR)), {axis: size}, NOW
                if take is not None:
                    pl.semaphore_wait(credit.at[take], PAIR)
            relay_up = rcopy(region(p2, 1), landing(0), sid[base], rid[base], up)
            relay_down = rcopy(region(p2, 0), landing(1), sid[base + 1], rid[base + 1], down)
            own_up = rcopy(region(p1, 0), landing(2), sid[base + 2], rid[base + 2], up)
            own_down = rcopy(region(p3, 1), landing(3), sid[base + 3], rid[base + 3], down)
            relay_up.start()
            relay_down.start()
            relayed = plan.send(axis, size)
            if not phase:
                yield NOW, {axis: size}, NOW
            own_up.start()
            own_down.start()
            plan.send(axis, size)
            yield relayed, {axis: size}, STEP
            relay_up.wait_recv()
            add(p1, 1, (0,))
            sum_up = rcopy(region(p1, 1), landing(4), sid[base + 4], rid[base + 4], up)
            sum_up.start()
            relay_down.wait_recv()
            add(p3, 0, (1,))
            sum_down = rcopy(region(p3, 0), landing(5), sid[base + 5], rid[base + 5], down)
            sum_down.start()
            ready = plan.send(axis, size)
            size /= RING

            def finals(phase=phase, p=p, add=add, own_up=own_up, own_down=own_down, sum_up=sum_up, sum_down=sum_down,
                       up=up, down=down):
                own_up.wait_recv()
                sum_down.wait_recv()
                add(p, 0, (2, 5))
                own_down.wait_recv()
                sum_up.wait_recv()
                add(p, 1, (3, 4))
                if give is not None and not phase:
                    given[give] = plan.now + 1.0
                    for target in (up, down):
                        pl.semaphore_signal(credit.at[give], device_id=target, device_id_type=MESH_ID)

            pending.extend((relay_up, relay_down, own_up, own_down, sum_up, sum_down))
        axis = order[2]
        size *= RING
        yield ready, {axis: size}, STEP
        finals()
        base = 12

        def spot(off):
            idx = dict(coord)
            idx[axis] = wrap(coord[axis] + off)
            return buf.at[idx['z'], idx['y'], idx['x'], sub, rsl, :], rv3.at[bank, sub, off - 1, rsl, :]

        last = [Fan(axis, spot, sid[base:], rid[base:])]
        last[0].start()
        yield plan.send(axis, size, TWO_HOPS), {}, STEP
        for copy in last:
            copy.wait_recv()
        got = [rv3[bank, sub, k, rsl, :] for k in range(3)]
        buf[zc, yc, xc, sub, rsl, :] = (buf[zc, yc, xc, sub, rsl, :] + got[0]) + (got[1] + got[2])
        for copy in pending + last:
            copy.wait_send()

    def scatter_lanes(buf, bank, batches, send_ids, recv_ids, give=False, take=False):
        return lanes_by_batch(lambda k, *args: scatter_lane(buf, bank, k if give else None, k if take else None, *args),
                              batches, send_ids, recv_ids, 15)

    released = []

    def quarter(src, dst, batch, send_id, recv_id, made, held=None):
        sub, begin, sizes = batch
        rsl = pl.ds(begin, sum(sizes))

        def send():
            if held is not None and not released:
                held.append(send)
                return
            copy = rcopy(src.at[pl.ds(z_other, PAIR), :, :, sub, rsl, :], dst.at[:, :, :, sub, rsl, :], send_id, recv_id,
                         peer)
            copy.start()
            made.append(copy)
        return send

    stat_recv = [new_ids('r', 9) for _ in range(PAIR)]
    stat_send = new_ids('s', 9)

    def stat_steps(parity, out):
        pending, ready, width = [], NOW, slice(half)
        for d, axis in enumerate(AXES):
            yield ready, {axis: STAT_SIZE}, STEP
            if d:
                stat[parity, d, coord[axis], :, width] = gathered_stat(parity, d - 1, pending)
            own = stat.at[parity, d, coord[axis], :, width]
            pending.append(Fan(axis, lambda off, own=own: (own, own), stat_send[d * 3:], stat_recv[parity][d * 3:]))
            pending[-1].start()
            ready = plan.send(axis, STAT_SIZE, TWO_HOPS)
        yield ready, {}, STEP
        out.append(gathered_stat(parity, d, pending))
        for copy in pending:
            copy.wait_send()

    def gathered_stat(parity, d, pending):
        pending[-1].wait_recv()
        got = [stat[parity, d, q, :, :half] for q in range(RING)]
        return (got[0] + got[1]) + (got[PAIR] + got[3])

    def stat_sum(parity):
        out = []
        steps = stat_steps(parity, out)
        next(steps)
        plan.expect(plan.now)
        for axis in AXES:
            ready = next(steps)[0]
            plan.need[axis] = FAR
            plan.pump(ready)
            plan.until(ready)
            plan.work(STEP)
        next(steps, None)
        return out[0]

    def row(k):
        return slice(k, k + 1)

    def first_row(v):
        return row(PAIR * v)

    def second_row(v):
        return row(PAIR * v + 1)

    def put_stat(parity, v, cols, first, second):
        stat[parity, 0, zc, first_row(v), cols] = first
        stat[parity, 0, zc, second_row(v), cols] = second

    def local(src, dst):
        copy = pltpu.make_async_copy(src, dst, lsem.at[new_ids('l', 1)[0]])
        copy.start()
        return copy

    row0 = pl.multiple_of(core * half + xc * quad, quad)
    subs = range(PAIR)
    w1_loads = [local(w_one.at[pl.ds(row0 + s * blk, blk), :], wg1.at[zc, yc, xc, s]) for s in subs]
    hrow = pl.multiple_of(mid * rows, rows)
    h_ids = [new_ids('s', RING), new_ids('r', RING)]
    h_pairs = []
    for v, h_ref in enumerate((h_a, h_b)):
        for kh in subs:
            h_pairs.append((h_ref.at[pl.ds(hrow, rows), pl.ds(kh * half, half)],
                            hx.at[kh, pl.ds(pl.multiple_of(v * vrows + core * rows, rows), rows), :]))
    more_loads = [local(src, dst) for src, dst in h_pairs]
    more_loads.append(local(g_one, gbuf.at[zc, yc, row(FIRST), :]))
    more_loads.append(local(b_one, gbuf.at[zc, yc, row(SECOND), :]))
    for s in subs:
        more_loads.append(local(w_two.at[:, pl.ds(row0 + s * blk, blk)], wg2.at[zc, yc, xc, s]))
        more_loads.append(local(w_three.at[pl.ds(row0 + s * blk, blk), :], wg3.at[zc, yc, xc, s]))

    barrier = pltpu.get_barrier_semaphore()
    greeted = [device(axis, off) for axis in AXES for off in OTHERS] + [peer]
    for target in greeted:
        pl.semaphore_signal(barrier, device_id=target, device_id_type=MESH_ID)
    pl.semaphore_wait(barrier, len(greeted))

    width = 66
    send_w = [new_ids('s', width) for _ in range(3)]
    recv_w = [new_ids('r', width) for _ in range(3)]
    send_w_all, recv_w_all = sum(send_w, []), sum(recv_w, [])
    send_g, recv_c = new_ids('s', 180), new_ids('r', 180)
    q_send, q_recv = new_ids('s', 10), new_ids('r', 10)
    q1, q2, q3, qg, held3 = [], [], [], [], []

    def add_gather(buf, dst, batches, send_ids, recv_ids, quarter_at, made, held=None):
        return [plan.add(lanes, quarter(buf, dst, batch, q_send[quarter_at + k], q_recv[quarter_at + k], made, held))
                for k, (batch, lanes) in enumerate(zip(batches, gather_lanes(buf, batches, send_ids, recv_ids)))]

    gb_recv = new_ids('r', 6)

    def gain_lane():
        ready, sent_copies = NOW, []
        for k, axis, own in ((0, 'y', gbuf.at[zc, yc]), (3, 'z', gbuf.at[zc])):
            yield ready, {axis: STAT_SIZE}, NOW
            for copy in sent_copies:
                copy.wait_recv()
            made = [Fan(axis, lambda off, own=own: (own, own), stat_send[k:], gb_recv[k:])]
            made[0].start()
            ready = plan.send(axis, STAT_SIZE, TWO_HOPS)
            sent_copies.extend(made)
        yield ready, {}, NOW
        for copy in made:
            copy.wait_recv()
        for copy in sent_copies:
            copy.wait_send()

    for copy in w1_loads:
        copy.wait()
    gather1 = add_gather(wg1, wq1, COARSE, send_w[0], recv_w[0], 0, q1)
    plan.pump(0.1)
    h_copies = [rcopy(src, dst, h_ids[0][k], h_ids[1][k], peer) for k, (src, dst) in enumerate(h_pairs)]
    for copy in h_copies:
        copy.start()
    for copy in more_loads:
        copy.wait()
    gather1.append(plan.add([gain_lane()], first=True))
    gather2 = add_gather(wg2, wq2, COARSE, send_w[1], recv_w[1], PAIR, q2)
    plan.finish(*gather1, alone=True)
    gather3 = add_gather(wg3, wq1, COARSE, send_w[PAIR], recv_w[PAIR], RING, q3, held3)
    for copy in h_copies:
        copy.wait_recv()
    plan.pump(plan.now + STEP)
    for copy in q1:
        copy.wait_recv()
    plan.work(PAIR)

    def gathered(k):
        return lanes_of(gbuf[z, i, row(k), :] for z in (z_own, z_own + 1) for i in range(RING))

    gain1, shift1 = gathered(0), gathered(1)
    my_cols = pl.ds(pl.multiple_of(core * half, half), half)
    gain2, shift2 = g_two[:, my_cols], b_two[:, my_cols]
    for k, value in enumerate((gain1, shift1, gain2, shift2)):
        sres[3, row(k), :] = value

    def view_rows(v):
        return pl.ds(v * vrows, vrows)

    def chunk_cols(j):
        return pl.ds(pl.multiple_of(j * quad, quad), quad)

    def over_chunks(fn):
        pl.loop(0, RING)(fn)

    def forward_rowsplit(act, own, got, views, emit, ready):
        for v, src_v in views:
            ready[v]()

            def body(j):
                zz, y0 = lax.div(j, PAIR), lax.rem(j, PAIR) * PAIR
                sides = [lanes_of(ref[z, yy].reshape(half, blk) for yy in (y0, y0 + 1))
                         for ref, z in ((own, z_own + zz), (got, zz))]
                emit(j, v, dot_nn(act[core, view_rows(src_v), :], sides[0])
                     + dot_nn(act[other, view_rows(src_v), :], sides[1]))
            over_chunks(body)

    def forward_colsplit(act, own, emit, ready):
        for v in subs:
            ready[v]()

            def body(j):
                sides = [lanes_of(own[PAIR * hh:PAIR * hh + PAIR, :, j, s].reshape(half, blk) for s in subs)
                         for hh in subs]
                emit(j, v, dot_nn(act[0, view_rows(v), :], sides[0]) + dot_nn(act[1, view_rows(v), :], sides[1]))
            over_chunks(body)

    def backward_rowsplit(act, own, views, emit, ready):
        for v, src_v in views:
            ready[v]()

            def body(j):
                sides = [lanes_of(own[PAIR * hh + i // RING, i % RING, j].reshape(quad, blk) for i in range(HALF_BLOCKS))
                         for hh in subs]
                emit(j, v, dot_nt(act[0, view_rows(src_v), :], sides[0])
                     + dot_nt(act[1, view_rows(src_v), :], sides[1]))
            over_chunks(body)

    def backward_colsplit(act, own, got, emit, ready):
        for v in subs:
            ready[v]()

            def body(j):
                sides = []
                zz, y0 = lax.div(j, PAIR), lax.rem(j, PAIR) * PAIR
                for ref, z in ((own, z_own + zz), (got, zz)):
                    bands = [lanes_of(ref[z, yy, t // PAIR, t % PAIR] for t in range(HALF_BLOCKS)) for yy in (y0, y0 + 1)]
                    sides.append(jnp.concatenate(bands, axis=0))
                emit(j, v, dot_nt(act[core, view_rows(v), :], sides[0]) + dot_nt(act[other, view_rows(v), :], sides[1]))
            over_chunks(body)

    def partial_rowsplit(dst, lhs, lhs_rows, rhs, rhs_rows):
        def body(j):
            left = lhs[core, lhs_rows, chunk_cols(j)]
            for hh in subs:
                for t in range(RING):
                    res = dot_tn(left, rhs[hh, rhs_rows, t * quad:(t + 1) * quad])
                    for i in subs:
                        for s in subs:
                            dst[PAIR * hh + t // PAIR, (t % PAIR) * PAIR + i, j, s] = res[s * blk:(s + 1) * blk,
                                                                                         i * blk:(i + 1) * blk]
        over_chunks(body)

    def partial_colsplit(dst, lhs, rhs, hh):
        def body(t):
            left = lhs[hh, :, chunk_cols(t)]
            zz, y0 = PAIR * hh + lax.div(t, PAIR), lax.rem(t, PAIR) * PAIR
            for q in range(RING):
                res = dot_tn(left, rhs[core, :, q * quad:(q + 1) * quad])
                for i, yy in enumerate((y0, y0 + 1)):
                    for s in subs:
                        dst[zz, yy, q, s] = res[i * blk:(i + 1) * blk, s * blk:(s + 1) * blk]
        over_chunks(body)

    def forward_emit(dst, parity):
        def emit(j, v, acc):
            cols = chunk_cols(j)
            dst[view_rows(v), cols] = acc
            put_stat(parity, v, cols, col_sum(acc), col_sum(acc * acc))
        return emit

    def moments(total, slot):
        for v in subs:
            mean = total[first_row(v), :half] * inv_n
            inv = lax.rsqrt(total[second_row(v), :half] * inv_n - mean * mean + BN_EPS)
            sres[slot, first_row(v), :] = mean
            sres[slot, second_row(v), :] = inv

    act_send, act_recv = new_ids('s', PAIR), new_ids('r', 10)

    def share(dst, v):
        region = dst.at[core, view_rows(v), :]
        copy = rcopy(region, region, act_send[v], act_recv.pop(), peer)
        copy.start()
        return copy

    rstep = min(32, vrows)

    def apply_rows(v, fn):
        @pl.loop(0, vrows // rstep)
        def _(i):
            fn(pl.ds(pl.multiple_of(v * vrows + i * rstep, rstep), rstep))

    def activate(src, slot, gain, shift, dst):
        copies = []
        for v in subs:
            mean = sres[slot, first_row(v), :]
            inv = sres[slot, second_row(v), :]

            def fn(rsl, mean=mean, inv=inv):
                norm = (src[rsl, :] - mean) * inv
                if gain is not None:
                    norm = jnp.maximum(gain * norm + shift, NOW)
                dst[core, rsl, :] = norm.astype(BF16)
            apply_rows(v, fn)
            copies.append(share(dst, v))
        plan.work(1)
        plan.pump(plan.now + PAIR)
        return copies

    def received(copies):
        return [copy.wait_recv for copy in copies]

    def sent(copies):
        for copy in copies:
            copy.wait_send()

    def nothing():
        pass

    both = ((0, 0), (1, 1))
    at_once = (nothing, nothing)
    all_rows = pl.ds(0, PAIR * vrows)

    MM = 3.7

    def product(fn, *args):
        plan.expect(plan.now + MM)
        plan.pump(plan.now + STEP)
        fn(*args)
        plan.work(MM)

    product(forward_rowsplit, hx, wg1, wq1, both, forward_emit(u1, 0), at_once)
    moments(stat_sum(0), 0)
    copies = activate(u1, 0, gain1, shift1, xf1)
    sent(q1 + h_copies)
    plan.finish(*gather2)
    product(forward_colsplit, xf1, wg2, forward_emit(u2, 1), received(copies))
    released.append(True)
    for send in held3:
        send()
    sent(copies)
    moments(stat_sum(1), 1)
    copies = activate(u2, 1, gain2, shift2, xf2)
    plan.finish(*gather3)
    for copy in q3:
        copy.wait_recv()
    product(forward_rowsplit, xf2, wg3, wq1, both, forward_emit(u3, 0), received(copies))
    sent(copies)
    moments(stat_sum(0), PAIR)
    copies = activate(u3, PAIR, None, None, zf)
    for copy in copies:
        copy.wait_recv()
    sent(copies)

    for v in subs:
        stat[1, 0, zc, row(v), :half] = col_sum(zf[core, view_rows(v), :].astype(F32))
    zsum_ids = new_ids('s', 1) + new_ids('r', 1)

    def zsum_lane():
        out = []
        yield from stat_steps(1, out)
        zsum[core] = out[0]
        copy = rcopy(zsum.at[core], zsum.at[core], *zsum_ids, peer)
        copy.start()
        yield plan.now + PAIR, {}, NOW
        copy.wait_recv()
        copy.wait_send()

    zsum_group = plan.add([zsum_lane()], first=True)

    partial_rowsplit(part, zf, view_rows(0), zf, view_rows(1))
    lam = lam_ref[0]
    losses = []

    def gradient_of(k, batch):
        def go():
            sub, begin, sizes = batch
            count = sum(sizes)
            rsl = pl.ds(begin, count)
            corr = part[zc, yc, xc, sub, rsl, :] * inv_n
            row_ids = (core * half + xc * quad + (sub * blk + begin)) + lax.broadcasted_iota(jnp.int32, (count, blk), 0)
            diag = row_ids == mid * blk + lax.broadcasted_iota(jnp.int32, (count, blk), 1)
            terms = jnp.where(diag, (1.0 - corr) * (1.0 - corr), lam * corr * corr)
            losses.append(jnp.sum(col_sum(terms), axis=1, keepdims=True))
            wg1[zc, yc, xc, sub, rsl, :] = jnp.where(diag, -2.0 * (1.0 - corr), 2.0 * lam * corr).astype(BF16)
            gather_g.append(plan.add(lanes_g[k], quarter(wg1, wq1, batch, q_send[6 + k], q_recv[6 + k], qg)))
        return go

    gather_g = []
    lanes_g = gather_lanes(wg1, FINE, send_g, recv_w_all)
    scatter_c = [plan.add(lanes, gradient_of(k, FINE[k]))
                 for k, lanes in enumerate(scatter_lanes(part, 0, FINE, send_w_all, recv_c))]
    plan.finish(zsum_group, *scatter_c)

    share_of = []
    sum_b = zsum[lax.div(mid, HALF_BLOCKS), row(SECOND), pl.ds(pl.multiple_of(lax.rem(mid, HALF_BLOCKS) * blk, blk), blk)]
    for s in subs:
        grad = wg1[zc, yc, xc, s].astype(F32)
        both_terms = grad * (part[zc, yc, xc, s] * inv_n)
        sum_a = zsum[core, row(FIRST), pl.ds(pl.multiple_of(xc * quad + s * blk, blk), blk)]
        share_of.append((col_sum((grad.T * sum_a).T) * inv_n, col_sum(both_terms), col_sum((grad * sum_b).T) * inv_n,
                         col_sum(both_terms.T)))
    (c0, c1, r00, r10), (d0, d1, r01, r11) = share_of
    loss_row = jnp.broadcast_to(sum(losses[1:], losses[0]), (1, blk))
    vec[zc, yc] = jnp.concatenate([c0 + d0, c1 + d1, r00, r01, r10, r11, loss_row, loss_row], axis=0)
    vec_send, vec_recv = new_ids('s', 10), new_ids('r', 10)

    def vec_lane():
        ready, pending = NOW, []
        for k, axis in enumerate(AXES[::-1][1:] + AXES[PAIR:]):
            yield ready, {axis: STAT_SIZE}, STEP
            for copy in pending[-1:]:
                copy.wait_recv()
            if axis == 'x':
                plane = [vec[t // RING, t % RING] for t in range(BLOCKS)]
                rest_rows = sum(plane[1:], plane[0])
                vecx[xc] = jnp.concatenate([item[:PAIR] for item in plane] + [rest_rows], axis=0)
            own = {'y': vec.at[zc, yc], 'z': vec.at[zc], 'x': vecx.at[xc]}[axis]
            made = [Fan(axis, lambda off, own=own: (own, own), vec_send[k * 3:], vec_recv[k * 3:])]
            made[0].start()
            ready = plan.send(axis, STAT_SIZE, TWO_HOPS)
            pending.extend(made)
        yield ready, {}, STEP
        for copy in made:
            copy.wait_recv()
        got = [vecx[q] for q in range(RING)]
        vecp[core] = (got[0] + got[1]) + (got[PAIR] + got[3])
        copy = rcopy(vecp.at[core], vecp.at[core], vec_send[9], vec_recv[9], peer)
        copy.start()
        yield plan.now + PAIR, {}, NOW
        copy.wait_recv()
        sent(pending + [copy])

    vec_group = plan.add([vec_lane()], first=True)
    plan.finish(*gather_g)

    def embed_emit(j, v, acc):
        u3[view_rows(v), chunk_cols(j)] = acc * inv_n

    backward_rowsplit(zf, wg1, ((0, 1),), embed_emit, at_once)
    for copy in qg:
        copy.wait_recv()
    forward_rowsplit(zf, wg1, wq1, ((1, 0),), embed_emit, at_once)
    dzf, duf = hx, zf
    plan.work(MM)
    plan.finish(vec_group)
    first_r = PAIR * BLOCKS + PAIR
    dgb[core, :, half:half + blk] = jnp.broadcast_to(vecp[core, row(first_r + RING), :], (RING, blk))
    mine = pl.ds(pl.multiple_of(BLOCKS * core, BLOCKS), BLOCKS)
    both_cores = vecp[0, mine, :] + vecp[1, mine, :]
    sums = [[lanes_of(vecx[q, row(first_r + PAIR * t + s), :] for q in range(RING) for s in subs) for t in subs],
            [lanes_of(both_cores[row(PAIR * i + t)] for i in range(HALF_BLOCKS)) for t in subs]]
    copies = []
    for v in subs:
        def embed_rows(rsl, mean_g=sums[v][0], mean_gz=sums[v][1], inv=sres[PAIR, second_row(v), :]):
            emb = zf[core, rsl, :].astype(F32)
            dzf[core, rsl, :] = (inv * (u3[rsl, :] - (mean_g + emb * mean_gz) * inv_n)).astype(BF16)
        apply_rows(v, embed_rows)
        copies.append(share(dzf, v))
    for copy in copies:
        copy.wait_recv()
    sent(copies + q2 + q3 + qg)

    out_ids = {(slot, s): (new_ids('s', 5), new_ids('r', 5)) for slot in range(3) for s in subs}

    def publish(slot, s):
        size = PAIR * blk * blk * PAIR
        up, down = device('x', 1), device('x', 3)
        sid, rid = out_ids[slot, s]
        own = out_w.at[slot, core, xc, s]
        made = [rcopy(own, own, sid[FIRST], rid[FIRST], up), rcopy(own, own, sid[SECOND], rid[SECOND], down)]
        yield NOW, {'x': size}, NOW
        for copy in made:
            copy.start()
        yield plan.send('x', size), {'x': size / PAIR}, NOW
        for k, (off, target) in enumerate(((3, up), (1, down))):
            made[k].wait_recv()
            src = out_w.at[slot, core, near['x'][off], s, pl.ds(k * blk // PAIR, blk // PAIR), :]
            made.append(rcopy(src, src, sid[PAIR + k], rid[PAIR + k], target))
            made[-1].start()
        yield plan.send('x', size / PAIR), {}, NOW
        made[PAIR].wait_recv()
        made[3].wait_recv()
        own = out_w.at[slot, core, :, s]
        made.append(rcopy(own, own, sid[RING], rid[RING], peer))
        made[-1].start()
        yield plan.now + PAIR, {}, NOW
        made[-1].wait_recv()
        sent(made)

    published = []

    def result(slot, buf, s, groups):
        def go():
            if not any(group['left'] for group in groups):
                out_w[slot, core, xc, s] = buf[zc, yc, xc, s]
                published.append(plan.add([publish(slot, s)], first=True))
        return go

    def layer_emit(src, slot, parity, k):
        def emit(j, v, acc):
            cols = chunk_cols(j)
            norm = (src[view_rows(v), cols] - sres[slot, first_row(v), cols]) * sres[slot, second_row(v), cols]
            lin = sres[3, row(k), cols] * norm + sres[3, row(k + 1), cols]
            grad = jnp.where(lin > 0, acc, NOW)
            u3[view_rows(v), cols] = grad
            put_stat(parity, v, cols, col_sum(grad), col_sum(grad * norm))
        return emit

    def layer_rows(src, slot, k, total, v, store):
        sum_lin, sum_norm = total[first_row(v), :half], total[second_row(v), :half]
        mean, inv = sres[slot, first_row(v), :], sres[slot, second_row(v), :]
        scale = sres[3, row(k), :] * inv

        def fn(rsl):
            norm = (src[rsl, :] - mean) * inv
            store(rsl, (scale * (u3[rsl, :] - (sum_lin + norm * sum_norm) * inv_n)).astype(BF16))
        apply_rows(v, fn)

    def affine_grads(total, k):
        dgb[core, row(k), :half] = total[second_row(FIRST), :half] + total[second_row(SECOND), :half]
        dgb[core, row(k + 1), :half] = total[first_row(FIRST), :half] + total[first_row(SECOND), :half]

    def add_scatter(slot, buf, batches, lanes):
        groups = {s: [] for s in subs}
        for batch, batch_lanes in zip(batches, lanes):
            s = batch[0]
            groups[s].append(plan.add(batch_lanes, result(slot, buf, s, groups[s])))
        return groups[0] + groups[1]

    partial_rowsplit(part, xf2, all_rows, dzf, all_rows)
    plan.work(3)
    scatter_3 = add_scatter(PAIR, part, BACK, scatter_lanes(part, 0, BACK, send_w_all, recv_c, give=True))
    product(backward_rowsplit, dzf, wg3, both, layer_emit(u2, 1, 0, PAIR), at_once)
    total = stat_sum(0)
    affine_grads(total, 0)
    copies = []
    for v in subs:
        def put_du2(rsl, value):
            duf[core, rsl, :] = value
        layer_rows(u2, 1, PAIR, total, v, put_du2)
        copies.append(share(duf, v))
    plan.work(1)
    plan.pump(plan.now + PAIR)
    for copy in q2:
        copy.wait_recv()
    product(backward_colsplit, duf, wg2, wq2, layer_emit(u1, 0, 1, 0), received(copies))
    sent(copies)
    scatter_2 = []

    def part2_lane(hh):
        yield NOW, {}, 1.9
        partial_colsplit(part2, xf1, duf, hh)
        plan.work(1.9)

    def start_2():
        scatter_2.extend(add_scatter(1, part2, BACK, scatter_lanes(part2, 1, BACK, send_g, recv_w_all, take=True)))

    part2_group = plan.add([part2_lane(hh) for hh in subs], start_2, first=True)
    total = stat_sum(1)
    plan.finish(part2_group)
    affine_grads(total, PAIR)
    dg_send, dg_recv = new_ids('s', 1)[0], new_ids('r', 1)[0]
    dg_copy = rcopy(dgb.at[core], dgb.at[core], dg_send, dg_recv, peer)
    dg_copy.start()

    for v in subs:
        def put_du1(rsl, value, v=v):
            start = rsl.start - v * vrows
            r = pl.multiple_of(lax.rem(start, rows), min(rstep, rows))
            c = lax.div(start, rows)
            for i in range(HALF_BLOCKS):
                du1[i // RING, i % RING, c, v, pl.ds(r, rstep), :] = value[:, i * blk:(i + 1) * blk]
        layer_rows(u1, 0, 0, total, v, put_du1)

    a2a_recv, a2a_send = new_ids('r', BLOCKS), new_ids('s', BLOCKS)

    slots = (hx, zf, xf1, xf2)
    per = RING * rows

    turn = (0, 1, 3, PAIR)

    def h_fetch(chunk):
        at = chunk % RING
        begin = pl.multiple_of(near['z'][turn[chunk // PAIR]] * per, per)
        made = [pltpu.make_async_copy((h_a, h_b)[chunk % PAIR].at[pl.ds(begin, per), pl.ds(kh * half, half)],
                                      slots[at].at[kh], hsem.at[at * PAIR + kh]) for kh in subs]
        for copy in made:
            copy.start()
        return made

    fetches = [h_fetch(chunk) for chunk in range(RING)]
    own_half = lax.div(mid, HALF_BLOCKS)
    self_out = jnp.where(own_half == core, PAIR * (mid - HALF_BLOCKS * core) + core, -1)
    self_in = jnp.where(own_half == core, mid, -1)
    a2a_home, a2a_sem = a2a.at[zc, yc], rsem.at[a2a_recv[0] + mid]

    def block(k):
        return du1.at[lax.div(k, HALF_BLOCKS), wrap(lax.div(k, PAIR)), lax.rem(k, PAIR)]

    @pl.loop(0, BLOCKS)
    def _(k):
        @pl.when(self_out == k)
        def _():
            a2a_home[...] = block(k)[...]

        @pl.when(self_out != k)
        def _():
            pltpu.make_async_remote_copy(
                src_ref=block(k), dst_ref=a2a_home, send_sem=ssem.at[a2a_send[0] + k], recv_sem=a2a_sem,
                device_id=(HALF_BLOCKS * core + lax.div(k, PAIR), x_base + lax.rem(k, PAIR)),
                device_id_type=MESH_ID).start()

    plan.work(1)
    arrived = max([plan.send(axis, 32 * rows * blk, TWO_HOPS) for axis in 'zy'])
    arrivals = [arrived - off for off in (4, PAIR, 1, 0)]
    for k in range(RING):
        plan.pump(arrivals[k])
        plan.until(arrivals[k])
        zz = near['z'][turn[k]]
        @pl.loop(0, RING)
        def _(i):
            @pl.when(self_in != zz * RING + i)
            def _():
                pltpu.make_async_copy(a2a.at[zz, i], a2a.at[zz, i], rsem.at[a2a_recv[0] + zz * RING + i]).wait()
        for v in subs:
            chunk = PAIR * k + v
            at = chunk % RING
            for copy in fetches[chunk]:
                copy.wait()
            grad = jnp.concatenate([a2a[zz, i, v] for i in range(RING)], axis=0)
            for kh in subs:
                for q in range(RING):
                    res = dot_tn(grad, slots[at][kh, :, q * quad:(q + 1) * quad])
                    spot = (slice(kh * blk, (kh + 1) * blk), slice(q * quad, (q + 1) * quad))
                    u2[spot] = res + u2[spot] if chunk else res
            if chunk < RING:
                fetches.append(h_fetch(chunk + RING))
        plan.work(1)
    @pl.loop(0, BLOCKS)
    def _(k):
        @pl.when(self_out != k)
        def _():
            pltpu.make_async_copy(block(k), block(k), ssem.at[a2a_send[0] + k]).wait()

    x_recv, x_send = new_ids('r', RING), new_ids('s', RING)

    def strip(k, cols=pl.ds(0, half)):
        return u2.at[pl.ds(pl.multiple_of(k * blk, blk), blk), cols]

    swap = rcopy(strip(other), strip(PAIR), x_send[0], x_recv[0], peer)
    swap.start()
    plan.need['x'] = plan.now + 3.0
    plan.pump(plan.now + PAIR)
    swap.wait_recv()
    swap.wait_send()
    strip(core)[...] = strip(core)[...] + strip(PAIR)[...]
    shifts = [Fan('x', lambda off: (strip(core, chunk_cols(wrap(xc + off))), strip(3, chunk_cols(off))), x_send[1:],
                  x_recv[1:])]
    for copy in shifts:
        copy.start()
    arrived = plan.send('x', PAIR * quad * blk * RING, TWO_HOPS)
    plan.pump(arrived)
    for copy in shifts:
        copy.wait_recv()
    got = [strip(3, chunk_cols(off))[...] for off in OTHERS]
    piece_sum = (strip(core, chunk_cols(xc))[...] + got[0]) + (got[1] + got[2])
    for s in subs:
        out_w[0, core, xc, s] = piece_sum[:, s * blk:(s + 1) * blk].T
    sent(shifts)
    plan.need['x'] = FAR
    published.append(plan.add([publish(0, s) for s in subs], first=True))
    plan.finish(*scatter_3, *scatter_2)
    plan.finish(*published)
    dg_copy.wait_recv()
    dg_copy.wait_send()
    w_copy = pltpu.make_async_copy(out_w, dw_out, lsem.at[0])
    w_copy.start()
    small_out[...] = dgb[...]
    w_copy.wait()


def split_kernel(blk, dw_ref, small_ref, loss_out, dw1_out, dw2_out, dw3_out, dg1_out, db1_out, dg2_out, db2_out,
                 stage, sem_in, sem_out):
    half = HALF_BLOCKS * blk
    mid = lax.axis_index('model')
    loads = []
    for slot in range(3):
        loads.append(pltpu.make_async_copy(dw_ref.at[slot], stage.at[slot], sem_in.at[slot]))
        loads[-1].start()
    loss_out[...] = small_ref[0, FIRST:SECOND, half:half + 1] + small_ref[1, FIRST:SECOND, half:half + 1]
    for hh in range(PAIR):
        dg2_out[:, hh * half:(hh + 1) * half] = small_ref[hh, FIRST:SECOND, :half]
        db2_out[:, hh * half:(hh + 1) * half] = small_ref[hh, SECOND:PAIR, :half]
    mcols = pl.ds(pl.multiple_of(lax.rem(mid, HALF_BLOCKS) * blk, blk), blk)
    dg1_out[...] = small_ref[lax.div(mid, HALF_BLOCKS), 2:3, mcols]
    db1_out[...] = small_ref[lax.div(mid, HALF_BLOCKS), 3:4, mcols]
    stores = []
    for slot in range(3):
        loads[slot].wait()
        for t in range(BLOCKS):
            begin = pl.ds(t * blk, blk)
            dst = (dw1_out.at[begin, :], dw2_out.at[:, begin], dw3_out.at[begin, :])[slot]
            stores.append(pltpu.make_async_copy(stage.at[slot, t // HALF_BLOCKS, (t // PAIR) % RING, t % PAIR], dst,
                                                sem_out.at[len(stores)]))
            stores[-1].start()
    for copy in stores:
        copy.wait()


def build_call(blk, rows, total_rows, vmem_limit):
    dim, half = BLOCKS * blk, HALF_BLOCKS * blk
    trows = RING * rows
    pieces = (RING, RING, RING, PAIR, blk, blk)
    got = (PAIR, RING, RING, PAIR, blk, blk)
    act = pltpu.VMEM((PAIR, trows, half), BF16)
    pre = pltpu.VMEM((trows, half), F32)
    bank = (PAIR, RING, PAIR, blk, blk)
    dma = pltpu.SemaphoreType.DMA
    scratch = [
        act, pre, pre, pre, act, act, act,
        pltpu.VMEM(pieces, BF16), pltpu.VMEM(got, BF16), pltpu.VMEM(pieces, BF16), pltpu.VMEM(got, BF16),
        pltpu.VMEM(pieces, BF16),
        pltpu.VMEM(pieces, F32), pltpu.VMEM(pieces, F32),
        pltpu.VMEM((PAIR, 6, RING, PAIR, blk, blk), F32), pltpu.VMEM((PAIR, PAIR, 6, PAIR, blk, blk), F32),
        pltpu.VMEM((PAIR, PAIR, 3, blk, blk), F32),
        pltpu.VMEM((RING, RING, HALF_BLOCKS, blk), F32),
        pltpu.VMEM((PAIR, 3, RING, RING, half), F32), pltpu.VMEM((RING, RING, half), F32),
        pltpu.VMEM((PAIR, RING, half + blk), F32),
        pltpu.VMEM((PAIR, RING, half), F32), pltpu.VMEM((RING, RING, HALF_BLOCKS, blk), F32),
        pltpu.VMEM((RING, 40, blk), F32), pltpu.VMEM((PAIR, 40, blk), F32),
        pltpu.VMEM((PAIR, RING, PAIR, PAIR, rows, blk), BF16), pltpu.VMEM((RING, RING, PAIR, rows, blk), BF16),
        pltpu.VMEM((3,) + bank, F32),
        dma((N_SEND,)), dma((N_RECV,)), dma((BLOCKS,)), dma((HALF_BLOCKS,)), pltpu.SemaphoreType.REGULAR((12,)),
    ]
    anyspec = pl.BlockSpec(memory_space=pl.ANY)
    vmem = pl.BlockSpec(memory_space=pltpu.VMEM)
    smem = pl.BlockSpec(memory_space=pltpu.SMEM)
    packed = jax.ShapeDtypeStruct((3,) + bank, F32)
    step_call = pl.pallas_call(
        functools.partial(mega_kernel, (blk, rows, total_rows)),
        out_shape=[packed, jax.ShapeDtypeStruct((PAIR, RING, half + blk), F32)],
        in_specs=[anyspec] * 7 + [vmem, vmem, smem],
        out_specs=[anyspec, vmem],
        scratch_shapes=scratch,
        compiler_params=pltpu.CompilerParams(collective_id=0, has_side_effects=True, vmem_limit_bytes=vmem_limit),
        name='barlow_step',
    )

    def line(n):
        return jax.ShapeDtypeStruct((1, n), F32)

    tall, wide = jax.ShapeDtypeStruct((dim, blk), F32), jax.ShapeDtypeStruct((blk, dim), F32)
    split_call = pl.pallas_call(
        functools.partial(split_kernel, blk),
        out_shape=[line(1), tall, wide, tall, line(blk), line(blk), line(dim), line(dim)],
        in_specs=[anyspec, vmem],
        out_specs=[vmem, anyspec, anyspec, anyspec, vmem, vmem, vmem, vmem],
        scratch_shapes=[pltpu.VMEM((3,) + bank, F32), dma((3,)), dma((48,))],
        name='split_results',
    )

    def call(*args):
        return split_call(*step_call(*args))

    return call


def solution(mesh):
    data_size = mesh.shape['data']

    def shard_body(h_a, h_b, w_one, w_two, w_three, g_one, b_one, g_two, b_two, lam_off):
        group_rows = h_a.shape[0]
        blk = w_three.shape[1]
        rows = group_rows // BLOCKS
        call = build_call(blk, rows, group_rows * data_size, 67_000_000)
        outs = call(h_a, h_b, w_one, w_two, w_three, g_one.reshape(1, -1), b_one.reshape(1, -1),
                    g_two.reshape(1, -1), b_two.reshape(1, -1), lam_off)
        loss, dw1, dw2, dw3, dg1, db1, dg2, db2 = outs
        return (loss.reshape(1), dw1, dw2, dw3, dg1.reshape(-1), db1.reshape(-1), dg2.reshape(-1), db2.reshape(-1))

    in_specs = (P('data', None), P('data', None), P(None, 'model'), P('model', None), P(None, 'model'),
                P('model'), P('model'), P(), P(), P())
    out_specs = (P(), P(None, 'model'), P('model', None), P(None, 'model'), P('model'), P('model'), P(), P())
    return jax.shard_map(shard_body, mesh=mesh, in_specs=in_specs, out_specs=out_specs, check_vma=False)
```

```python
import functools

import jax
import jax.numpy as jnp
from jax import lax
from jax.experimental import pallas as pl
from jax.experimental.pallas import tpu as pltpu
from jax.sharding import PartitionSpec as P

BN_EPS = 1e-5
MESH_ID = pl.DeviceIdType.MESH
RING = 4
PAIR = 2
AXES = ('z', 'y', 'x')
ORDERS = (('x', 'y', 'z'), ('y', 'z', 'x'), ('z', 'x', 'y'))
COARSE = ((0, 0, (40, 48, 40)), (1, 0, (48, 40, 40)))
FINE = COARSE
BACK = COARSE
OTHERS = (1, 2, 3)
N_SEND = 560
N_RECV = 560
BYTES_PER_US = 46600.0
HOP = 1.9
TWO_HOPS = 2.7
BACKLOG = 5.0
SMALL = 60000
FAR = 1e9
F32 = jnp.float32
BF16 = jnp.bfloat16
WHOLE = slice(None)
FIRST, SECOND = 0, 1
BLOCKS, HALF_BLOCKS = 16, 8
NOW = 0.0
STEP = 0.2
STAT_SIZE = 32768


def dot_nn(a, b):
    return lax.dot_general(a, b, (((1,), (0,)), ((), ())), preferred_element_type=F32)


def dot_nt(a, b):
    return lax.dot_general(a, b, (((1,), (1,)), ((), ())), preferred_element_type=F32)


def dot_tn(a, b):
    return lax.dot_general(a, b, (((0,), (0,)), ((), ())), preferred_element_type=F32)


def col_sum(value):
    return jnp.sum(value, axis=0, keepdims=True)


def lanes_of(values):
    return jnp.concatenate(list(values), axis=1)


def wrap(value):
    return lax.rem(value, RING)


class Plan:
    def __init__(self):
        self.now = 0.0
        self.free = dict.fromkeys(AXES, 0.0)
        self.need = [dict.fromkeys(AXES, FAR) for _ in range(PAIR)]
        self.lanes = []
        self.first = None

    def work(self, us):
        self.now += us

    def until(self, when):
        self.now = max(self.now, when)

    def send(self, axis, size, flight=HOP):
        self.free[axis] = max(self.free[axis], self.now) + size / BYTES_PER_US
        return self.free[axis] + flight

    def add(self, gens, then=None, first=False):
        group = {'left': 0, 'then': then, 'done': NOW, 'first': first}
        made = []
        for gen in gens:
            group['left'] += 1
            made.append([gen, next(gen), group])
        self.lanes = made + self.lanes if first else self.lanes + made
        return group

    def start_of(self, lane):
        ready, loads, _ = lane[1]
        start = max(self.now, ready() if callable(ready) else ready)
        if self.first is not None and lane[2] not in self.first and max(loads.values(), default=0) > SMALL:
            return FAR
        if not lane[2]['first']:
            for axis in loads:
                start = max(start, self.free[axis] - BACKLOG)
        for axis, size in loads.items():
            needed = min(need[axis] for need in self.need)
            if not lane[2]['first'] and max(self.free[axis], start) + size / BYTES_PER_US > needed + 1.0:
                return FAR
        return start

    def advance(self, limit):
        best, begin = None, limit
        for lane in self.lanes:
            start = self.start_of(lane)
            if start < begin and start + lane[1][2] < limit + 1.0:
                best, begin = lane, start
        if best is None:
            return False
        self.until(begin)
        info = next(best[0], None)
        if info is not None:
            best[1] = info
            return True
        self.lanes = [lane for lane in self.lanes if lane is not best]
        group = best[2]
        group['left'] -= 1
        group['done'] = self.now
        if not group['left'] and group['then'] is not None:
            group['then']()
        return True

    def pump(self, limit):
        while self.advance(limit):
            pass

    def finish(self, *groups, alone=False):
        self.first = groups if alone else None
        while any(group['left'] for group in groups):
            if not self.advance(FAR):
                self.clear()
        self.first = None

    def clear(self):
        for need in self.need:
            need.update(dict.fromkeys(AXES, FAR))

    def expect(self, v, when, axes=AXES):
        for axis in AXES:
            self.need[v][axis] = FAR
        for axis in axes:
            self.need[v][axis] = when
            when += 3.6


def mega_kernel(cfg, h_a, h_b, w_one, w_two, w_three, g_one, b_one, g_two, b_two, lam_ref,
                out_w, small_out,
                hx, u1, u2, u3, xf1, xf2, zf, wg1, wq1, wg2, wq2, wg3, part, part2, rv1, rv2, rv3,
                gbuf, stat, sres, dgb, zsum, vec, vecx, vecp, du1, a2a, ssem, rsem, lsem, hsem, credit):
    blk, rows, total_rows = cfg
    plan = Plan()
    half = HALF_BLOCKS * blk
    quad = PAIR * blk
    vrows = PAIR * rows
    inv_n = 1.0 / total_rows

    mid = lax.axis_index('model')
    did = lax.axis_index('data')
    core = lax.rem(did, PAIR)
    other = 1 - core
    coord = {'z': lax.div(mid, RING), 'y': wrap(mid), 'x': lax.div(did, PAIR)}
    zc, yc, xc = coord['z'], coord['y'], coord['x']
    near = {axis: [coord[axis]] + [wrap(coord[axis] + off) for off in OTHERS] for axis in AXES}
    z_base, x_base = zc * RING, xc * PAIR
    targets_of = {'z': [(q * RING + yc, did) for q in near['z']], 'y': [(z_base + q, did) for q in near['y']],
                  'x': [(mid, q * PAIR + core) for q in near['x']]}
    peer = (mid, x_base + other)

    def device(axis, off):
        if isinstance(off, int):
            return targets_of[axis][off]
        q = wrap(coord[axis] + off)
        return {'z': (q * RING + yc, did), 'y': (z_base + q, did), 'x': (mid, q * PAIR + core)}[axis]

    class Fan:
        def __init__(self, axis, place, sid, rid):
            def make(off):
                src, dst = place(off)
                return rcopy(src, dst, sid[0] + off - 1, rid[0] + off - 1, device(axis, off))
            self.make = make

        def each(self, action):
            @pl.loop(1, RING)
            def _(off):
                getattr(self.make(off), action)()

        def start(self):
            self.each('start')

        def wait_recv(self):
            self.each('wait_recv')

        def wait_send(self):
            self.each('wait_send')

    z_own, z_other = PAIR * core, PAIR * other
    counters = {'s': 0, 'r': 0, 'l': 0}

    def new_ids(kind, count):
        first = counters[kind]
        counters[kind] = first + count
        assert counters[kind] <= {'s': N_SEND, 'r': N_RECV, 'l': BLOCKS}[kind]
        return list(range(first, first + count))

    def rcopy(src, dst, send_id, recv_id, target):
        return pltpu.make_async_remote_copy(src_ref=src, dst_ref=dst, send_sem=ssem.at[send_id],
                                            recv_sem=rsem.at[recv_id], device_id=target, device_id_type=MESH_ID)

    def bands(batches):
        for sub, begin, sizes in batches:
            for colour, size in enumerate(sizes):
                yield sub, colour, pl.ds(begin, size), size * blk
                begin += size

    def gather_lane(buf, sub, colour, rsl, cells, sid, rid):
        order = ORDERS[colour]
        size = PAIR * cells

        def region(axis, have, q, part_id=None):
            idx = dict(coord)
            idx[axis] = q
            for name in have:
                idx[name] = WHOLE
            if part_id is not None:
                idx[have[-1]] = pl.ds(PAIR * part_id, PAIR)
            return buf.at[idx['z'], idx['y'], idx['x'], sub, rsl, :]

        axis = order[0]
        yield NOW, {axis: PAIR * size}, NOW
        own = region(axis, (), coord[axis])
        pending = [Fan(axis, lambda off, own=own: (own, own), sid, rid)]
        pending[0].start()
        ready = plan.send(axis, PAIR * size, TWO_HOPS)
        for phase in (1, 2):
            size *= RING
            axis, have = order[phase], order[:phase]
            yield ready, {axis: size}, STEP
            for copy in pending[-PAIR:]:
                copy.wait_recv()
            base = phase * RING - 1
            up, down = device(axis, 1), device(axis, 3)
            own = region(axis, have, coord[axis])
            to_up = rcopy(own, own, sid[base], rid[base], up)
            to_down = rcopy(own, own, sid[base + 1], rid[base + 1], down)
            to_up.start()
            to_down.start()
            yield plan.send(axis, size), {axis: size / PAIR}, STEP
            to_up.wait_recv()
            src = region(axis, have, near[axis][3], 0)
            relay_up = rcopy(src, src, sid[base + 2], rid[base + 2], up)
            relay_up.start()
            to_down.wait_recv()
            src = region(axis, have, near[axis][1], 1)
            relay_down = rcopy(src, src, sid[base + 3], rid[base + 3], down)
            relay_down.start()
            ready = plan.send(axis, size / PAIR)
            pending.extend((to_up, to_down, relay_up, relay_down))
        yield ready, {}, STEP
        for copy in pending[-2:]:
            copy.wait_recv()
        for copy in pending:
            copy.wait_send()

    def lanes_by_batch(make, batches, send_ids, recv_ids, width):
        lanes = []
        for k, found in enumerate(bands(batches)):
            ids = slice(k * width, (k + 1) * width)
            lanes.append(make(k, *found, send_ids[ids], recv_ids[ids]))
        return [lanes[k:k + 3] for k in range(0, len(lanes), 3)]

    def gather_lanes(buf, batches, send_ids, recv_ids):
        return lanes_by_batch(lambda k, *args: gather_lane(buf, *args), batches, send_ids, recv_ids, 11)

    given = {}

    def scatter_lane(buf, bank, give, take, sub, colour, rsl, cells, sid, rid):
        order = ORDERS[colour]
        pending = []
        ready = NOW
        size = cells * 32
        for phase in (0, 1):
            axis = order[phase]
            left = tuple(name for name in AXES if name in order[phase + 1:])
            p = coord[axis]
            base = phase * 6

            def region(q, part_id, axis=axis, left=left):
                idx = dict(coord)
                idx[axis] = q
                for name in left[:-1]:
                    idx[name] = WHOLE
                idx[left[-1]] = pl.ds(PAIR * part_id, PAIR)
                return buf.at[idx['z'], idx['y'], idx['x'], sub, rsl, :]

            def landing(slot, phase=phase):
                if phase:
                    return rv2.at[bank, sub, slot, :, rsl, :]
                return rv1.at[sub, slot, :, :, rsl, :]

            def add(q, part_id, slots, axis=axis, left=left, phase=phase):
                def one(i, j):
                    idx = dict(coord)
                    idx[axis] = q
                    idx[left[-1]] = PAIR * part_id + j
                    if not phase:
                        idx[left[0]] = i
                    total = buf[idx['z'], idx['y'], idx['x'], sub, rsl, :]
                    for slot in slots:
                        total = total + (rv2[bank, sub, slot, j, rsl, :] if phase else rv1[sub, slot, i, j, rsl, :])
                    buf[idx['z'], idx['y'], idx['x'], sub, rsl, :] = total

                if phase:
                    for j in range(PAIR):
                        one(0, j)
                else:
                    @pl.loop(0, RING)
                    def _(i):
                        for j in range(PAIR):
                            one(i, j)

            up, down = device(axis, 1), device(axis, 3)
            p1, p2, p3 = near[axis][1:]
            if phase:
                yield ready, {axis: PAIR * size}, STEP
                finals()
            else:
                yield (ready if take is None else lambda: given.get(take, FAR)), {axis: size}, NOW
                if take is not None:
                    pl.semaphore_wait(credit.at[take], PAIR)
            relay_up = rcopy(region(p2, 1), landing(0), sid[base], rid[base], up)
            relay_down = rcopy(region(p2, 0), landing(1), sid[base + 1], rid[base + 1], down)
            own_up = rcopy(region(p1, 0), landing(2), sid[base + 2], rid[base + 2], up)
            own_down = rcopy(region(p3, 1), landing(3), sid[base + 3], rid[base + 3], down)
            relay_up.start()
            relay_down.start()
            relayed = plan.send(axis, size)
            if not phase:
                yield NOW, {axis: size}, NOW
            own_up.start()
            own_down.start()
            plan.send(axis, size)
            yield relayed, {axis: size}, STEP
            relay_up.wait_recv()
            add(p1, 1, (0,))
            sum_up = rcopy(region(p1, 1), landing(4), sid[base + 4], rid[base + 4], up)
            sum_up.start()
            relay_down.wait_recv()
            add(p3, 0, (1,))
            sum_down = rcopy(region(p3, 0), landing(5), sid[base + 5], rid[base + 5], down)
            sum_down.start()
            ready = plan.send(axis, size)
            size /= RING

            def finals(phase=phase, p=p, add=add, own_up=own_up, own_down=own_down, sum_up=sum_up, sum_down=sum_down,
                       up=up, down=down):
                own_up.wait_recv()
                sum_down.wait_recv()
                add(p, 0, (2, 5))
                own_down.wait_recv()
                sum_up.wait_recv()
                add(p, 1, (3, 4))
                if give is not None and not phase:
                    given[give] = plan.now + 1.0
                    for target in (up, down):
                        pl.semaphore_signal(credit.at[give], device_id=target, device_id_type=MESH_ID)

            pending.extend((relay_up, relay_down, own_up, own_down, sum_up, sum_down))
        axis = order[2]
        size *= RING
        yield ready, {axis: size}, STEP
        finals()
        base = 12

        def spot(off):
            idx = dict(coord)
            idx[axis] = wrap(coord[axis] + off)
            return buf.at[idx['z'], idx['y'], idx['x'], sub, rsl, :], rv3.at[bank, sub, off - 1, rsl, :]

        last = [Fan(axis, spot, sid[base:], rid[base:])]
        last[0].start()
        yield plan.send(axis, size, TWO_HOPS), {}, STEP
        for copy in last:
            copy.wait_recv()
        got = [rv3[bank, sub, k, rsl, :] for k in range(3)]
        buf[zc, yc, xc, sub, rsl, :] = (buf[zc, yc, xc, sub, rsl, :] + got[0]) + (got[1] + got[2])
        for copy in pending + last:
            copy.wait_send()

    def scatter_lanes(buf, bank, batches, send_ids, recv_ids, give=False, take=False):
        return lanes_by_batch(lambda k, *args: scatter_lane(buf, bank, k if give else None, k if take else None, *args),
                              batches, send_ids, recv_ids, 15)

    released = []

    def quarter(src, dst, batch, send_id, recv_id, made, held=None):
        sub, begin, sizes = batch
        rsl = pl.ds(begin, sum(sizes))

        def send():
            if held is not None and not released:
                held.append(send)
                return
            copy = rcopy(src.at[pl.ds(z_other, PAIR), :, :, sub, rsl, :], dst.at[:, :, :, sub, rsl, :], send_id, recv_id,
                         peer)
            copy.start()
            made.append(copy)
        return send

    stat_recv = [[new_ids('r', 9) for _ in range(PAIR)] for _ in range(PAIR)]
    stat_send = [new_ids('s', 9) for _ in range(PAIR)]

    def stat_steps(parity, v, out):
        pending, ready = [], plan.now
        for d, axis in enumerate(AXES):
            plan.expect(v, ready, AXES[d:])
            yield ready, {axis: STAT_SIZE / PAIR}, STEP
            if d:
                stat[parity, v, d, coord[axis]] = gathered_stat(parity, v, d - 1, pending)
            own = stat.at[parity, v, d, coord[axis]]
            pending.append(Fan(axis, lambda off, own=own: (own, own), stat_send[v][d * 3:], stat_recv[parity][v][d * 3:]))
            pending[-1].start()
            ready = plan.send(axis, STAT_SIZE / PAIR, TWO_HOPS + 0.5)
        plan.expect(v, FAR)
        yield ready, {}, STEP
        out.append(gathered_stat(parity, v, d, pending))
        for copy in pending:
            copy.wait_send()

    def gathered_stat(parity, v, d, pending):
        pending[-1].wait_recv()
        got = [stat[parity, v, d, q] for q in range(RING)]
        return (got[0] + got[1]) + (got[PAIR] + got[3])

    def row(k):
        return slice(k, k + 1)

    def first_row(v):
        return row(PAIR * v)

    def second_row(v):
        return row(PAIR * v + 1)

    def put_stat(parity, v, cols, first, second):
        stat[parity, v, 0, zc, row(FIRST), cols] = first
        stat[parity, v, 0, zc, row(SECOND), cols] = second

    def local(src, dst):
        copy = pltpu.make_async_copy(src, dst, lsem.at[new_ids('l', 1)[0]])
        copy.start()
        return copy

    row0 = pl.multiple_of(core * half + xc * quad, quad)
    subs = range(PAIR)
    w1_loads = [local(w_one.at[pl.ds(row0 + s * blk, blk), :], wg1.at[zc, yc, xc, s]) for s in subs]
    hrow = pl.multiple_of(mid * rows, rows)
    h_ids = [new_ids('s', RING), new_ids('r', RING)]
    h_pairs = []
    for v, h_ref in enumerate((h_a, h_b)):
        for kh in subs:
            h_pairs.append((h_ref.at[pl.ds(hrow, rows), pl.ds(kh * half, half)],
                            hx.at[kh, pl.ds(pl.multiple_of(v * vrows + core * rows, rows), rows), :]))
    more_loads = [local(src, dst) for src, dst in h_pairs]
    more_loads.append(local(g_one, gbuf.at[zc, yc, row(FIRST), :]))
    more_loads.append(local(b_one, gbuf.at[zc, yc, row(SECOND), :]))
    for s in subs:
        more_loads.append(local(w_two.at[:, pl.ds(row0 + s * blk, blk)], wg2.at[zc, yc, xc, s]))
        more_loads.append(local(w_three.at[pl.ds(row0 + s * blk, blk), :], wg3.at[zc, yc, xc, s]))

    barrier = pltpu.get_barrier_semaphore()
    greeted = [device(axis, off) for axis in AXES for off in OTHERS] + [peer]
    for target in greeted:
        pl.semaphore_signal(barrier, device_id=target, device_id_type=MESH_ID)
    pl.semaphore_wait(barrier, len(greeted))

    width = 66
    send_w = [new_ids('s', width) for _ in range(3)]
    recv_w = [new_ids('r', width) for _ in range(3)]
    send_w_all, recv_w_all = sum(send_w, []), sum(recv_w, [])
    send_g, recv_c = new_ids('s', 180), new_ids('r', 180)
    q_send, q_recv = new_ids('s', 10), new_ids('r', 10)
    q1, q2, q3, qg, held3 = [], [], [], [], []

    def add_gather(buf, dst, batches, send_ids, recv_ids, quarter_at, made, held=None):
        return [plan.add(lanes, quarter(buf, dst, batch, q_send[quarter_at + k], q_recv[quarter_at + k], made, held))
                for k, (batch, lanes) in enumerate(zip(batches, gather_lanes(buf, batches, send_ids, recv_ids)))]

    gb_recv = new_ids('r', 6)

    def gain_lane():
        ready, sent_copies = NOW, []
        for k, axis, own in ((0, 'y', gbuf.at[zc, yc]), (3, 'z', gbuf.at[zc])):
            yield ready, {axis: STAT_SIZE}, NOW
            for copy in sent_copies:
                copy.wait_recv()
            made = [Fan(axis, lambda off, own=own: (own, own), stat_send[0][k:], gb_recv[k:])]
            made[0].start()
            ready = plan.send(axis, STAT_SIZE, TWO_HOPS)
            sent_copies.extend(made)
        yield ready, {}, NOW
        for copy in made:
            copy.wait_recv()
        for copy in sent_copies:
            copy.wait_send()

    for copy in w1_loads:
        copy.wait()
    gather1 = add_gather(wg1, wq1, COARSE, send_w[0], recv_w[0], 0, q1)
    plan.pump(0.1)
    h_copies = [rcopy(src, dst, h_ids[0][k], h_ids[1][k], peer) for k, (src, dst) in enumerate(h_pairs)]
    for copy in h_copies:
        copy.start()
    for copy in more_loads:
        copy.wait()
    gather1.append(plan.add([gain_lane()], first=True))
    gather2 = add_gather(wg2, wq2, COARSE, send_w[1], recv_w[1], PAIR, q2)
    plan.finish(*gather1, alone=True)
    gather3 = add_gather(wg3, wq1, COARSE, send_w[PAIR], recv_w[PAIR], RING, q3, held3)
    def gathered(k):
        return lanes_of(gbuf[z, i, row(k), :] for z in (z_own, z_own + 1) for i in range(RING))

    my_cols = pl.ds(pl.multiple_of(core * half, half), half)

    def view_rows(v):
        return pl.ds(v * vrows, vrows)

    def chunk_cols(j):
        return pl.ds(pl.multiple_of(j * quad, quad), quad)

    def over_chunks(fn):
        pl.loop(0, RING)(fn)

    def forward_rowsplit(act, own, got, views, emit):
        for v, src_v in views:

            def body(j):
                zz, y0 = lax.div(j, PAIR), lax.rem(j, PAIR) * PAIR
                sides = [lanes_of(ref[z, yy].reshape(half, blk) for yy in (y0, y0 + 1))
                         for ref, z in ((own, z_own + zz), (got, zz))]
                emit(j, v, dot_nn(act[core, view_rows(src_v), :], sides[0])
                     + dot_nn(act[other, view_rows(src_v), :], sides[1]))
            over_chunks(body)

    def forward_colsplit(act, own, views, emit):
        for v, _ in views:

            def body(j):
                sides = [lanes_of(own[PAIR * hh:PAIR * hh + PAIR, :, j, s].reshape(half, blk) for s in subs)
                         for hh in subs]
                emit(j, v, dot_nn(act[0, view_rows(v), :], sides[0]) + dot_nn(act[1, view_rows(v), :], sides[1]))
            over_chunks(body)

    def backward_rowsplit(act, own, views, emit):
        for v, src_v in views:

            def body(j):
                sides = [lanes_of(own[PAIR * hh + i // RING, i % RING, j].reshape(quad, blk) for i in range(HALF_BLOCKS))
                         for hh in subs]
                emit(j, v, dot_nt(act[0, view_rows(src_v), :], sides[0])
                     + dot_nt(act[1, view_rows(src_v), :], sides[1]))
            over_chunks(body)

    def backward_colsplit(act, own, got, views, emit):
        for v, _ in views:

            def body(j):
                sides = []
                zz, y0 = lax.div(j, PAIR), lax.rem(j, PAIR) * PAIR
                for ref, z in ((own, z_own + zz), (got, zz)):
                    bands = [lanes_of(ref[z, yy, t // PAIR, t % PAIR] for t in range(HALF_BLOCKS)) for yy in (y0, y0 + 1)]
                    sides.append(jnp.concatenate(bands, axis=0))
                emit(j, v, dot_nt(act[core, view_rows(v), :], sides[0]) + dot_nt(act[other, view_rows(v), :], sides[1]))
            over_chunks(body)

    def partial_rowsplit(dst, lhs, lhs_rows, rhs, rhs_rows):
        def body(j):
            left = lhs[core, lhs_rows, chunk_cols(j)]
            for hh in subs:
                for t in range(RING):
                    res = dot_tn(left, rhs[hh, rhs_rows, t * quad:(t + 1) * quad])
                    for i in subs:
                        for s in subs:
                            dst[PAIR * hh + t // PAIR, (t % PAIR) * PAIR + i, j, s] = res[s * blk:(s + 1) * blk,
                                                                                         i * blk:(i + 1) * blk]
        over_chunks(body)

    def partial_colsplit(dst, lhs, rhs, hh):
        def body(t):
            left = lhs[hh, :, chunk_cols(t)]
            zz, y0 = PAIR * hh + lax.div(t, PAIR), lax.rem(t, PAIR) * PAIR
            for q in range(RING):
                res = dot_tn(left, rhs[core, :, q * quad:(q + 1) * quad])
                for i, yy in enumerate((y0, y0 + 1)):
                    for s in subs:
                        dst[zz, yy, q, s] = res[i * blk:(i + 1) * blk, s * blk:(s + 1) * blk]
        over_chunks(body)

    def forward_emit(dst, parity):
        def emit(j, v, acc):
            cols = chunk_cols(j)
            dst[view_rows(v), cols] = acc
            put_stat(parity, v, cols, col_sum(acc), col_sum(acc * acc))
        return emit

    def moments(total, slot, v):
        mean = total[row(FIRST)] * inv_n
        inv = lax.rsqrt(total[row(SECOND)] * inv_n - mean * mean + BN_EPS)
        sres[slot, first_row(v), :] = mean
        sres[slot, second_row(v), :] = inv

    act_send, act_recv = new_ids('s', PAIR), new_ids('r', 10)

    def share(dst, v):
        region = dst.at[core, view_rows(v), :]
        copy = rcopy(region, region, act_send[v], act_recv.pop(), peer)
        copy.start()
        return copy

    rstep = min(32, vrows)

    def apply_rows(v, fn):
        @pl.loop(0, vrows // rstep)
        def _(i):
            fn(pl.ds(pl.multiple_of(v * vrows + i * rstep, rstep), rstep))

    def activate(src, slot, v, gain, shift, dst):
        mean = sres[slot, first_row(v), :]
        inv = sres[slot, second_row(v), :]

        def fn(rsl):
            norm = (src[rsl, :] - mean) * inv
            if gain is not None:
                norm = jnp.maximum(gain[...] * norm + shift[...], NOW)
            dst[core, rsl, :] = norm.astype(BF16)
        apply_rows(v, fn)
        return share(dst, v)

    def nothing():
        pass

    def sent(copies):
        for copy in copies:
            copy.wait_send()

    all_rows = pl.ds(0, PAIR * vrows)
    MM = 1.85
    SHARE = 2.2
    occurred = set()

    def once(name, fn):
        if name not in occurred:
            occurred.add(name)
            fn()

    def after(groups, extra=NOW):
        def ready():
            return FAR if any(group['left'] for group in groups) else max(group['done'] for group in groups) + extra
        return ready

    def at_last(*readies):
        return lambda: max(ready() if callable(ready) else ready for ready in readies)

    shares = {}

    def dense(v, name, ready, before, product, src, slot, parity, gain, shift, dst):
        plan.expect(v, FAR)
        yield ready, {}, MM
        before()
        product(v)
        plan.work(MM)
        out = []
        yield from stat_steps(parity, v, out)
        moments(out[0], slot, v)
        copy = activate(src, slot, v, gain, shift, dst)
        plan.work(0.5)
        yield plan.now + SHARE, {}, NOW
        copy.wait_recv()
        copy.wait_send()
        shares[name, v] = True

    zsum_ids = [new_ids('s', 1) + new_ids('r', 1) for _ in subs]

    def settle_h():
        for copy in h_copies:
            copy.wait_recv()
        for copy in h_copies:
            copy.wait_send()
        for copy in q1:
            copy.wait_recv()
        for copy in q1:
            copy.wait_send()
        gains = (gathered(FIRST), gathered(SECOND), g_two[:, my_cols], b_two[:, my_cols])
        for k, value in enumerate(gains):
            sres[3, row(k), :] = value

    def release():
        released.append(True)
        for send in held3:
            send()

    def settle_q3():
        for copy in q3:
            copy.wait_recv()

    def forward_lane(v):
        views = ((v, v),)
        yield from dense(v, 1, after(gather1, 3.0), lambda: once('h', settle_h),
                         lambda v: forward_rowsplit(hx, wg1, wq1, views, forward_emit(u1, 0)), u1, 0, 0,
                         sres.at[3, row(FIRST)], sres.at[3, row(SECOND)], xf1)
        if (1, 1 - v) in shares:
            release()
        yield from dense(v, PAIR, after(gather2), nothing,
                         lambda v: forward_colsplit(xf1, wg2, views, forward_emit(u2, 1)), u2, 1, 1,
                         sres.at[3, row(PAIR)], sres.at[3, row(3)], xf2)
        yield from dense(v, 3, lambda: after(gather3, 3.0)() if len(q3) == PAIR else FAR, lambda: once('q3', settle_q3),
                         lambda v: forward_rowsplit(xf2, wg3, wq1, views, forward_emit(u3, 0)), u3, PAIR, 0,
                         None, None, zf)
        plan.add([zsum_lane(v)], summed, first=True)

    def summed():
        shares['sums', len(shares)] = True

    def zsum_lane(v):
        yield NOW, {}, STEP
        stat[1, v, 0, zc, row(FIRST), :] = col_sum(zf[core, view_rows(v), :].astype(F32))
        stat[1, v, 0, zc, row(SECOND), :] = jnp.zeros((1, half), F32)
        out = []
        yield from stat_steps(1, v, out)
        zsum[core, v] = out[0]
        copy = rcopy(zsum.at[core, v], zsum.at[core, v], *zsum_ids[v], peer)
        copy.start()
        yield plan.now + PAIR, {}, NOW
        copy.wait_recv()
        copy.wait_send()

    forward = plan.add([forward_lane(v) for v in subs], first=True)
    plan.finish(forward)

    partial_rowsplit(part, zf, view_rows(0), zf, view_rows(1))
    lam = lam_ref[0]
    losses = []

    def gradient_of(k, batch):
        def go():
            sub, begin, sizes = batch
            count = sum(sizes)
            rsl = pl.ds(begin, count)
            corr = part[zc, yc, xc, sub, rsl, :] * inv_n
            row_ids = (core * half + xc * quad + (sub * blk + begin)) + lax.broadcasted_iota(jnp.int32, (count, blk), 0)
            diag = row_ids == mid * blk + lax.broadcasted_iota(jnp.int32, (count, blk), 1)
            terms = jnp.where(diag, (1.0 - corr) * (1.0 - corr), lam * corr * corr)
            losses.append(jnp.sum(col_sum(terms), axis=1, keepdims=True))
            wg1[zc, yc, xc, sub, rsl, :] = jnp.where(diag, -2.0 * (1.0 - corr), 2.0 * lam * corr).astype(BF16)
            gather_g.append(plan.add(lanes_g[k], quarter(wg1, wq1, batch, q_send[6 + k], q_recv[6 + k], qg)))
        return go

    gather_g = []
    lanes_g = gather_lanes(wg1, FINE, send_g, recv_w_all)
    scatter_c = [plan.add(lanes, gradient_of(k, FINE[k]))
                 for k, lanes in enumerate(scatter_lanes(part, 0, FINE, send_w_all, recv_c))]
    plan.finish(*scatter_c)
    while sum(name == 'sums' for name, _ in shares) < PAIR:
        plan.advance(FAR)

    share_of = []
    sum_b = zsum[lax.div(mid, HALF_BLOCKS), SECOND, row(FIRST), pl.ds(pl.multiple_of(lax.rem(mid, HALF_BLOCKS) * blk, blk), blk)]
    for s in subs:
        grad = wg1[zc, yc, xc, s].astype(F32)
        both_terms = grad * (part[zc, yc, xc, s] * inv_n)
        sum_a = zsum[core, FIRST, row(FIRST), pl.ds(pl.multiple_of(xc * quad + s * blk, blk), blk)]
        share_of.append((col_sum((grad.T * sum_a).T) * inv_n, col_sum(both_terms), col_sum((grad * sum_b).T) * inv_n,
                         col_sum(both_terms.T)))
    (c0, c1, r00, r10), (d0, d1, r01, r11) = share_of
    loss_row = jnp.broadcast_to(sum(losses[1:], losses[0]), (1, blk))
    vec[zc, yc] = jnp.concatenate([c0 + d0, c1 + d1, r00, r01, r10, r11, loss_row, loss_row], axis=0)
    vec_send, vec_recv = new_ids('s', 10), new_ids('r', 10)

    def vec_lane():
        ready, pending = NOW, []
        for k, axis in enumerate(AXES[::-1][1:] + AXES[PAIR:]):
            yield ready, {axis: STAT_SIZE}, STEP
            for copy in pending[-1:]:
                copy.wait_recv()
            if axis == 'x':
                plane = [vec[t // RING, t % RING] for t in range(BLOCKS)]
                rest_rows = sum(plane[1:], plane[0])
                vecx[xc] = jnp.concatenate([item[:PAIR] for item in plane] + [rest_rows], axis=0)
            own = {'y': vec.at[zc, yc], 'z': vec.at[zc], 'x': vecx.at[xc]}[axis]
            made = [Fan(axis, lambda off, own=own: (own, own), vec_send[k * 3:], vec_recv[k * 3:])]
            made[0].start()
            ready = plan.send(axis, STAT_SIZE, TWO_HOPS)
            pending.extend(made)
        yield ready, {}, STEP
        for copy in made:
            copy.wait_recv()
        got = [vecx[q] for q in range(RING)]
        vecp[core] = (got[0] + got[1]) + (got[PAIR] + got[3])
        copy = rcopy(vecp.at[core], vecp.at[core], vec_send[9], vec_recv[9], peer)
        copy.start()
        yield plan.now + PAIR, {}, NOW
        copy.wait_recv()
        sent(pending + [copy])

    vec_group = plan.add([vec_lane()], first=True)

    dzf, duf = hx, zf

    def embed_emit(j, v, acc):
        u3[view_rows(v), chunk_cols(j)] = acc * inv_n

    def settle_qg():
        for copy in qg:
            copy.wait_recv()

    def embed_product(v):
        if v:
            once('qg', settle_qg)
            forward_rowsplit(zf, wg1, wq1, ((1, 0),), embed_emit)
        else:
            backward_rowsplit(zf, wg1, ((0, 1),), embed_emit)

    sums = []

    def embed_sums():
        first_r = PAIR * BLOCKS + PAIR
        dgb[core, :, half:half + blk] = jnp.broadcast_to(vecp[core, row(first_r + RING), :], (RING, blk))
        mine = pl.ds(pl.multiple_of(BLOCKS * core, BLOCKS), BLOCKS)
        both_cores = vecp[0, mine, :] + vecp[1, mine, :]
        sums.append([lanes_of(vecx[q, row(first_r + PAIR * t + s), :] for q in range(RING) for s in subs) for t in subs])
        sums.append([lanes_of(both_cores[row(PAIR * i + t)] for i in range(HALF_BLOCKS)) for t in subs])

    def embed_apply(v):
        once('sums', embed_sums)
        mean_g, mean_gz = sums[v]
        inv = sres[PAIR, second_row(v), :]

        def fn(rsl):
            emb = zf[core, rsl, :].astype(F32)
            dzf[core, rsl, :] = (inv * (u3[rsl, :] - (mean_g + emb * mean_gz) * inv_n)).astype(BF16)
        apply_rows(v, fn)

    out_ids = {(slot, s): (new_ids('s', 5), new_ids('r', 5)) for slot in range(3) for s in subs}

    def publish(slot, s):
        size = PAIR * blk * blk * PAIR
        up, down = device('x', 1), device('x', 3)
        sid, rid = out_ids[slot, s]
        own = out_w.at[slot, core, xc, s]
        made = [rcopy(own, own, sid[FIRST], rid[FIRST], up), rcopy(own, own, sid[SECOND], rid[SECOND], down)]
        yield NOW, {'x': size}, NOW
        for copy in made:
            copy.start()
        yield plan.send('x', size), {'x': size / PAIR}, NOW
        for k, (off, target) in enumerate(((3, up), (1, down))):
            made[k].wait_recv()
            src = out_w.at[slot, core, near['x'][off], s, pl.ds(k * blk // PAIR, blk // PAIR), :]
            made.append(rcopy(src, src, sid[PAIR + k], rid[PAIR + k], target))
            made[-1].start()
        yield plan.send('x', size / PAIR), {}, NOW
        made[PAIR].wait_recv()
        made[3].wait_recv()
        own = out_w.at[slot, core, :, s]
        made.append(rcopy(own, own, sid[RING], rid[RING], peer))
        made[-1].start()
        yield plan.now + PAIR, {}, NOW
        made[-1].wait_recv()
        sent(made)

    published = []

    def result(slot, buf, s, groups):
        def go():
            if not any(group['left'] for group in groups):
                out_w[slot, core, xc, s] = buf[zc, yc, xc, s]
                published.append(plan.add([publish(slot, s)], first=True))
        return go

    def layer_emit(src, slot, parity, k):
        def emit(j, v, acc):
            cols = chunk_cols(j)
            norm = (src[view_rows(v), cols] - sres[slot, first_row(v), cols]) * sres[slot, second_row(v), cols]
            lin = sres[3, row(k), cols] * norm + sres[3, row(k + 1), cols]
            grad = jnp.where(lin > 0, acc, NOW)
            u3[view_rows(v), cols] = grad
            put_stat(parity, v, cols, col_sum(grad), col_sum(grad * norm))
        return emit

    def layer_rows(src, slot, k, total, v, store):
        sum_lin, sum_norm = total[row(FIRST)], total[row(SECOND)]
        mean, inv = sres[slot, first_row(v), :], sres[slot, second_row(v), :]
        scale = sres[3, row(k), :] * inv

        def fn(rsl):
            norm = (src[rsl, :] - mean) * inv
            store(rsl, (scale * (u3[rsl, :] - (sum_lin + norm * sum_norm) * inv_n)).astype(BF16))
        apply_rows(v, fn)

    def affine_grads(total, k):
        spots = ((row(k), total[row(SECOND)]), (row(k + 1), total[row(FIRST)]))
        for spot, value in spots:
            if ('affine', k) in occurred:
                value = value + dgb[core, spot, :half]
            dgb[core, spot, :half] = value
        occurred.add(('affine', k))

    def add_scatter(slot, buf, batches, lanes):
        groups = {s: [] for s in subs}
        for batch, batch_lanes in zip(batches, lanes):
            s = batch[0]
            groups[s].append(plan.add(batch_lanes, result(slot, buf, s, groups[s])))
        return groups[0] + groups[1]

    scatter_3, scatter_2, part2_groups = [], [], []

    def part3_lane():
        yield NOW, {}, 3.0
        partial_rowsplit(part, xf2, all_rows, dzf, all_rows)
        plan.work(3)

    def start_3():
        scatter_3.extend(add_scatter(PAIR, part, BACK, scatter_lanes(part, 0, BACK, send_w_all, recv_c, give=True)))

    def part2_lane(hh):
        yield NOW, {}, 1.9
        partial_colsplit(part2, xf1, duf, hh)
        plan.work(1.9)

    def start_2():
        scatter_2.extend(add_scatter(1, part2, BACK, scatter_lanes(part2, 1, BACK, send_g, recv_w_all, take=True)))

    a2a_recv, a2a_send = [new_ids('r', BLOCKS) for _ in subs], [new_ids('s', BLOCKS) for _ in subs]
    own_half = lax.div(mid, HALF_BLOCKS)
    self_out = jnp.where(own_half == core, PAIR * (mid - HALF_BLOCKS * core) + core, -1)
    self_in = jnp.where(own_half == core, mid, -1)

    def block(k, v):
        return du1.at[lax.div(k, HALF_BLOCKS), wrap(lax.div(k, PAIR)), lax.rem(k, PAIR), v]

    def spread(v):
        home, home_sem = a2a.at[zc, yc, v], rsem.at[a2a_recv[v][0] + mid]

        @pl.loop(0, BLOCKS)
        def _(k):
            @pl.when(self_out == k)
            def _():
                home[...] = block(k, v)[...]

            @pl.when(self_out != k)
            def _():
                pltpu.make_async_remote_copy(
                    src_ref=block(k, v), dst_ref=home, send_sem=ssem.at[a2a_send[v][0] + k], recv_sem=home_sem,
                    device_id=(HALF_BLOCKS * core + lax.div(k, PAIR), x_base + lax.rem(k, PAIR)),
                    device_id_type=MESH_ID).start()

    def spread_sent(v):
        @pl.loop(0, BLOCKS)
        def _(k):
            @pl.when(self_out != k)
            def _():
                pltpu.make_async_copy(block(k, v), block(k, v), ssem.at[a2a_send[v][0] + k]).wait()

    slots = (hx, zf, xf1, xf2)
    per = RING * rows
    turn = (0, 1, 3, PAIR)
    fetches = {}

    def h_fetch(v, k):
        begin = pl.multiple_of(near['z'][turn[k]] * per, per)
        made = [pltpu.make_async_copy((h_a, h_b)[v].at[pl.ds(begin, per), pl.ds(kh * half, half)],
                                      slots[k].at[kh], hsem.at[k * PAIR + kh]) for kh in subs]
        for copy in made:
            copy.start()
        fetches[v, k] = made

    def dw1_product(v, k):
        zz = near['z'][turn[k]]

        @pl.loop(0, RING)
        def _(i):
            @pl.when(self_in != zz * RING + i)
            def _():
                pltpu.make_async_copy(a2a.at[zz, i, v], a2a.at[zz, i, v],
                                      rsem.at[a2a_recv[v][0] + zz * RING + i]).wait()
        for copy in fetches[v, k]:
            copy.wait()
        grad = jnp.concatenate([a2a[zz, i, v] for i in range(RING)], axis=0)
        more = 'dw1' in occurred
        for kh in subs:
            for q in range(RING):
                res = dot_tn(grad, slots[k][kh, :, q * quad:(q + 1) * quad])
                spot = (slice(kh * blk, (kh + 1) * blk), slice(q * quad, (q + 1) * quad))
                u2[spot] = res + u2[spot] if more else res
        occurred.add('dw1')

    def put_du1(rsl, value, v):
        start = rsl.start - v * vrows
        r = pl.multiple_of(lax.rem(start, rows), min(rstep, rows))
        c = lax.div(start, rows)
        for i in range(HALF_BLOCKS):
            du1[i // RING, i % RING, c, v, pl.ds(r, rstep), :] = value[:, i * blk:(i + 1) * blk]

    def put_du2(rsl, value, v):
        duf[core, rsl, :] = value

    def settle_q2():
        for copy in q2:
            copy.wait_recv()

    def both_in(name):
        return lambda: plan.now if all((name, v) in occurred for v in subs) else FAR

    def backward_lane(v):
        views = ((v, v),)
        yield after(gather_g, v * 3.0), {}, MM
        embed_product(v)
        plan.work(MM)
        yield after([vec_group]), {}, STEP
        embed_apply(v)
        plan.work(0.6)
        copy = share(dzf, v)
        yield plan.now + SHARE, {}, MM
        copy.wait_recv()
        copy.wait_send()
        occurred.add(('dz', v))
        if both_in('dz')() < FAR:
            plan.add([part3_lane()], start_3, first=True)
        backward_rowsplit(dzf, wg3, views, layer_emit(u2, 1, 0, PAIR))
        plan.work(MM)
        out = []
        yield from stat_steps(0, v, out)
        affine_grads(out[0], 0)
        yield both_in('dz'), {}, STEP
        layer_rows(u2, 1, PAIR, out[0], v, functools.partial(put_du2, v=v))
        plan.work(0.6)
        copy = share(duf, v)
        occurred.add(('du2', v))
        if both_in('du2')() < FAR:
            part2_groups.append(plan.add([part2_lane(hh) for hh in subs], start_2, first=True))
        yield plan.now + SHARE, {}, MM
        copy.wait_recv()
        copy.wait_send()
        once('q2', settle_q2)
        backward_colsplit(duf, wg2, wq2, views, layer_emit(u1, 0, 1, 0))
        plan.work(MM)
        occurred.add(('dx1', v))
        yield from stat_steps(1, v, out)
        affine_grads(out[1], PAIR)
        layer_rows(u1, 0, 0, out[1], v, functools.partial(put_du1, v=v))
        spread(v)
        plan.work(0.6)
        arrived = max([plan.send(axis, BLOCKS * rows * blk, TWO_HOPS) for axis in 'zy'])
        early = (PAIR, 1, 0, 0)
        if 'fetch' not in occurred:
            yield lambda: FAR if not part2_groups else max(after(part2_groups)(), both_in('dx1')()), {}, NOW
            if 'fetch' not in occurred:
                occurred.add('fetch')
                for k in range(RING):
                    h_fetch(v, k)
        for k in range(RING):
            yield lambda k=k: arrived - early[k] if (v, k) in fetches else FAR, {}, 0.5
            dw1_product(v, k)
            plan.work(0.6)
            if (1 - v, k) not in fetches:
                h_fetch(1 - v, k)
        spread_sent(v)

    backward = plan.add([backward_lane(v) for v in subs], first=True)
    plan.finish(backward)
    sent(q2 + q3 + qg)
    dg_send, dg_recv = new_ids('s', 1)[0], new_ids('r', 1)[0]
    dg_copy = rcopy(dgb.at[core], dgb.at[core], dg_send, dg_recv, peer)
    dg_copy.start()

    x_recv, x_send = new_ids('r', RING), new_ids('s', RING)

    def strip(k, cols=pl.ds(0, half)):
        return u2.at[pl.ds(pl.multiple_of(k * blk, blk), blk), cols]

    swap = rcopy(strip(other), strip(PAIR), x_send[0], x_recv[0], peer)
    swap.start()
    plan.expect(0, plan.now + 3.0, 'x')
    plan.pump(plan.now + PAIR)
    swap.wait_recv()
    swap.wait_send()
    strip(core)[...] = strip(core)[...] + strip(PAIR)[...]
    shifts = [Fan('x', lambda off: (strip(core, chunk_cols(wrap(xc + off))), strip(3, chunk_cols(off))), x_send[1:],
                  x_recv[1:])]
    for copy in shifts:
        copy.start()
    arrived = plan.send('x', PAIR * quad * blk * RING, TWO_HOPS)
    plan.pump(arrived)
    for copy in shifts:
        copy.wait_recv()
    got = [strip(3, chunk_cols(off))[...] for off in OTHERS]
    piece_sum = (strip(core, chunk_cols(xc))[...] + got[0]) + (got[1] + got[2])
    for s in subs:
        out_w[0, core, xc, s] = piece_sum[:, s * blk:(s + 1) * blk].T
    sent(shifts)
    plan.clear()
    published.append(plan.add([publish(0, s) for s in subs], first=True))
    plan.finish(*scatter_3, *scatter_2)
    plan.finish(*published)
    dg_copy.wait_recv()
    dg_copy.wait_send()
    small_out[...] = dgb[...]


def split_kernel(blk, dw_ref, small_ref, loss_out, dw1_out, dw2_out, dw3_out, dg1_out, db1_out, dg2_out, db2_out,
                 sem_out):
    half = HALF_BLOCKS * blk
    mid = lax.axis_index('model')
    loss_out[...] = small_ref[0, FIRST:SECOND, half:half + 1] + small_ref[1, FIRST:SECOND, half:half + 1]
    for hh in range(PAIR):
        dg2_out[:, hh * half:(hh + 1) * half] = small_ref[hh, FIRST:SECOND, :half]
        db2_out[:, hh * half:(hh + 1) * half] = small_ref[hh, SECOND:PAIR, :half]
    mcols = pl.ds(pl.multiple_of(lax.rem(mid, HALF_BLOCKS) * blk, blk), blk)
    dg1_out[...] = small_ref[lax.div(mid, HALF_BLOCKS), 2:3, mcols]
    db1_out[...] = small_ref[lax.div(mid, HALF_BLOCKS), 3:4, mcols]
    stores = []
    for slot in range(3):
        for t in range(BLOCKS):
            begin = pl.ds(t * blk, blk)
            dst = (dw1_out.at[begin, :], dw2_out.at[:, begin], dw3_out.at[begin, :])[slot]
            stores.append(pltpu.make_async_copy(dw_ref.at[slot, t // HALF_BLOCKS, (t // PAIR) % RING, t % PAIR], dst,
                                                sem_out.at[len(stores)]))
            stores[-1].start()
    for copy in stores:
        copy.wait()


def build_call(blk, rows, total_rows, vmem_limit):
    dim, half = BLOCKS * blk, HALF_BLOCKS * blk
    trows = RING * rows
    pieces = (RING, RING, RING, PAIR, blk, blk)
    got = (PAIR, RING, RING, PAIR, blk, blk)
    act = pltpu.VMEM((PAIR, trows, half), BF16)
    pre = pltpu.VMEM((trows, half), F32)
    bank = (PAIR, RING, PAIR, blk, blk)
    dma = pltpu.SemaphoreType.DMA
    scratch = [
        act, pre, pre, pre, act, act, act,
        pltpu.VMEM(pieces, BF16), pltpu.VMEM(got, BF16), pltpu.VMEM(pieces, BF16), pltpu.VMEM(got, BF16),
        pltpu.VMEM(pieces, BF16),
        pltpu.VMEM(pieces, F32), pltpu.VMEM(pieces, F32),
        pltpu.VMEM((PAIR, 6, RING, PAIR, blk, blk), F32), pltpu.VMEM((PAIR, PAIR, 6, PAIR, blk, blk), F32),
        pltpu.VMEM((PAIR, PAIR, 3, blk, blk), F32),
        pltpu.VMEM((RING, RING, HALF_BLOCKS, blk), F32),
        pltpu.VMEM((PAIR, PAIR, 3, RING, PAIR, half), F32), pltpu.VMEM((RING, RING, half), F32),
        pltpu.VMEM((PAIR, RING, half + blk), F32),
        pltpu.VMEM((PAIR, PAIR, PAIR, half), F32), pltpu.VMEM((RING, RING, HALF_BLOCKS, blk), F32),
        pltpu.VMEM((RING, 40, blk), F32), pltpu.VMEM((PAIR, 40, blk), F32),
        pltpu.VMEM((PAIR, RING, PAIR, PAIR, rows, blk), BF16), pltpu.VMEM((RING, RING, PAIR, rows, blk), BF16),
        dma((N_SEND,)), dma((N_RECV,)), dma((BLOCKS,)), dma((HALF_BLOCKS,)), pltpu.SemaphoreType.REGULAR((12,)),
    ]
    anyspec = pl.BlockSpec(memory_space=pl.ANY)
    vmem = pl.BlockSpec(memory_space=pltpu.VMEM)
    smem = pl.BlockSpec(memory_space=pltpu.SMEM)
    packed = jax.ShapeDtypeStruct((3,) + bank, F32)
    step_call = pl.pallas_call(
        functools.partial(mega_kernel, (blk, rows, total_rows)),
        out_shape=[pltpu.VMEM((3,) + bank, F32), jax.ShapeDtypeStruct((PAIR, RING, half + blk), F32)],
        in_specs=[anyspec] * 7 + [vmem, vmem, smem],
        out_specs=[vmem, vmem],
        scratch_shapes=scratch,
        compiler_params=pltpu.CompilerParams(collective_id=0, has_side_effects=True, vmem_limit_bytes=vmem_limit),
        name='barlow_step',
    )

    def line(n):
        return jax.ShapeDtypeStruct((1, n), F32)

    tall, wide = jax.ShapeDtypeStruct((dim, blk), F32), jax.ShapeDtypeStruct((blk, dim), F32)
    split_call = pl.pallas_call(
        functools.partial(split_kernel, blk),
        out_shape=[line(1), tall, wide, tall, line(blk), line(blk), line(dim), line(dim)],
        in_specs=[vmem, vmem],
        out_specs=[vmem, anyspec, anyspec, anyspec, vmem, vmem, vmem, vmem],
        scratch_shapes=[dma((48,))],
        name='split_results',
    )

    def call(*args):
        packed, small = step_call(*args)
        return split_call(pltpu.with_memory_space_constraint(packed, pltpu.VMEM), small)

    return call


def solution(mesh):
    data_size = mesh.shape['data']

    def shard_body(h_a, h_b, w_one, w_two, w_three, g_one, b_one, g_two, b_two, lam_off):
        group_rows = h_a.shape[0]
        blk = w_three.shape[1]
        rows = group_rows // BLOCKS
        call = build_call(blk, rows, group_rows * data_size, 63_700_000)
        outs = call(h_a, h_b, w_one, w_two, w_three, g_one.reshape(1, -1), b_one.reshape(1, -1),
                    g_two.reshape(1, -1), b_two.reshape(1, -1), lam_off)
        loss, dw1, dw2, dw3, dg1, db1, dg2, db2 = outs
        return (loss.reshape(1), dw1, dw2, dw3, dg1.reshape(-1), db1.reshape(-1), dg2.reshape(-1), db2.reshape(-1))

    in_specs = (P('data', None), P('data', None), P(None, 'model'), P('model', None), P(None, 'model'),
                P('model'), P('model'), P(), P(), P())
    out_specs = (P(), P(None, 'model'), P('model', None), P(None, 'model'), P('model'), P('model'), P(), P())
    return jax.shard_map(shard_body, mesh=mesh, in_specs=in_specs, out_specs=out_specs, check_vma=False)
```
